32 devices in a mesh: rep: 4 (over y, core), fsdp: 8 (over z, x).
Axes of the slice: x: 2, y: 2, z: 4, core: 2. Of those that a mesh axis runs over, the one named last changes fastest.
Arguments:
- tokens: bfloat16 [32128, 768], P(('rep', 'fsdp')), may hold values from -6 to 6
- read_memory: bfloat16 [320, 768], P(('rep', 'fsdp')), may hold values from -6 to 6
- doc_ids: int32 [32, 1004], P(('rep', 'fsdp')), may hold values from 0 to 15, never falling along the last dimension, each value on 1 to 256 neighbouring positions
- w_query: bfloat16 [768, 768], P('fsdp'), may hold values from -0.21875 to 0.21875
- w_key: bfloat16 [768, 768], P('fsdp'), may hold values from -0.21875 to 0.21875
- w_value: bfloat16 [768, 768], P('fsdp'), may hold values from -0.21875 to 0.21875
- w_out: bfloat16 [768, 768], P('fsdp'), may hold values from -1.75 to 1.75
- query_bias: bfloat16 [768], P('fsdp'), may hold values from -3 to 3
- value_bias: bfloat16 [768], P('fsdp'), may hold values from -3 to 3
- out_bias: bfloat16 [768], P('fsdp'), may hold values from -3 to 3
- norm_one_gain: bfloat16 [768], P('fsdp'), may hold values from 0.099609375 to 1.8984375
- norm_one_bias: bfloat16 [768], P('fsdp'), may hold values from -3 to 3
- w_inner: bfloat16 [768, 3072], P('fsdp'), may hold values from -0.21875 to 0.21875
- inner_bias: bfloat16 [3072], P('fsdp'), may hold values from -3 to 3
- w_outer: bfloat16 [3072, 768], P('fsdp'), may hold values from -0.109375 to 0.109375
- outer_bias: bfloat16 [768], P('fsdp'), may hold values from -3 to 3
- norm_two_gain: bfloat16 [768], P('fsdp'), may hold values from 0.099609375 to 1.8984375
- norm_two_bias: bfloat16 [768], P('fsdp'), may hold values from -3 to 3
- out_grad: bfloat16 [32768, 768], P(('rep', 'fsdp')), may hold values from -6 to 6
Outputs:
- layer_out: bfloat16 [32768, 768], P(('rep', 'fsdp'))
- grad_tokens: bfloat16 [32128, 768], P(('rep', 'fsdp'))
- grad_memory: bfloat16 [320, 768], P(('rep', 'fsdp'))
- grad_w_query: float32 [768, 768], P('fsdp')
- grad_w_key: float32 [768, 768], P('fsdp')
- grad_w_value: float32 [768, 768], P('fsdp')
- grad_w_out: float32 [768, 768], P('fsdp')
- grad_query_bias: float32 [768], P('fsdp')
- grad_value_bias: float32 [768], P('fsdp')
- grad_out_bias: float32 [768], P('fsdp')
- grad_norm_one_gain: float32 [768], P('fsdp')
- grad_norm_one_bias: float32 [768], P('fsdp')
- grad_w_inner: float32 [768, 3072], P('fsdp')
- grad_inner_bias: float32 [3072], P('fsdp')
- grad_w_outer: float32 [3072, 768], P('fsdp')
- grad_outer_bias: float32 [768], P('fsdp')
- grad_norm_two_gain: float32 [768], P('fsdp')
- grad_norm_two_bias: float32 [768], P('fsdp')
The draws below stay inside these ranges and needn't reach their ends.
Inputs may be any that keep to these rules, and one draw needn't show every extreme that they name: `doc_ids`: in each sequence the document numbers never fall, every number occurs, each document holds at most 256 tokens and one holds exactly that many.
All inputs are finite; a program needn't handle non-finite values.
Results may differ from the reference program's by a relative error of at most 0.02.
Values may be sent and summed in bfloat16 or wider, within the bound.
A program may use at most 320 MiB of HBM per device.

```python
import math
import jax
import jax.numpy as jnp
import numpy as np
from jax import lax

D = 768
FF = 3072
HEADS = 12
HEAD_DIM = 64
MEM = 10
SEQ_LEN = 1024
SEG_COUNT = 16
SEG_MOST = 256
SEG_ROWS = 1004
SEQS = 32


def steps_of(own_key, shape, shards, least, largest):
    level, own = 1.0, jax.random.fold_in(own_key, 6)
    for position, parts in shards:
        draws = jnp.exp(jax.random.uniform(jax.random.fold_in(own, position), (parts,), jnp.float32, least / len(shards), largest / len(shards)))
        level = level * jnp.repeat(draws, shape[position] // parts).reshape([-1 if axis == position else 1 for axis in range(len(shape))])
    return level


def split_up(count, total, bound, lean):
    loads = [(1 << 20) // math.isqrt(rank ** lean) + 1 for rank in range(2, count + 1)]
    spare, given = total - bound - (count - 1), [1] * (count - 1)
    while spare > 0:
        free = [i for i in range(count - 1) if given[i] < bound]
        mass, remaining = sum([loads[i] for i in free]), spare
        for i in free:
            more = min(bound - given[i], max(1, remaining * loads[i] // mass), spare)
            given[i] = given[i] + more
            spare = spare - more
    return np.array([bound] + given)


def uneven_parts(rng, number_of, total, most, slope):
    if number_of == 2:
        one = jax.random.randint(rng, (), max(1, total - most), min(most, total - 1) + 1)
        return jnp.stack([one, total - one])
    tallies = jnp.asarray(split_up(number_of, total, most, slope), jnp.int32)
    pairs = (number_of - 1) // 2
    donor, taker = tallies[1:1 + 2 * pairs:2], tallies[2:2 + 2 * pairs:2]
    room = jnp.minimum(donor - 1, most - taker)
    passed = jax.random.randint(jax.random.fold_in(rng, 1), (pairs,), 0, 1 << 20) % (room + 1)
    tallies = tallies.at[1:1 + 2 * pairs:2].set(donor - passed).at[2:2 + 2 * pairs:2].set(taker + passed)
    return tallies[jax.random.permutation(jax.random.fold_in(rng, 2), number_of)]


def normal_values(stream_key, extent, width, bound, split=(), kind=jnp.bfloat16):
    drawn = width * jax.random.normal(stream_key, extent, jnp.float32)
    if split:
        drawn = drawn * steps_of(stream_key, extent, split, -0.22, 0.18)
    return jnp.clip(drawn, -bound, bound).astype(kind)


def setup_inputs(seed: int = 0) -> dict:
    key_list = jax.random.split(jax.random.key(seed), 20)
    return {
        "tokens": normal_values(key_list[0], (SEQS * SEG_ROWS, D), 1.0, 6.0, ((0, 32),)),
        "read_memory": normal_values(key_list[1], (SEQS * MEM, D), 1.0, 6.0, ((0, 32),)),
        "doc_ids": jax.vmap(lambda own: jnp.searchsorted(jnp.cumsum(uneven_parts(own, SEG_COUNT, SEG_ROWS, SEG_MOST, 2)), jnp.arange(SEG_ROWS), side="right"))(jax.random.split(key_list[2], SEQS)).reshape((SEQS, SEG_ROWS)).astype(jnp.int32),
        "w_query": normal_values(key_list[3], (D, D), D ** -0.5, 0.21875, ((0, 8),)),
        "w_key": normal_values(key_list[4], (D, D), D ** -0.5, 0.21875, ((0, 8),)),
        "w_value": normal_values(key_list[5], (D, D), D ** -0.5, 0.21875, ((0, 8),)),
        "w_out": normal_values(key_list[6], (D, D), (D // 64) ** -0.5, 1.75, ((0, 8),)),
        "query_bias": normal_values(key_list[7], (D,), 0.5, 3.0, ((0, 8),)),
        "value_bias": normal_values(key_list[8], (D,), 0.5, 3.0, ((0, 8),)),
        "out_bias": normal_values(key_list[9], (D,), 0.5, 3.0, ((0, 8),)),
        "norm_one_gain": jnp.clip(1.0 + 0.18 * jax.random.normal(key_list[10], (D,), jnp.float32), 0.099609375, 1.8984375).astype(jnp.bfloat16),
        "norm_one_bias": normal_values(key_list[11], (D,), 0.5, 3.0, ((0, 8),)),
        "w_inner": normal_values(key_list[12], (D, FF), D ** -0.5, 0.21875, ((0, 8),)),
        "inner_bias": normal_values(key_list[13], (FF,), 0.5, 3.0, ((0, 8),)),
        "w_outer": normal_values(key_list[14], (FF, D), FF ** -0.5, 0.109375, ((0, 8),)),
        "outer_bias": normal_values(key_list[15], (D,), 0.5, 3.0, ((0, 8),)),
        "norm_two_gain": jnp.clip(1.0 + 0.18 * jax.random.normal(key_list[16], (D,), jnp.float32), 0.099609375, 1.8984375).astype(jnp.bfloat16),
        "norm_two_bias": normal_values(key_list[17], (D,), 0.5, 3.0, ((0, 8),)),
        "out_grad": normal_values(key_list[18], (SEQS * SEQ_LEN, D), 1.0, 6.0, ((0, 32),)),
    }


@jax.custom_vjp
def low(v):
    return lax.optimization_barrier(v.astype(jnp.bfloat16)).astype(jnp.float32)

@jax.custom_vjp
def low_back(v):
    return v

def low_keep(v):
    return (low(v), None)

def low_pass(kept, grad):
    return (grad,)

def back_keep(v):
    return (v, None)

def back_low(kept, grad):
    return (low(grad),)
low.defvjp(low_keep, low_pass)
low_back.defvjp(back_keep, back_low)

def layer_norm(value, gain, shift):
    mean = lax.optimization_barrier(jnp.mean(value, axis=-1, keepdims=True))
    centered = value - mean
    spread = lax.optimization_barrier(jnp.mean(centered * centered, axis=-1, keepdims=True))
    return centered * lax.rsqrt(spread + 1e-05) * gain + shift

def matmul(left, right):
    return jnp.dot(left, right, precision=lax.Precision.HIGHEST)

def attend_block(query_block, id_block, keys, values, ids):
    scores = jnp.einsum('qhd,khd->hqk', query_block, keys, precision=lax.Precision.HIGHEST)
    scores = low_back(scores * HEAD_DIM ** (-0.5))
    allowed = (id_block[:, None] == ids[None, :]) | (id_block[:, None] < 0) | (ids[None, :] < 0)
    scores = jnp.where(allowed[None], scores, jnp.float32(-1e+30))
    peak = lax.optimization_barrier(jnp.max(scores, axis=-1, keepdims=True))
    weights = jnp.exp(scores - peak)
    probs = weights / lax.optimization_barrier(jnp.sum(weights, axis=-1, keepdims=True))
    return jnp.einsum('hqk,khd->qhd', low(probs), values, precision=lax.Precision.HIGHEST)

def sequence_forward(rows, ids, params):
    query_mat, key_mat, value_mat, out_mat, query_shift, value_shift, out_shift, gain_one, shift_one, inner_mat, inner_shift, outer_mat, outer_shift, gain_two, shift_two = params
    rows_low = low(rows)
    query = low_back(low(matmul(rows_low, query_mat) + query_shift)).reshape(SEQ_LEN, HEADS, HEAD_DIM)
    keys = low_back(low(matmul(rows_low, key_mat))).reshape(SEQ_LEN, HEADS, HEAD_DIM)
    values = low_back(low(matmul(rows_low, value_mat) + value_shift)).reshape(SEQ_LEN, HEADS, HEAD_DIM)
    block = min(512, SEQ_LEN)
    query_blocks = query.reshape(SEQ_LEN // block, block, HEADS, HEAD_DIM)
    id_blocks = ids.reshape(SEQ_LEN // block, block)
    attended = lax.map(jax.checkpoint(lambda pair: attend_block(pair[0], pair[1], keys, values, ids)), (query_blocks, id_blocks))
    attended = low_back(low(attended.reshape(SEQ_LEN, D)))
    branch = low_back(matmul(attended, out_mat) + out_shift)
    normed = layer_norm(rows + branch, gain_one, shift_one)
    inner = low_back(matmul(low(normed), inner_mat) + inner_shift)
    active = low(jax.nn.gelu(inner, approximate=False))
    outer = low_back(matmul(active, outer_mat) + outer_shift)
    return layer_norm(normed + outer, gain_two, shift_two)

def forward(tokens, memory, params, doc_ids):
    token_rows = tokens.reshape(SEQS, SEG_ROWS, D)
    memory_rows = memory.reshape(SEQS, MEM, D)
    rows = jnp.concatenate([memory_rows, token_rows, memory_rows], axis=1)
    marks = jnp.full((SEQS, MEM), -1, jnp.int32)
    ids = jnp.concatenate([marks, doc_ids.astype(jnp.int32), marks], axis=1)
    result = lax.map(jax.checkpoint(lambda pair: sequence_forward(pair[0], pair[1], params)), (rows, ids))
    return result.reshape(SEQS * SEQ_LEN, D)

def reference(tokens, read_memory, doc_ids, w_query, w_key, w_value, w_out, query_bias, value_bias, out_bias, norm_one_gain, norm_one_bias, w_inner, inner_bias, w_outer, outer_bias, norm_two_gain, norm_two_bias, out_grad):
    params = tuple((item.astype(jnp.float32) for item in (w_query, w_key, w_value, w_out, query_bias, value_bias, out_bias, norm_one_gain, norm_one_bias, w_inner, inner_bias, w_outer, outer_bias, norm_two_gain, norm_two_bias)))
    output, pull = jax.vjp(lambda tok, mem, par: forward(tok, mem, par, doc_ids), tokens.astype(jnp.float32), read_memory.astype(jnp.float32), params)
    grad_tok, grad_mem, grad_par = pull(out_grad.astype(jnp.float32))
    g_wq, g_wk, g_wv, g_wo, g_bq, g_bv, g_bo, g_g1, g_n1, g_w1, g_b1, g_w2, g_b2, g_g2, g_n2 = grad_par
    return (output.astype(jnp.bfloat16), grad_tok.astype(jnp.bfloat16), grad_mem.astype(jnp.bfloat16), g_wq, g_wk, g_wv, g_wo, g_bq, g_bv, g_bo, g_g1, g_n1, g_w1, g_b1, g_w2, g_b2, g_g2, g_n2)
```

```python
from functools import partial

import jax
import jax.numpy as jnp
from jax import lax
from jax.experimental import pallas as pl
from jax.experimental.pallas import tpu as pltpu
from jax.sharding import PartitionSpec as P

MESH_ID = pl.DeviceIdType.MESH
W = 768


class Copies:
    def __init__(self, send, recv):
        self.send, self.recv, self.made = send, recv, {}

    def start(self, name, src, dst, to):
        slot = len(self.made)
        copy = pltpu.make_async_remote_copy(
            src_ref=src,
            dst_ref=dst,
            send_sem=self.send.at[slot],
            recv_sem=self.recv.at[slot],
            device_id=to,
            device_id_type=MESH_ID,
        )
        copy.start()
        self.made[name] = copy

    def arrived(self, name):
        self.made[name].wait_recv()

    def drain(self):
        for copy in self.made.values():
            copy.wait_send()


def place():
    rep, owner = lax.axis_index("rep"), lax.axis_index("fsdp")
    y, c, z, x = rep // 2, rep % 2, owner // 2, owner % 2
    where = {
        "core": (y * 2 + 1 - c, owner),
        "y": ((1 - y) * 2 + c, owner),
        "x": (rep, z * 2 + 1 - x),
    }
    for k in (1, 2, 3):
        where["z", k] = (rep, ((z + k) % 4) * 2 + x)
        where["zx", k] = (rep, ((z + k) % 4) * 2 + 1 - x)
    return rep, owner, y, c, z, x, where


def greet(where):
    barrier = pltpu.get_barrier_semaphore()
    for to in where.values():
        pl.semaphore_signal(barrier, inc=1, device_id=to, device_id_type=MESH_ID)
    pl.semaphore_wait(barrier, len(where))


def gather_kernel(a0, a1, a2, av, o0, o1, o2, ov, send, recv, own_sem):
    rep, owner, y, c, z, x, where = place()
    part = W // 8

    def in0(k, other_x):
        z_of, x_of = (z - k + 4) % 4, (1 - x if other_x else x)
        return o0.at[pl.ds(c * 2, 2), pl.ds((z_of * 2 + x_of) * part, part), :]

    def in1(k, other_x, quarter):
        z_of, x_of = (z - k + 4) % 4, (1 - x if other_x else x)
        return o1.at[quarter, pl.ds((z_of * 2 + x_of) * part, part), :]

    def in2(k, other_x, quarter):
        z_of, x_of = (z - k + 4) % 4, (1 - x if other_x else x)
        return o2.at[pl.ds((z_of * 2 + x_of) * 4 * part + quarter * part, part), :]

    mine, across = rep, (1 - y) * 2 + c
    greet(where)
    own = [
        pltpu.make_async_copy(a0, o0.at[:, pl.ds(owner * part, part), :], own_sem.at[0]),
        pltpu.make_async_copy(a2, o2.at[pl.ds(owner * 4 * part, 4 * part), :], own_sem.at[1]),
        pltpu.make_async_copy(av, ov.at[owner], own_sem.at[2]),
    ]
    for r in range(4):
        own.append(
            pltpu.make_async_copy(
                a1.at[:, r * W : (r + 1) * W],
                o1.at[r, pl.ds(owner * part, part), :],
                own_sem.at[3 + r],
            )
        )
    copies = Copies(send, recv)
    from0 = a0.at[pl.ds(c * 2, 2), :, :]
    from1 = a1.at[:, pl.ds(pl.multiple_of(rep * W, W), W)]
    from2 = a2.at[pl.ds(rep * part, part), :]
    for k in (1, 3, 2):
        copies.start((1, "z", k), from1, in1(0, False, mine), where["z", k])
        copies.start((2, "z", k), from2, in2(0, False, mine), where["z", k])
        copies.start((0, "z", k), from0, in0(0, False), where["z", k])
    copies.start((1, "x", 0), from1, in1(0, False, mine), where["x"])
    copies.start((2, "x", 0), from2, in2(0, False, mine), where["x"])
    copies.start((0, "x", 0), from0, in0(0, False), where["x"])
    for k in (1, 2, 3):
        copies.start(("v", "z", k), av, ov.at[owner], where["z", k])
        copies.start(("v", "zx", k), av, ov.at[owner], where["zx", k])
    copies.start(("v", "x", 0), av, ov.at[owner], where["x"])
    for copy in own:
        copy.start()

    def pass_on(k, other_x, stage):
        for g in (1, 2, 0):
            copies.arrived((g, stage, k))
            here = (
                in0(k, other_x)
                if g == 0
                else in1(k, other_x, mine) if g == 1 else in2(k, other_x, mine)
            )
            if stage == "z":
                copies.start((g, "x", k), here, here, where["x"])
            if g > 0:
                copies.start((g, "y", k, other_x), here, here, where["y"])
            copies.start((g, "core", k, other_x), here, here, where["core"])

    order = [(0, True, "x"), (1, False, "z"), (3, False, "z"), (1, True, "x"), (2, False, "z")]
    order += [(3, True, "x"), (2, True, "x")]
    for step in order:
        pass_on(*step)
    for k, other_x, _ in order:
        for g in (1, 2):
            copies.arrived((g, "y", k, other_x))
            here = in1(k, other_x, across) if g == 1 else in2(k, other_x, across)
            copies.start((g, "diagonal", k, other_x), here, here, where["core"])
    for k, other_x, _ in order:
        for g in (0, 1, 2):
            copies.arrived((g, "core", k, other_x))
        for g in (1, 2):
            copies.arrived((g, "diagonal", k, other_x))
    for k in (1, 2, 3):
        copies.arrived(("v", "z", k))
        copies.arrived(("v", "zx", k))
    copies.arrived(("v", "x", 0))
    copies.drain()
    for copy in own:
        copy.wait()


GATHER_COPIES = 3 * 3 + 3 + 7 + (3 * 3 + 2 * 7 + 3 * 7 + 2 * 7)


def gather_all(stack, inner, outer, vectors):
    low = jnp.bfloat16
    anywhere = pl.BlockSpec(memory_space=pl.ANY)
    return pl.pallas_call(
        gather_kernel,
        out_shape=(
            jax.ShapeDtypeStruct((4, W, W), low),
            jax.ShapeDtypeStruct((4, W, W), low),
            jax.ShapeDtypeStruct((4 * W, W), low),
            jax.ShapeDtypeStruct((8,) + vectors.shape, vectors.dtype),
        ),
        in_specs=[pl.BlockSpec(memory_space=pltpu.VMEM)] * 4,
        out_specs=[anywhere] * 4,
        scratch_shapes=[
            pltpu.SemaphoreType.DMA((GATHER_COPIES,)),
            pltpu.SemaphoreType.DMA((GATHER_COPIES,)),
            pltpu.SemaphoreType.DMA((7,)),
        ],
        compiler_params=pltpu.CompilerParams(collective_id=0, has_side_effects=True),
        name="gather_weights",
    )(stack, inner, outer, vectors)


def total(*refs):
    value = refs[0][...].astype(jnp.float32)
    for ref in refs[1:]:
        value = value + ref[...].astype(jnp.float32)
    return value


def reduce_kernel(
    g0, g1, g2, gv, r0, r1, r2, rv,
    k0, c0, x0, z0, e0, k1, c1, y1, x1, z1, e1, got, vec, send, recv, own_sem, out_sem,
):
    rep, owner, y, c, z, x, where = place()
    part = W // 8
    low = jnp.bfloat16
    flat = [(k, o) for o in (1, 0) for k in (1, 3, 2, 0)]
    slot = {pair: i for i, pair in enumerate(flat)}

    def shard(k, o):
        return ((z + k) % 4) * 2 + (1 - x if o else x)

    def part0(half, k, o):
        return g0.at[pl.ds(half * 2, 2), pl.ds(shard(k, o) * part, part), :]

    def part1(quarter, k, o):
        return g1.at[quarter, pl.ds(shard(k, o) * part, part), :]

    def part2(quarter, k, o):
        return g2.at[pl.ds(shard(k, o) * 4 * part + quarter * part, part), :]

    pieces = {1: part1, 2: part2}
    greet(where)
    copies = Copies(send, recv)
    own = {}

    def load(name, src, dst):
        copy = pltpu.make_async_copy(src, dst, own_sem.at[len(own)])
        copy.start()
        own[name] = copy

    for side in (1, 0):
        quarter_row = (1 - y) if side else y
        for pair in flat:
            i = slot[pair]
            for g in (1, 2):
                piece = pieces[g]
                copies.start(
                    (g, "core", side, i), piece(quarter_row * 2 + 1 - c, *pair),
                    c1.at[g - 1, side, i], where["core"],
                )
                load((g, side, i), piece(quarter_row * 2 + c, *pair), k1.at[g - 1, side, i])
            if side:
                copies.start((0, "core", i), part0(1 - c, *pair), c0.at[i], where["core"])
                load((0, i), part0(c, *pair), k0.at[i])
    for k in (1, 2, 3):
        copies.start(("v", "z", k), gv.at[shard(k, 0)], got.at[k], where["z", k])
        copies.start(("v", "zx", k), gv.at[shard(k, 1)], got.at[3 + k], where["zx", k])
    copies.start(("v", "x", 0), gv.at[shard(0, 1)], got.at[7], where["x"])

    def ready(g, *rest):
        own[(g,) + rest].wait()
        copies.arrived((g, "core") + rest)

    for pair in flat:
        i = slot[pair]
        for g in (1, 2):
            ready(g, 1, i)
            k1[g - 1, 1, i] = total(k1.at[g - 1, 1, i], c1.at[g - 1, 1, i]).astype(low)
            copies.start((g, "y", i), k1.at[g - 1, 1, i], y1.at[g - 1, i], where["y"])
        if pair[1] == 1:
            ready(0, i)
            k0[i] = total(k0.at[i], c0.at[i]).astype(low)
            copies.start((0, "x", i), k0.at[i], x0.at[i], where["x"])
    for pair in flat:
        k, o = pair
        i = slot[pair]
        j = slot[k, 1]
        if o == 1:
            for g in (1, 2):
                ready(g, 0, i)
                copies.arrived((g, "y", i))
                k1[g - 1, 0, i] = total(
                    k1.at[g - 1, 0, i], c1.at[g - 1, 0, i], y1.at[g - 1, i]
                ).astype(low)
                copies.start((g, "x", i), k1.at[g - 1, 0, i], x1.at[g - 1, i], where["x"])
        elif k > 0:
            ready(0, i)
            copies.arrived((0, "x", j))
            k0[i] = total(k0.at[i], c0.at[i], x0.at[j]).astype(low)
            copies.start((0, "z", k), k0.at[i], z0.at[k - 1], where["z", k])
            for g in (1, 2):
                ready(g, 0, i)
                copies.arrived((g, "y", i))
                copies.arrived((g, "x", j))
                k1[g - 1, 0, i] = total(
                    k1.at[g - 1, 0, i], c1.at[g - 1, 0, i], y1.at[g - 1, i], x1.at[g - 1, j]
                ).astype(low)
                copies.start((g, "z", k), k1.at[g - 1, 0, i], z1.at[g - 1, k - 1], where["z", k])
    for k in (1, 2, 3):
        copies.arrived(("v", "z", k))
        copies.arrived(("v", "zx", k))
    copies.arrived(("v", "x", 0))
    load("v", gv.at[owner], got.at[0])
    own["v"].wait()
    value = got[0]
    for i in range(1, 8):
        value = value + got[i]
    vec[0] = value
    copies.start(("v", "core"), vec.at[0], vec.at[1], where["core"])
    i, j = slot[0, 0], slot[0, 1]
    ready(0, i)
    copies.arrived((0, "x", j))
    for k in (1, 2, 3):
        copies.arrived((0, "z", k))
    e0[0] = total(k0.at[i], c0.at[i], x0.at[j], z0.at[0], z0.at[1], z0.at[2]).astype(low)
    copies.start((0, "y"), e0.at[0], e0.at[1], where["y"])
    for g in (1, 2):
        ready(g, 0, i)
        copies.arrived((g, "y", i))
        copies.arrived((g, "x", j))
        for k in (1, 2, 3):
            copies.arrived((g, "z", k))
        e1[g - 1, 0] = total(
            k1.at[g - 1, 0, i], c1.at[g - 1, 0, i], y1.at[g - 1, i], x1.at[g - 1, j],
            z1.at[g - 1, 0], z1.at[g - 1, 1], z1.at[g - 1, 2],
        ).astype(low)
        copies.start((g, "ey"), e1.at[g - 1, 0], e1.at[g - 1, 1], where["y"])
        copies.start((g, "ecore"), e1.at[g - 1, 0], e1.at[g - 1, 2], where["core"])
    copies.arrived(("v", "core"))
    vec[2] = vec[0] + vec[1]
    copies.start(("v", "y"), vec.at[2], vec.at[3], where["y"])
    copies.arrived((0, "y"))
    e0[2] = total(e0.at[0], e0.at[1]).astype(low)
    copies.start((0, "ecore"), e0.at[2], e0.at[3], where["core"])
    for g in (1, 2):
        copies.arrived((g, "ey"))
        copies.start((g, "ediagonal"), e1.at[g - 1, 1], e1.at[g - 1, 3], where["core"])
    r0[pl.ds(c * 2, 2)] = e0[2].astype(jnp.float32)
    outs = (rep, (1 - y) * 2 + c, y * 2 + 1 - c, (1 - y) * 2 + 1 - c)
    for g, r in ((1, r1), (2, r2)):
        r[outs[0]] = e1[g - 1, 0].astype(jnp.float32)
        r[outs[1]] = e1[g - 1, 1].astype(jnp.float32)
        copies.arrived((g, "ecore"))
        r[outs[2]] = e1[g - 1, 2].astype(jnp.float32)
    copies.arrived(("v", "y"))
    rv[...] = vec[2] + vec[3]
    copies.arrived((0, "ecore"))
    r0[pl.ds((1 - c) * 2, 2)] = e0[3].astype(jnp.float32)
    for g, r in ((1, r1), (2, r2)):
        copies.arrived((g, "ediagonal"))
        r[outs[3]] = e1[g - 1, 3].astype(jnp.float32)
    copies.drain()


REDUCE_COPIES = 2 * 16 + 8 + 7 + 16 + 4 + 8 + 9 + 1 + 1 + 4 + 1 + 1 + 2


def reduce_all(stack, inner, outer, vectors):
    low, full = jnp.bfloat16, jnp.float32
    part = W // 8
    anywhere, near = pl.BlockSpec(memory_space=pl.ANY), pl.BlockSpec(memory_space=pltpu.VMEM)
    return pl.pallas_call(
        reduce_kernel,
        out_shape=(
            jax.ShapeDtypeStruct((4, part, W), full),
            jax.ShapeDtypeStruct((4, part, W), full),
            jax.ShapeDtypeStruct((4, part, W), full),
            jax.ShapeDtypeStruct(vectors.shape[1:], full),
        ),
        in_specs=[anywhere] * 4,
        out_specs=[near] * 4,
        scratch_shapes=[
            pltpu.VMEM((8, 2, part, W), low),
            pltpu.VMEM((8, 2, part, W), low),
            pltpu.VMEM((4, 2, part, W), low),
            pltpu.VMEM((3, 2, part, W), low),
            pltpu.VMEM((4, 2, part, W), low),
            pltpu.VMEM((2, 2, 8, part, W), low),
            pltpu.VMEM((2, 2, 8, part, W), low),
            pltpu.VMEM((2, 8, part, W), low),
            pltpu.VMEM((2, 4, part, W), low),
            pltpu.VMEM((2, 3, part, W), low),
            pltpu.VMEM((2, 4, part, W), low),
            pltpu.VMEM(vectors.shape, full),
            pltpu.VMEM((4,) + vectors.shape[1:], full),
            pltpu.SemaphoreType.DMA((REDUCE_COPIES,)),
            pltpu.SemaphoreType.DMA((REDUCE_COPIES,)),
            pltpu.SemaphoreType.DMA((2 * 16 + 8 + 1,)),
            pltpu.SemaphoreType.DMA((1,)),
        ],
        compiler_params=pltpu.CompilerParams(
            collective_id=1, has_side_effects=True, vmem_limit_bytes=56 << 20
        ),
        name="reduce_gradients",
    )(stack, inner, outer, vectors)


SMALL = 9


def pack_shard(values, part):
    flat = jnp.concatenate([value.reshape(-1) for value in values])
    room = -(-flat.shape[0] // 2048) * 2048
    return jnp.pad(flat, (0, room - flat.shape[0])).reshape(-1, 128)


def unpack_full(packed, part):
    flat = packed.reshape(packed.shape[0], -1)
    ends = [part * i for i in range(9)] + [part * 12]
    return [flat[:, lo:hi].reshape(-1) for lo, hi in zip(ends[:-1], ends[1:])]


def pack_full(vectors, owners, part):
    flat = jnp.concatenate([value.reshape(owners, -1) for value in vectors], axis=1)
    room = -(-flat.shape[1] // 2048) * 2048
    return jnp.pad(flat, ((0, 0), (0, room - flat.shape[1]))).reshape(owners, -1, 128)


def plain_gather(stack, inner, outer, vectors):
    owners = lax.axis_size("fsdp")
    gathered = lax.all_gather(inner, "fsdp", axis=0, tiled=True)
    return (
        lax.all_gather(stack, "fsdp", axis=1, tiled=True),
        gathered.reshape(W, 4, W).transpose(1, 0, 2),
        lax.all_gather(outer, "fsdp", axis=0, tiled=True),
        lax.all_gather(vectors, "fsdp", axis=0),
    )


def plain_reduce(stack, inner, outer, vectors):
    def over_all(value, axis):
        part = lax.psum_scatter(value, "fsdp", scatter_dimension=axis, tiled=True)
        return lax.psum(part, "rep").astype(jnp.float32)

    outer_part = over_all(outer, 0)
    return (
        over_all(stack, 1),
        over_all(inner, 1),
        outer_part.reshape(4, -1, W),
        over_all(vectors, 0)[0],
    )


HEADS = 12
HEAD_DIM = 64
def layer_norm(value, gain, shift):
    mean = jnp.mean(value, axis=-1, keepdims=True)
    centered = value - mean
    spread = jnp.mean(centered * centered, axis=-1, keepdims=True)
    return centered * lax.rsqrt(spread + 1e-05) * gain + shift


def product(left, right):
    return jnp.dot(left, right, preferred_element_type=jnp.float32)


def inner_rows(left, right):
    return lax.dot_general(
        left, right, (((0,), (0,)), ((), ())), preferred_element_type=jnp.float32
    )


def against(left, right):
    return lax.dot_general(
        left, right, (((1,), (1,)), ((), ())), preferred_element_type=jnp.float32
    )


def column_sum(values):
    return jnp.sum(values.astype(jnp.float32), axis=0)


def block_scores(query_block, keys, row_ids, col_ids, factor):
    scores = (
        jnp.einsum("qhd,khd->hqk", query_block, keys, preferred_element_type=jnp.float32) * factor
    )
    allowed = (
        (row_ids[:, None] == col_ids[None, :]) | (row_ids[:, None] < 0) | (col_ids[None, :] < 0)
    )
    return jnp.where(allowed[None], scores, jnp.float32(-1e30))


def attend_forward(query, keys, values, ids, factor, block):
    pieces = []
    sums = []
    for start in range(0, query.shape[0], block):
        scores = block_scores(
            query[start : start + block], keys, ids[start : start + block], ids, factor
        )
        peak = jnp.max(scores, axis=-1, keepdims=True)
        weights = jnp.exp(scores - peak)
        total = jnp.sum(weights, axis=-1, keepdims=True)
        probs = (weights / total).astype(jnp.bfloat16)
        pieces.append(jnp.einsum("hqk,khd->qhd", probs, values, preferred_element_type=jnp.float32))
        sums.append(peak + jnp.log(total))
    return (jnp.concatenate(pieces, axis=0), jnp.concatenate(sums, axis=1))


def attend_backward(query, keys, values, ids, log_sums, grad_out, factor, block):
    grad_query = []
    grad_keys = jnp.zeros(keys.shape, jnp.float32)
    grad_values = jnp.zeros(values.shape, jnp.float32)
    for start in range(0, query.shape[0], block):
        query_block = query[start : start + block]
        scores = block_scores(query_block, keys, ids[start : start + block], ids, factor)
        probs = jnp.exp(scores - log_sums[:, start : start + block])
        grad_block = grad_out[start : start + block]
        grad_values = grad_values + jnp.einsum(
            "hqk,qhd->khd",
            probs.astype(jnp.bfloat16),
            grad_block,
            preferred_element_type=jnp.float32,
        )
        grad_probs = jnp.einsum(
            "qhd,khd->hqk", grad_block, values, preferred_element_type=jnp.float32
        )
        centre = jnp.sum(probs * grad_probs, axis=-1, keepdims=True)
        grad_scores = (probs * (grad_probs - centre)).astype(jnp.bfloat16)
        grad_query.append(
            jnp.einsum("hqk,khd->qhd", grad_scores, keys, preferred_element_type=jnp.float32)
            * factor
        )
        grad_keys = (
            grad_keys
            + jnp.einsum(
                "hqk,qhd->khd", grad_scores, query_block, preferred_element_type=jnp.float32
            )
            * factor
        )
    return (jnp.concatenate(grad_query, axis=0), grad_keys, grad_values)


def on_device(
    tokens,
    read_memory,
    doc_ids,
    w_query,
    w_key,
    w_value,
    w_out,
    query_bias,
    value_bias,
    out_bias,
    norm_one_gain,
    norm_one_bias,
    w_inner,
    inner_bias,
    w_outer,
    outer_bias,
    norm_two_gain,
    norm_two_bias,
    out_grad,
):
    owners = lax.axis_size("fsdp")
    wide = owners == 8 and lax.axis_size("rep") == 4
    part = w_query.shape[0]
    small = pack_shard(
        (
            query_bias, value_bias, out_bias, norm_one_gain,
            norm_one_bias, outer_bias, norm_two_gain, norm_two_bias, inner_bias,
        ),
        part,
    )
    gather, reduce = (gather_all, reduce_all) if wide else (plain_gather, plain_reduce)
    weights, inner_blocks, outer_mat, vectors = gather(
        jnp.stack([w_query, w_key, w_value, w_out]), w_inner, w_outer, small
    )
    query_mat, key_mat, value_mat, out_mat = weights
    inner_mat = inner_blocks.transpose(1, 0, 2).reshape(W, 4 * W)
    (
        query_shift, value_shift, out_shift, gain_one,
        shift_one, outer_shift, gain_two, shift_two, inner_shift,
    ) = unpack_full(vectors, part)
    back_query, back_key, back_value, back_out = query_mat, key_mat, value_mat, out_mat
    back_inner, back_outer = inner_mat, outer_mat
    seqs = doc_ids.shape[0]
    seg = doc_ids.shape[1]
    width = tokens.shape[1]
    mem = read_memory.shape[0] // seqs
    length = seg + 2 * mem
    block = min(512, length)
    factor = HEAD_DIM ** (-0.5)
    memory_rows = read_memory.reshape(seqs, mem, width)
    rows = jnp.concatenate([memory_rows, tokens.reshape(seqs, seg, width), memory_rows], axis=1)
    rows = rows.reshape(seqs * length, width)
    marks = jnp.full((seqs, mem), -1, jnp.int32)
    ids = jnp.concatenate([marks, doc_ids, marks], axis=1)

    def split(value):
        return value.reshape(seqs, length, HEADS, HEAD_DIM)

    query = (product(rows, query_mat) + query_shift.astype(jnp.float32)).astype(jnp.bfloat16)
    keys = product(rows, key_mat).astype(jnp.bfloat16)
    values = (product(rows, value_mat) + value_shift.astype(jnp.float32)).astype(jnp.bfloat16)
    attended, log_sums = lax.map(
        lambda item: attend_forward(item[0], item[1], item[2], item[3], factor, block),
        (split(query), split(keys), split(values), ids),
    )
    attended_low = attended.reshape(seqs * length, width).astype(jnp.bfloat16)
    residual = (
        rows.astype(jnp.float32) + product(attended_low, out_mat) + out_shift.astype(jnp.float32)
    )
    normed, norm_one_pull = jax.vjp(
        layer_norm, residual, gain_one.astype(jnp.float32), shift_one.astype(jnp.float32)
    )
    normed_low = normed.astype(jnp.bfloat16)
    inner = product(normed_low, inner_mat) + inner_shift.astype(jnp.float32)
    active, gelu_pull = jax.vjp(partial(jax.nn.gelu, approximate=False), inner)
    active_low = active.astype(jnp.bfloat16)
    second = normed + product(active_low, outer_mat) + outer_shift.astype(jnp.float32)
    output, norm_two_pull = jax.vjp(
        layer_norm, second, gain_two.astype(jnp.float32), shift_two.astype(jnp.float32)
    )
    grad_second, grad_gain_two, grad_shift_two = norm_two_pull(out_grad.astype(jnp.float32))
    grad_outer_low = grad_second.astype(jnp.bfloat16)
    grad_w_outer = inner_rows(active_low, grad_outer_low)
    grad_outer_bias = column_sum(grad_outer_low)
    (grad_inner,) = gelu_pull(against(grad_outer_low, back_outer))
    grad_inner_low = grad_inner.astype(jnp.bfloat16)
    grad_w_inner = inner_rows(normed_low, grad_inner_low)
    grad_inner_bias = column_sum(grad_inner_low)
    grad_normed = grad_second + against(grad_inner_low, back_inner)
    grad_residual, grad_gain_one, grad_shift_one = norm_one_pull(grad_normed)
    grad_branch_low = grad_residual.astype(jnp.bfloat16)
    grad_w_out = inner_rows(attended_low, grad_branch_low)
    grad_out_bias = column_sum(grad_branch_low)
    grad_attended = against(grad_branch_low, back_out).astype(jnp.bfloat16)
    grad_query, grad_keys, grad_values = lax.map(
        lambda item: attend_backward(
            item[0], item[1], item[2], item[3], item[4], item[5], factor, block
        ),
        (split(query), split(keys), split(values), ids, log_sums, split(grad_attended)),
    )
    grad_query_low = grad_query.reshape(seqs * length, width).astype(jnp.bfloat16)
    grad_keys_low = grad_keys.reshape(seqs * length, width).astype(jnp.bfloat16)
    grad_values_low = grad_values.reshape(seqs * length, width).astype(jnp.bfloat16)
    grad_w_query = inner_rows(rows, grad_query_low)
    grad_w_key = inner_rows(rows, grad_keys_low)
    grad_w_value = inner_rows(rows, grad_values_low)
    grad_query_bias = column_sum(grad_query_low)
    grad_value_bias = column_sum(grad_values_low)
    grad_rows = (
        grad_residual
        + against(grad_query_low, back_query)
        + against(grad_keys_low, back_key)
        + against(grad_values_low, back_value)
    ).reshape(seqs, length, width)
    grad_tokens = grad_rows[:, mem : mem + seg].reshape(seqs * seg, width).astype(jnp.bfloat16)
    grad_memory = (
        (grad_rows[:, :mem] + grad_rows[:, mem + seg :])
        .reshape(seqs * mem, width)
        .astype(jnp.bfloat16)
    )
    low = jnp.bfloat16
    stack_share, inner_share, outer_share, small_share = reduce(
        jnp.stack([grad_w_query, grad_w_key, grad_w_value, grad_w_out]).astype(low),
        grad_w_inner.astype(low).reshape(W, 4, W).transpose(1, 0, 2),
        grad_w_outer.astype(low),
        pack_full(
            (
                grad_query_bias, grad_value_bias, grad_out_bias, grad_gain_one,
                grad_shift_one, grad_outer_bias, grad_gain_two, grad_shift_two, grad_inner_bias,
            ),
            owners,
            part,
        ),
    )
    (
        final_bq, final_bv, final_bo, final_g1, final_n1, final_b2, final_g2, final_n2, final_b1,
    ) = unpack_full(small_share[None], part)
    return (
        output.astype(low),
        grad_tokens,
        grad_memory,
        stack_share[0],
        stack_share[1],
        stack_share[2],
        stack_share[3],
        final_bq,
        final_bv,
        final_bo,
        final_g1,
        final_n1,
        inner_share.transpose(1, 0, 2).reshape(part, 4 * W),
        final_b1,
        outer_share.reshape(4 * part, W),
        final_b2,
        final_g2,
        final_n2,
    )


def solution(mesh):
    return jax.shard_map(
        on_device,
        mesh=mesh,
        in_specs=(
            P(("rep", "fsdp"), None),
            P(("rep", "fsdp"), None),
            P(("rep", "fsdp"), None),
            P("fsdp", None),
            P("fsdp", None),
            P("fsdp", None),
            P("fsdp", None),
            P("fsdp"),
            P("fsdp"),
            P("fsdp"),
            P("fsdp"),
            P("fsdp"),
            P("fsdp", None),
            P("fsdp"),
            P("fsdp", None),
            P("fsdp"),
            P("fsdp"),
            P("fsdp"),
            P(("rep", "fsdp"), None),
        ),
        out_specs=(
            P(("rep", "fsdp"), None),
            P(("rep", "fsdp"), None),
            P(("rep", "fsdp"), None),
            P("fsdp", None),
            P("fsdp", None),
            P("fsdp", None),
            P("fsdp", None),
            P("fsdp"),
            P("fsdp"),
            P("fsdp"),
            P("fsdp"),
            P("fsdp"),
            P("fsdp", None),
            P("fsdp"),
            P("fsdp", None),
            P("fsdp"),
            P("fsdp"),
            P("fsdp"),
        ),
        check_vma=False,
    )
```

```python
import functools
import math

import jax
import jax.numpy as jnp
from jax import lax
from jax.experimental import pallas as pl
from jax.experimental.pallas import tpu as pltpu
from jax.sharding import PartitionSpec as P

MESH_ID = pl.DeviceIdType.MESH
W = 768


class Copies:
    def __init__(self, send, recv):
        self.send, self.recv, self.made = send, recv, {}

    def start(self, name, src, dst, to):
        slot = len(self.made)
        copy = pltpu.make_async_remote_copy(
            src_ref=src,
            dst_ref=dst,
            send_sem=self.send.at[slot],
            recv_sem=self.recv.at[slot],
            device_id=to,
            device_id_type=MESH_ID,
        )
        copy.start()
        self.made[name] = copy

    def arrived(self, name):
        self.made[name].wait_recv()

    def drain(self):
        for copy in self.made.values():
            copy.wait_send()


def place():
    rep, owner = lax.axis_index("rep"), lax.axis_index("fsdp")
    y, c, z, x = rep // 2, rep % 2, owner // 2, owner % 2
    where = {
        "core": (y * 2 + 1 - c, owner),
        "y": ((1 - y) * 2 + c, owner),
        "x": (rep, z * 2 + 1 - x),
    }
    for k in (1, 2, 3):
        where["z", k] = (rep, ((z + k) % 4) * 2 + x)
        where["zx", k] = (rep, ((z + k) % 4) * 2 + 1 - x)
    return rep, owner, y, c, z, x, where


def greet(where):
    barrier = pltpu.get_barrier_semaphore()
    for to in where.values():
        pl.semaphore_signal(barrier, inc=1, device_id=to, device_id_type=MESH_ID)
    pl.semaphore_wait(barrier, len(where))


def gather_kernel(a0, a1, a2, av, o0, o1, o2, ov, send, recv, own_sem):
    rep, owner, y, c, z, x, where = place()
    part = W // 8

    def in0(k, other_x):
        z_of, x_of = (z - k + 4) % 4, (1 - x if other_x else x)
        return o0.at[pl.ds(c * 2, 2), pl.ds((z_of * 2 + x_of) * part, part), :]

    def in1(k, other_x, quarter):
        z_of, x_of = (z - k + 4) % 4, (1 - x if other_x else x)
        return o1.at[quarter, pl.ds((z_of * 2 + x_of) * part, part), :]

    def in2(k, other_x, quarter):
        z_of, x_of = (z - k + 4) % 4, (1 - x if other_x else x)
        return o2.at[pl.ds((z_of * 2 + x_of) * 4 * part + quarter * part, part), :]

    mine, across = rep, (1 - y) * 2 + c
    greet(where)
    own = [
        pltpu.make_async_copy(a0, o0.at[:, pl.ds(owner * part, part), :], own_sem.at[0]),
        pltpu.make_async_copy(a2, o2.at[pl.ds(owner * 4 * part, 4 * part), :], own_sem.at[1]),
        pltpu.make_async_copy(av, ov.at[owner], own_sem.at[2]),
    ]
    for r in range(4):
        own.append(
            pltpu.make_async_copy(
                a1.at[:, r * W : (r + 1) * W],
                o1.at[r, pl.ds(owner * part, part), :],
                own_sem.at[3 + r],
            )
        )
    copies = Copies(send, recv)
    from0 = a0.at[pl.ds(c * 2, 2), :, :]
    from1 = a1.at[:, pl.ds(pl.multiple_of(rep * W, W), W)]
    from2 = a2.at[pl.ds(rep * part, part), :]
    for k in (1, 3, 2):
        copies.start((1, "z", k), from1, in1(0, False, mine), where["z", k])
        copies.start((2, "z", k), from2, in2(0, False, mine), where["z", k])
        copies.start((0, "z", k), from0, in0(0, False), where["z", k])
    copies.start((1, "x", 0), from1, in1(0, False, mine), where["x"])
    copies.start((2, "x", 0), from2, in2(0, False, mine), where["x"])
    copies.start((0, "x", 0), from0, in0(0, False), where["x"])
    for k in (1, 2, 3):
        copies.start(("v", "z", k), av, ov.at[owner], where["z", k])
        copies.start(("v", "zx", k), av, ov.at[owner], where["zx", k])
    copies.start(("v", "x", 0), av, ov.at[owner], where["x"])
    for copy in own:
        copy.start()

    def pass_on(k, other_x, stage):
        for g in (1, 2, 0):
            copies.arrived((g, stage, k))
            here = (
                in0(k, other_x)
                if g == 0
                else in1(k, other_x, mine) if g == 1 else in2(k, other_x, mine)
            )
            if stage == "z":
                copies.start((g, "x", k), here, here, where["x"])
            if g > 0:
                copies.start((g, "y", k, other_x), here, here, where["y"])
            copies.start((g, "core", k, other_x), here, here, where["core"])

    order = [(0, True, "x"), (1, False, "z"), (3, False, "z"), (1, True, "x"), (2, False, "z")]
    order += [(3, True, "x"), (2, True, "x")]
    for step in order:
        pass_on(*step)
    for k, other_x, _ in order:
        for g in (1, 2):
            copies.arrived((g, "y", k, other_x))
            here = in1(k, other_x, across) if g == 1 else in2(k, other_x, across)
            copies.start((g, "diagonal", k, other_x), here, here, where["core"])
    for k, other_x, _ in order:
        for g in (0, 1, 2):
            copies.arrived((g, "core", k, other_x))
        for g in (1, 2):
            copies.arrived((g, "diagonal", k, other_x))
    for k in (1, 2, 3):
        copies.arrived(("v", "z", k))
        copies.arrived(("v", "zx", k))
    copies.arrived(("v", "x", 0))
    copies.drain()
    for copy in own:
        copy.wait()


GATHER_COPIES = 3 * 3 + 3 + 7 + (3 * 3 + 2 * 7 + 3 * 7 + 2 * 7)


def gather_all(stack, inner, outer, vectors):
    low = jnp.bfloat16
    anywhere = pl.BlockSpec(memory_space=pl.ANY)
    return pl.pallas_call(
        gather_kernel,
        out_shape=(
            jax.ShapeDtypeStruct((4, W, W), low),
            jax.ShapeDtypeStruct((4, W, W), low),
            jax.ShapeDtypeStruct((4 * W, W), low),
            jax.ShapeDtypeStruct((8,) + vectors.shape, vectors.dtype),
        ),
        in_specs=[pl.BlockSpec(memory_space=pltpu.VMEM)] * 4,
        out_specs=[anywhere] * 4,
        scratch_shapes=[
            pltpu.SemaphoreType.DMA((GATHER_COPIES,)),
            pltpu.SemaphoreType.DMA((GATHER_COPIES,)),
            pltpu.SemaphoreType.DMA((7,)),
        ],
        compiler_params=pltpu.CompilerParams(collective_id=0, has_side_effects=True),
        name="gather_weights",
    )(stack, inner, outer, vectors)


def total(*refs):
    value = refs[0][...].astype(jnp.float32)
    for ref in refs[1:]:
        value = value + ref[...].astype(jnp.float32)
    return value


def reduce_kernel(
    g0, g1, g2, gv, r0, r1, r2, rv,
    k0, c0, x0, z0, e0, k1, c1, y1, x1, z1, e1, got, vec, send, recv, own_sem, out_sem,
):
    rep, owner, y, c, z, x, where = place()
    part = W // 8
    low = jnp.bfloat16
    flat = [(k, o) for o in (1, 0) for k in (1, 3, 2, 0)]
    slot = {pair: i for i, pair in enumerate(flat)}

    def shard(k, o):
        return ((z + k) % 4) * 2 + (1 - x if o else x)

    def part0(half, k, o):
        return g0.at[pl.ds(half * 2, 2), pl.ds(shard(k, o) * part, part), :]

    def part1(quarter, k, o):
        return g1.at[quarter, pl.ds(shard(k, o) * part, part), :]

    def part2(quarter, k, o):
        return g2.at[pl.ds(shard(k, o) * 4 * part + quarter * part, part), :]

    pieces = {1: part1, 2: part2}
    greet(where)
    copies = Copies(send, recv)
    own = {}

    def load(name, src, dst):
        copy = pltpu.make_async_copy(src, dst, own_sem.at[len(own)])
        copy.start()
        own[name] = copy

    for side in (1, 0):
        quarter_row = (1 - y) if side else y
        for pair in flat:
            i = slot[pair]
            for g in (1, 2):
                piece = pieces[g]
                copies.start(
                    (g, "core", side, i), piece(quarter_row * 2 + 1 - c, *pair),
                    c1.at[g - 1, side, i], where["core"],
                )
                load((g, side, i), piece(quarter_row * 2 + c, *pair), k1.at[g - 1, side, i])
            if side:
                copies.start((0, "core", i), part0(1 - c, *pair), c0.at[i], where["core"])
                load((0, i), part0(c, *pair), k0.at[i])
    for k in (1, 2, 3):
        copies.start(("v", "z", k), gv.at[shard(k, 0)], got.at[k], where["z", k])
        copies.start(("v", "zx", k), gv.at[shard(k, 1)], got.at[3 + k], where["zx", k])
    copies.start(("v", "x", 0), gv.at[shard(0, 1)], got.at[7], where["x"])

    def ready(g, *rest):
        own[(g,) + rest].wait()
        copies.arrived((g, "core") + rest)

    for pair in flat:
        i = slot[pair]
        for g in (1, 2):
            ready(g, 1, i)
            k1[g - 1, 1, i] = total(k1.at[g - 1, 1, i], c1.at[g - 1, 1, i]).astype(low)
            copies.start((g, "y", i), k1.at[g - 1, 1, i], y1.at[g - 1, i], where["y"])
        if pair[1] == 1:
            ready(0, i)
            k0[i] = total(k0.at[i], c0.at[i]).astype(low)
            copies.start((0, "x", i), k0.at[i], x0.at[i], where["x"])
    for pair in flat:
        k, o = pair
        i = slot[pair]
        j = slot[k, 1]
        if o == 1:
            for g in (1, 2):
                ready(g, 0, i)
                copies.arrived((g, "y", i))
                k1[g - 1, 0, i] = total(
                    k1.at[g - 1, 0, i], c1.at[g - 1, 0, i], y1.at[g - 1, i]
                ).astype(low)
                copies.start((g, "x", i), k1.at[g - 1, 0, i], x1.at[g - 1, i], where["x"])
        elif k > 0:
            ready(0, i)
            copies.arrived((0, "x", j))
            k0[i] = total(k0.at[i], c0.at[i], x0.at[j]).astype(low)
            copies.start((0, "z", k), k0.at[i], z0.at[k - 1], where["z", k])
            for g in (1, 2):
                ready(g, 0, i)
                copies.arrived((g, "y", i))
                copies.arrived((g, "x", j))
                k1[g - 1, 0, i] = total(
                    k1.at[g - 1, 0, i], c1.at[g - 1, 0, i], y1.at[g - 1, i], x1.at[g - 1, j]
                ).astype(low)
                copies.start((g, "z", k), k1.at[g - 1, 0, i], z1.at[g - 1, k - 1], where["z", k])
    for k in (1, 2, 3):
        copies.arrived(("v", "z", k))
        copies.arrived(("v", "zx", k))
    copies.arrived(("v", "x", 0))
    load("v", gv.at[owner], got.at[0])
    own["v"].wait()
    value = got[0]
    for i in range(1, 8):
        value = value + got[i]
    vec[0] = value
    copies.start(("v", "core"), vec.at[0], vec.at[1], where["core"])
    i, j = slot[0, 0], slot[0, 1]
    ready(0, i)
    copies.arrived((0, "x", j))
    for k in (1, 2, 3):
        copies.arrived((0, "z", k))
    e0[0] = total(k0.at[i], c0.at[i], x0.at[j], z0.at[0], z0.at[1], z0.at[2]).astype(low)
    copies.start((0, "y"), e0.at[0], e0.at[1], where["y"])
    for g in (1, 2):
        ready(g, 0, i)
        copies.arrived((g, "y", i))
        copies.arrived((g, "x", j))
        for k in (1, 2, 3):
            copies.arrived((g, "z", k))
        e1[g - 1, 0] = total(
            k1.at[g - 1, 0, i], c1.at[g - 1, 0, i], y1.at[g - 1, i], x1.at[g - 1, j],
            z1.at[g - 1, 0], z1.at[g - 1, 1], z1.at[g - 1, 2],
        ).astype(low)
        copies.start((g, "ey"), e1.at[g - 1, 0], e1.at[g - 1, 1], where["y"])
        copies.start((g, "ecore"), e1.at[g - 1, 0], e1.at[g - 1, 2], where["core"])
    copies.arrived(("v", "core"))
    vec[2] = vec[0] + vec[1]
    copies.start(("v", "y"), vec.at[2], vec.at[3], where["y"])
    copies.arrived((0, "y"))
    e0[2] = total(e0.at[0], e0.at[1]).astype(low)
    copies.start((0, "ecore"), e0.at[2], e0.at[3], where["core"])
    for g in (1, 2):
        copies.arrived((g, "ey"))
        copies.start((g, "ediagonal"), e1.at[g - 1, 1], e1.at[g - 1, 3], where["core"])
    r0[pl.ds(c * 2, 2)] = e0[2].astype(jnp.float32)
    outs = (rep, (1 - y) * 2 + c, y * 2 + 1 - c, (1 - y) * 2 + 1 - c)
    for g, r in ((1, r1), (2, r2)):
        r[outs[0]] = e1[g - 1, 0].astype(jnp.float32)
        r[outs[1]] = e1[g - 1, 1].astype(jnp.float32)
        copies.arrived((g, "ecore"))
        r[outs[2]] = e1[g - 1, 2].astype(jnp.float32)
    copies.arrived(("v", "y"))
    rv[...] = vec[2] + vec[3]
    copies.arrived((0, "ecore"))
    r0[pl.ds((1 - c) * 2, 2)] = e0[3].astype(jnp.float32)
    for g, r in ((1, r1), (2, r2)):
        copies.arrived((g, "ediagonal"))
        r[outs[3]] = e1[g - 1, 3].astype(jnp.float32)
    copies.drain()


REDUCE_COPIES = 2 * 16 + 8 + 7 + 16 + 4 + 8 + 9 + 1 + 1 + 4 + 1 + 1 + 2


def reduce_all(stack, inner, outer, vectors):
    low, full = jnp.bfloat16, jnp.float32
    part = W // 8
    anywhere, near = pl.BlockSpec(memory_space=pl.ANY), pl.BlockSpec(memory_space=pltpu.VMEM)
    return pl.pallas_call(
        reduce_kernel,
        out_shape=(
            jax.ShapeDtypeStruct((4, part, W), full),
            jax.ShapeDtypeStruct((4, part, W), full),
            jax.ShapeDtypeStruct((4, part, W), full),
            jax.ShapeDtypeStruct(vectors.shape[1:], full),
        ),
        in_specs=[anywhere] * 4,
        out_specs=[near] * 4,
        scratch_shapes=[
            pltpu.VMEM((8, 2, part, W), low),
            pltpu.VMEM((8, 2, part, W), low),
            pltpu.VMEM((4, 2, part, W), low),
            pltpu.VMEM((3, 2, part, W), low),
            pltpu.VMEM((4, 2, part, W), low),
            pltpu.VMEM((2, 2, 8, part, W), low),
            pltpu.VMEM((2, 2, 8, part, W), low),
            pltpu.VMEM((2, 8, part, W), low),
            pltpu.VMEM((2, 4, part, W), low),
            pltpu.VMEM((2, 3, part, W), low),
            pltpu.VMEM((2, 4, part, W), low),
            pltpu.VMEM(vectors.shape, full),
            pltpu.VMEM((4,) + vectors.shape[1:], full),
            pltpu.SemaphoreType.DMA((REDUCE_COPIES,)),
            pltpu.SemaphoreType.DMA((REDUCE_COPIES,)),
            pltpu.SemaphoreType.DMA((2 * 16 + 8 + 1,)),
            pltpu.SemaphoreType.DMA((1,)),
        ],
        compiler_params=pltpu.CompilerParams(
            collective_id=1, has_side_effects=True, vmem_limit_bytes=56 << 20
        ),
        name="reduce_gradients",
    )(stack, inner, outer, vectors)


def pack_shard(values, part):
    flat = jnp.concatenate([value.reshape(-1) for value in values])
    room = -(-flat.shape[0] // 2048) * 2048
    return jnp.pad(flat, (0, room - flat.shape[0])).reshape(-1, 128)


def unpack_full(packed, part):
    flat = packed.reshape(packed.shape[0], -1)
    ends = [part * i for i in range(9)] + [part * 12]
    return [flat[:, lo:hi].reshape(-1) for lo, hi in zip(ends[:-1], ends[1:])]


def pack_full(vectors, owners, part):
    flat = jnp.concatenate([value.reshape(owners, -1) for value in vectors], axis=1)
    room = -(-flat.shape[1] // 2048) * 2048
    return jnp.pad(flat, ((0, 0), (0, room - flat.shape[1]))).reshape(owners, -1, 128)


def plain_gather(stack, inner, outer, vectors):
    owners = lax.axis_size("fsdp")
    gathered = lax.all_gather(inner, "fsdp", axis=0, tiled=True)
    return (
        lax.all_gather(stack, "fsdp", axis=1, tiled=True),
        gathered.reshape(W, 4, W).transpose(1, 0, 2),
        lax.all_gather(outer, "fsdp", axis=0, tiled=True),
        lax.all_gather(vectors, "fsdp", axis=0),
    )


def plain_reduce(stack, inner, outer, vectors):
    def over_all(value, axis):
        part = lax.psum_scatter(value, "fsdp", scatter_dimension=axis, tiled=True)
        return lax.psum(part, "rep").astype(jnp.float32)

    outer_part = over_all(outer, 0)
    return (
        over_all(stack, 1),
        over_all(inner, 1),
        outer_part.reshape(4, -1, W),
        over_all(vectors, 0)[0],
    )


def layer_norm(value, gain, shift):
    mean = jnp.mean(value, axis=-1, keepdims=True)
    centered = value - mean
    spread = jnp.mean(centered * centered, axis=-1, keepdims=True)
    return centered * lax.rsqrt(spread + 1e-05) * gain + shift


def product(left, right):
    return jnp.dot(left, right, preferred_element_type=jnp.float32)


def inner_rows(left, right):
    return lax.dot_general(
        left, right, (((0,), (0,)), ((), ())), preferred_element_type=jnp.float32
    )


def against(left, right):
    return lax.dot_general(
        left, right, (((1,), (1,)), ((), ())), preferred_element_type=jnp.float32
    )


def column_sum(values):
    return jnp.sum(values.astype(jnp.float32), axis=0)


TILE = 128
HEAD_DIM = 64
FACTOR = HEAD_DIM ** (-0.5)
HIDDEN = -1e30


def spans(i, count):
    last = count - 1
    if i == last:
        return [(0, count * TILE)]
    low, high = max(0, i - 2), min(last, i + 2)
    if high == last:
        return [(low * TILE, count * TILE)]
    return [(low * TILE, (high + 1) * TILE), (last * TILE, count * TILE)]


def two_heads(block):
    lanes = lax.broadcasted_iota(jnp.int32, block.shape, 1)
    zero = jnp.zeros_like(block)
    first = jnp.where(lanes < HEAD_DIM, block, zero)
    second = jnp.where(lanes < HEAD_DIM, zero, block)
    return jnp.concatenate([first, second], axis=0)


def own_head(value):
    rows = lax.broadcasted_iota(jnp.int32, (TILE, TILE), 0)
    return jnp.where(rows < HEAD_DIM, value[:, :TILE], value[:, TILE:]).T


def masked_scores(k_ref, key_ids, query_ids, stacked, i, span, count):
    low, high = span
    scores = against(k_ref[low:high, :], stacked)
    ids = key_ids[low:high, :]
    row = query_ids[i : i + 1, :]
    seen = ids == row
    if high == count * TILE:
        seen = seen | (ids < 0)
    if i == count - 1:
        seen = seen | (row < 0)
    return jnp.concatenate(
        [jnp.where(seen, scores[:, :TILE], HIDDEN), jnp.where(seen, scores[:, TILE:], HIDDEN)], axis=1
    )


def attend_kernel(key_ids, query_ids, q_ref, k_ref, v_ref, out_ref, lse_ref, v_turned):
    count = q_ref.shape[0] // TILE
    v_turned[...] = v_ref[...].T
    for i in range(count):
        rows = slice(i * TILE, (i + 1) * TILE)
        stacked = two_heads(q_ref[rows, :] * jnp.bfloat16(FACTOR))
        parts = spans(i, count)
        scores = [masked_scores(k_ref, key_ids, query_ids, stacked, i, p, count) for p in parts]
        peak = functools.reduce(
            jnp.maximum, [jnp.max(s, axis=0, keepdims=True) for s in scores]
        )
        weights = [jnp.exp(s - peak) for s in scores]
        total = sum(jnp.sum(w, axis=0, keepdims=True) for w in weights)
        mixed = sum(
            product(v_turned[:, low:high], w.astype(jnp.bfloat16)) for (low, high), w in zip(parts, weights)
        )
        out_ref[rows, :] = own_head(mixed * (1.0 / total)).astype(jnp.bfloat16)
        lse_ref[0, i : i + 1, :] = peak + jnp.log(total)


def attend_back_kernel(
    key_ids, query_ids, q_ref, k_ref, v_ref, g_ref, lse_ref, gq_ref, gk_ref, gv_ref,
    k_turned, k_total, v_total,
):
    count = q_ref.shape[0] // TILE
    k_turned[...] = k_ref[...].T
    k_total[...] = jnp.zeros_like(k_total)
    v_total[...] = jnp.zeros_like(v_total)
    for i in range(count):
        rows = slice(i * TILE, (i + 1) * TILE)
        stacked = two_heads(q_ref[rows, :] * jnp.bfloat16(FACTOR))
        grads = two_heads(g_ref[rows, :])
        lse = lse_ref[0, i : i + 1, :]
        parts = spans(i, count)
        probs, pulls = [], []
        for low, high in parts:
            scores = masked_scores(k_ref, key_ids, query_ids, stacked, i, (low, high), count)
            p = jnp.exp(scores - lse)
            v_total[low:high, :] += product(p.astype(jnp.bfloat16), grads)
            probs.append(p)
            pulls.append(against(v_ref[low:high, :], grads))
        centre = sum(jnp.sum(p * g, axis=0, keepdims=True) for p, g in zip(probs, pulls))
        mixed = 0.0
        for (low, high), p, g in zip(parts, probs, pulls):
            turned = (p * (g - centre)).astype(jnp.bfloat16)
            k_total[low:high, :] += product(turned, stacked)
            mixed = mixed + product(k_turned[:, low:high], turned)
        gq_ref[rows, :] = (own_head(mixed) * FACTOR).astype(jnp.bfloat16)
    gk_ref[...] = k_total[...].astype(jnp.bfloat16)
    gv_ref[...] = v_total[...].astype(jnp.bfloat16)


def attend(key_ids, query_ids, query, keys, values):
    rows, width = query.shape
    pair = 2 * HEAD_DIM
    count = rows // TILE
    column = pl.BlockSpec((rows, pair), lambda h: (0, h))
    whole = lambda a: pl.BlockSpec(a.shape, lambda h: (0, 0))
    return pl.pallas_call(
        attend_kernel,
        grid=(width // pair,),
        out_shape=(
            jax.ShapeDtypeStruct((rows, width), jnp.bfloat16),
            jax.ShapeDtypeStruct((width // pair, count, 2 * TILE), jnp.float32),
        ),
        in_specs=[whole(key_ids), whole(query_ids), column, column, column],
        out_specs=[column, pl.BlockSpec((1, count, 2 * TILE), lambda h: (h, 0, 0))],
        scratch_shapes=[pltpu.VMEM((pair, rows), jnp.bfloat16)],
        compiler_params=pltpu.CompilerParams(vmem_limit_bytes=48 << 20),
        name="attend",
    )(key_ids, query_ids, query, keys, values)


def attend_back(key_ids, query_ids, query, keys, values, grads, lse):
    rows, width = query.shape
    pair = 2 * HEAD_DIM
    count = rows // TILE
    column = pl.BlockSpec((rows, pair), lambda h: (0, h))
    whole = lambda a: pl.BlockSpec(a.shape, lambda h: (0, 0))
    return pl.pallas_call(
        attend_back_kernel,
        grid=(width // pair,),
        out_shape=(jax.ShapeDtypeStruct((rows, width), jnp.bfloat16),) * 3,
        in_specs=[whole(key_ids), whole(query_ids)]
        + [column] * 4
        + [pl.BlockSpec((1, count, 2 * TILE), lambda h: (h, 0, 0))],
        out_specs=[column] * 3,
        scratch_shapes=[
            pltpu.VMEM((pair, rows), jnp.bfloat16),
            pltpu.VMEM((rows, pair), jnp.float32),
            pltpu.VMEM((rows, pair), jnp.float32),
        ],
        compiler_params=pltpu.CompilerParams(vmem_limit_bytes=48 << 20),
        name="attend_back",
    )(key_ids, query_ids, query, keys, values, grads, lse)


ERFC_TERMS = (
    -1.26551223, 1.00002368, 0.37409196, 0.09678418, -0.18628806,
    0.27886807, -1.13520398, 1.48851587, -0.82215223, 0.17087277,
)


def gelu_and_slope(value):
    half_square = value * value * 0.5
    step = 1.0 / (1.0 + jnp.abs(value) * (0.5 * 0.5**0.5))
    power = ERFC_TERMS[-1]
    for term in ERFC_TERMS[-2::-1]:
        power = power * step + term
    tail = 0.5 * step * jnp.exp(power - half_square)
    cover = jnp.where(value < 0, tail, 1.0 - tail)
    density = jnp.exp(-half_square) * ((0.5 / math.pi) ** 0.5)
    return value * cover, cover + value * density


def on_device(
    tokens,
    read_memory,
    doc_ids,
    w_query,
    w_key,
    w_value,
    w_out,
    query_bias,
    value_bias,
    out_bias,
    norm_one_gain,
    norm_one_bias,
    w_inner,
    inner_bias,
    w_outer,
    outer_bias,
    norm_two_gain,
    norm_two_bias,
    out_grad,
):
    owners = lax.axis_size("fsdp")
    wide = owners == 8 and lax.axis_size("rep") == 4
    part = w_query.shape[0]
    small = pack_shard(
        (
            query_bias, value_bias, out_bias, norm_one_gain,
            norm_one_bias, outer_bias, norm_two_gain, norm_two_bias, inner_bias,
        ),
        part,
    )
    gather, reduce = (gather_all, reduce_all) if wide else (plain_gather, plain_reduce)
    weights, inner_blocks, outer_mat, vectors = gather(
        jnp.stack([w_query, w_key, w_value, w_out]), w_inner, w_outer, small
    )
    query_mat, key_mat, value_mat, out_mat = weights
    inner_mat = inner_blocks.transpose(1, 0, 2).reshape(W, 4 * W)
    (
        query_shift, value_shift, out_shift, gain_one,
        shift_one, outer_shift, gain_two, shift_two, inner_shift,
    ) = unpack_full(vectors, part)
    back_query, back_key, back_value, back_out = query_mat, key_mat, value_mat, out_mat
    back_inner, back_outer = inner_mat, outer_mat
    seqs, seg = doc_ids.shape
    width = tokens.shape[1]
    mem = read_memory.shape[0] // seqs
    length = seg + 2 * mem
    memory_rows = read_memory.reshape(seqs, mem, width)
    rows = jnp.concatenate([tokens.reshape(seqs, seg, width), memory_rows, memory_rows], axis=1)
    rows = rows.reshape(seqs * length, width)
    marks = jnp.full((seqs, 2 * mem), -1, jnp.int32)
    ids = jnp.concatenate([doc_ids, marks], axis=1)
    out_rows = out_grad.reshape(seqs, length, width)
    out_rows = jnp.concatenate(
        [out_rows[:, mem : mem + seg], out_rows[:, :mem], out_rows[:, mem + seg :]], axis=1
    ).reshape(seqs * length, width)

    def each(function, *arrays):
        results = []
        for s in range(seqs):
            own = slice(s * length, (s + 1) * length)
            spread = jnp.broadcast_to(ids[s][:, None], (length, TILE))
            by_block = ids[s].reshape(length // TILE, TILE)
            results.append(function(spread, by_block, *[a[own] for a in arrays[: len(arrays)]]))
        return results

    query = (product(rows, query_mat) + query_shift.astype(jnp.float32)).astype(jnp.bfloat16)
    keys = product(rows, key_mat).astype(jnp.bfloat16)
    values = (product(rows, value_mat) + value_shift.astype(jnp.float32)).astype(jnp.bfloat16)
    pairs = each(attend, query, keys, values)
    attended_low = jnp.concatenate([pair[0] for pair in pairs], axis=0)
    residual = (
        rows.astype(jnp.float32) + product(attended_low, out_mat) + out_shift.astype(jnp.float32)
    )
    normed, norm_one_pull = jax.vjp(
        layer_norm, residual, gain_one.astype(jnp.float32), shift_one.astype(jnp.float32)
    )
    normed_low = normed.astype(jnp.bfloat16)
    inner = product(normed_low, inner_mat) + inner_shift.astype(jnp.float32)
    active, slope = gelu_and_slope(inner)
    active_low = active.astype(jnp.bfloat16)
    second = normed + product(active_low, outer_mat) + outer_shift.astype(jnp.float32)
    output, norm_two_pull = jax.vjp(
        layer_norm, second, gain_two.astype(jnp.float32), shift_two.astype(jnp.float32)
    )
    grad_second, grad_gain_two, grad_shift_two = norm_two_pull(out_rows.astype(jnp.float32))
    grad_outer_low = grad_second.astype(jnp.bfloat16)
    grad_w_outer = inner_rows(active_low, grad_outer_low)
    grad_outer_bias = column_sum(grad_outer_low)
    grad_inner_low = (against(grad_outer_low, back_outer) * slope).astype(jnp.bfloat16)
    grad_w_inner = inner_rows(normed_low, grad_inner_low)
    grad_inner_bias = column_sum(grad_inner_low)
    grad_normed = grad_second + against(grad_inner_low, back_inner)
    grad_residual, grad_gain_one, grad_shift_one = norm_one_pull(grad_normed)
    grad_branch_low = grad_residual.astype(jnp.bfloat16)
    grad_w_out = inner_rows(attended_low, grad_branch_low)
    grad_out_bias = column_sum(grad_branch_low)
    grad_attended = against(grad_branch_low, back_out).astype(jnp.bfloat16)
    triples = [
        attend_back(spread, by_block, q, k, v, g, pairs[s][1])
        for s, (spread, by_block, q, k, v, g) in enumerate(
            each(lambda *a: a, query, keys, values, grad_attended)
        )
    ]
    grad_query_low, grad_keys_low, grad_values_low = (
        jnp.concatenate([triple[i] for triple in triples], axis=0) for i in range(3)
    )
    grad_w_query = inner_rows(rows, grad_query_low)
    grad_w_key = inner_rows(rows, grad_keys_low)
    grad_w_value = inner_rows(rows, grad_values_low)
    grad_query_bias = column_sum(grad_query_low)
    grad_value_bias = column_sum(grad_values_low)
    grad_rows = (
        grad_residual
        + against(grad_query_low, back_query)
        + against(grad_keys_low, back_key)
        + against(grad_values_low, back_value)
    ).reshape(seqs, length, width)
    grad_tokens = grad_rows[:, :seg].reshape(seqs * seg, width).astype(jnp.bfloat16)
    grad_memory = (
        (grad_rows[:, seg : seg + mem] + grad_rows[:, seg + mem :])
        .reshape(seqs * mem, width)
        .astype(jnp.bfloat16)
    )
    low = jnp.bfloat16
    layer_out = output.astype(low).reshape(seqs, length, width)
    layer_out = jnp.concatenate(
        [layer_out[:, seg : seg + mem], layer_out[:, :seg], layer_out[:, seg + mem :]], axis=1
    ).reshape(seqs * length, width)
    stack_share, inner_share, outer_share, small_share = reduce(
        jnp.stack([grad_w_query, grad_w_key, grad_w_value, grad_w_out]).astype(low),
        grad_w_inner.astype(low).reshape(W, 4, W).transpose(1, 0, 2),
        grad_w_outer.astype(low),
        pack_full(
            (
                grad_query_bias, grad_value_bias, grad_out_bias, grad_gain_one,
                grad_shift_one, grad_outer_bias, grad_gain_two, grad_shift_two, grad_inner_bias,
            ),
            owners,
            part,
        ),
    )
    (
        final_bq, final_bv, final_bo, final_g1, final_n1, final_b2, final_g2, final_n2, final_b1,
    ) = unpack_full(small_share[None], part)
    return (
        layer_out,
        grad_tokens,
        grad_memory,
        stack_share[0],
        stack_share[1],
        stack_share[2],
        stack_share[3],
        final_bq,
        final_bv,
        final_bo,
        final_g1,
        final_n1,
        inner_share.transpose(1, 0, 2).reshape(part, 4 * W),
        final_b1,
        outer_share.reshape(4 * part, W),
        final_b2,
        final_g2,
        final_n2,
    )


def solution(mesh):
    return jax.shard_map(
        on_device,
        mesh=mesh,
        in_specs=(
            P(("rep", "fsdp"), None),
            P(("rep", "fsdp"), None),
            P(("rep", "fsdp"), None),
            P("fsdp", None),
            P("fsdp", None),
            P("fsdp", None),
            P("fsdp", None),
            P("fsdp"),
            P("fsdp"),
            P("fsdp"),
            P("fsdp"),
            P("fsdp"),
            P("fsdp", None),
            P("fsdp"),
            P("fsdp", None),
            P("fsdp"),
            P("fsdp"),
            P("fsdp"),
            P(("rep", "fsdp"), None),
        ),
        out_specs=(
            P(("rep", "fsdp"), None),
            P(("rep", "fsdp"), None),
            P(("rep", "fsdp"), None),
            P("fsdp", None),
            P("fsdp", None),
            P("fsdp", None),
            P("fsdp", None),
            P("fsdp"),
            P("fsdp"),
            P("fsdp"),
            P("fsdp"),
            P("fsdp"),
            P("fsdp", None),
            P("fsdp"),
            P("fsdp", None),
            P("fsdp"),
            P("fsdp"),
            P("fsdp"),
        ),
        check_vma=False,
    )
```

```python
import functools
import math

import jax
import jax.numpy as jnp
from jax import lax
from jax.experimental import pallas as pl
from jax.experimental.pallas import tpu as pltpu
from jax.sharding import PartitionSpec as P

MESH_ID = pl.DeviceIdType.MESH
W = 768


class Copies:
    def __init__(self, send, recv):
        self.send, self.recv, self.made = send, recv, {}

    def start(self, name, src, dst, to):
        slot = len(self.made)
        copy = pltpu.make_async_remote_copy(
            src_ref=src,
            dst_ref=dst,
            send_sem=self.send.at[slot],
            recv_sem=self.recv.at[slot],
            device_id=to,
            device_id_type=MESH_ID,
        )
        copy.start()
        self.made[name] = copy

    def start_either(self, name, core, sources, dst, to):
        slot = len(self.made)

        def describe(src):
            return pltpu.make_async_remote_copy(
                src_ref=src,
                dst_ref=dst,
                send_sem=self.send.at[slot],
                recv_sem=self.recv.at[slot],
                device_id=to,
                device_id_type=MESH_ID,
            )

        for which in (0, 1):

            @pl.when(core == which)
            def _():
                describe(sources[which]).start()

        self.made[name] = describe(dst)

    def arrived(self, name):
        self.made[name].wait_recv()

    def drain(self):
        for copy in self.made.values():
            copy.wait_send()


def place():
    rep, owner = lax.axis_index("rep"), lax.axis_index("fsdp")
    y, c, z, x = rep // 2, rep % 2, owner // 2, owner % 2
    where = {
        "core": (y * 2 + 1 - c, owner),
        "y": ((1 - y) * 2 + c, owner),
        "x": (rep, z * 2 + 1 - x),
    }
    for k in (1, 2, 3):
        where["z", k] = (rep, ((z + k) % 4) * 2 + x)
        where["zx", k] = (rep, ((z + k) % 4) * 2 + 1 - x)
    return rep, owner, y, c, z, x, where


def greet(where):
    barrier = pltpu.get_barrier_semaphore()
    for to in where.values():
        pl.semaphore_signal(barrier, inc=1, device_id=to, device_id_type=MESH_ID)
    pl.semaphore_wait(barrier, len(where))


def gather_kernel(
    wq, wk, wv, wo, w1, w2, vec, o0, o1, o2, ov, a0, a1, a2, av, send, recv, own_sem, load_sem
):
    rep, owner, y, c, z, x, where = place()
    part = W // 8
    sources = (wq, wk, wv, wo, w1, w2, vec)
    shards = (a0.at[0], a0.at[1], a0.at[2], a0.at[3], a1, a2, av)
    loads = [
        pltpu.make_async_copy(source, shard, load_sem.at[i])
        for i, (source, shard) in enumerate(zip(sources, shards))
    ]
    for load in loads:
        load.start()

    def in0(k, other_x):
        z_of, x_of = (z - k + 4) % 4, (1 - x if other_x else x)
        return o0.at[pl.ds(c * 2, 2), pl.ds((z_of * 2 + x_of) * part, part), :]

    def in1(k, other_x, quarter):
        z_of, x_of = (z - k + 4) % 4, (1 - x if other_x else x)
        return o1.at[quarter, pl.ds((z_of * 2 + x_of) * part, part), :]

    def in2(k, other_x, quarter):
        z_of, x_of = (z - k + 4) % 4, (1 - x if other_x else x)
        return o2.at[pl.ds((z_of * 2 + x_of) * 4 * part + quarter * part, part), :]

    mine, across = rep, (1 - y) * 2 + c
    greet(where)
    for load in loads:
        load.wait()
    own = [
        pltpu.make_async_copy(a0, o0.at[:, pl.ds(owner * part, part), :], own_sem.at[0]),
        pltpu.make_async_copy(a2, o2.at[pl.ds(owner * 4 * part, 4 * part), :], own_sem.at[1]),
        pltpu.make_async_copy(av, ov.at[owner], own_sem.at[2]),
    ]
    for r in range(4):
        own.append(
            pltpu.make_async_copy(
                a1.at[:, r * W : (r + 1) * W],
                o1.at[r, pl.ds(owner * part, part), :],
                own_sem.at[3 + r],
            )
        )
    copies = Copies(send, recv)
    from0 = a0.at[pl.ds(c * 2, 2), :, :]
    from1 = a1.at[:, pl.ds(pl.multiple_of(rep * W, W), W)]
    from2 = a2.at[pl.ds(rep * part, part), :]
    for k in (1, 3, 2):
        copies.start((1, "z", k), from1, in1(0, False, mine), where["z", k])
        copies.start((2, "z", k), from2, in2(0, False, mine), where["z", k])
        copies.start((0, "z", k), from0, in0(0, False), where["z", k])
    copies.start((1, "x", 0), from1, in1(0, False, mine), where["x"])
    copies.start((2, "x", 0), from2, in2(0, False, mine), where["x"])
    copies.start((0, "x", 0), from0, in0(0, False), where["x"])
    for k in (1, 2, 3):
        copies.start(("v", "z", k), av, ov.at[owner], where["z", k])
        copies.start(("v", "zx", k), av, ov.at[owner], where["zx", k])
    copies.start(("v", "x", 0), av, ov.at[owner], where["x"])
    for copy in own:
        copy.start()

    def pass_on(k, other_x, stage):
        for g in (1, 2, 0):
            copies.arrived((g, stage, k))
            here = (
                in0(k, other_x)
                if g == 0
                else in1(k, other_x, mine) if g == 1 else in2(k, other_x, mine)
            )
            if stage == "z":
                copies.start((g, "x", k), here, here, where["x"])
            if g > 0:
                copies.start((g, "y", k, other_x), here, here, where["y"])
            copies.start((g, "core", k, other_x), here, here, where["core"])

    order = [(0, True, "x"), (1, False, "z"), (3, False, "z"), (1, True, "x"), (2, False, "z")]
    order += [(3, True, "x"), (2, True, "x")]
    for step in order:
        pass_on(*step)
    for k, other_x, _ in order:
        for g in (1, 2):
            copies.arrived((g, "y", k, other_x))
            here = in1(k, other_x, across) if g == 1 else in2(k, other_x, across)
            copies.start((g, "diagonal", k, other_x), here, here, where["core"])
    for k, other_x, _ in order:
        for g in (0, 1, 2):
            copies.arrived((g, "core", k, other_x))
        for g in (1, 2):
            copies.arrived((g, "diagonal", k, other_x))
    for k in (1, 2, 3):
        copies.arrived(("v", "z", k))
        copies.arrived(("v", "zx", k))
    copies.arrived(("v", "x", 0))
    copies.drain()
    for copy in own:
        copy.wait()


GATHER_COPIES = 3 * 3 + 3 + 7 + (3 * 3 + 2 * 7 + 3 * 7 + 2 * 7)


def gather_all(wq, wk, wv, wo, inner, outer, vectors):
    low = jnp.bfloat16
    anywhere = pl.BlockSpec(memory_space=pl.ANY)
    return pl.pallas_call(
        gather_kernel,
        out_shape=(
            jax.ShapeDtypeStruct((4, W, W), low),
            jax.ShapeDtypeStruct((4, W, W), low),
            jax.ShapeDtypeStruct((4 * W, W), low),
            jax.ShapeDtypeStruct((8,) + vectors.shape, vectors.dtype),
        ),
        in_specs=[anywhere] * 7,
        out_specs=[anywhere] * 4,
        scratch_shapes=[
            pltpu.VMEM((4, W // 8, W), low),
            pltpu.VMEM(inner.shape, low),
            pltpu.VMEM(outer.shape, low),
            pltpu.VMEM(vectors.shape, low),
            pltpu.SemaphoreType.DMA((GATHER_COPIES,)),
            pltpu.SemaphoreType.DMA((GATHER_COPIES,)),
            pltpu.SemaphoreType.DMA((7,)),
            pltpu.SemaphoreType.DMA((7,)),
        ],
        compiler_params=pltpu.CompilerParams(collective_id=0, has_side_effects=True),
        name="gather_weights",
    )(wq, wk, wv, wo, inner, outer, vectors)


def total(*refs):
    value = refs[0][...].astype(jnp.float32)
    for ref in refs[1:]:
        value = value + ref[...].astype(jnp.float32)
    return value


def reduce_kernel(
    gq, gk, gw, go, g1, g2, gv, rq, rk, rw, ro, r1, r2, rv,
    k0, c0, x0, z0, e0, k1, c1, y1, x1, z1, e1, got, vec, send, recv, own_sem, out_sem,
):
    rep, owner, y, c, z, x, where = place()
    part = W // 8
    low = jnp.bfloat16
    flat = [(k, o) for o in (1, 0) for k in (1, 3, 2, 0)]
    slot = {pair: i for i, pair in enumerate(flat)}

    def shard(k, o):
        return ((z + k) % 4) * 2 + (1 - x if o else x)

    def part0(grad, k, o):
        return grad.at[pl.ds(shard(k, o) * part, part), :]

    def part1(quarter, k, o):
        columns = pl.ds(pl.multiple_of(quarter * W, W), W)
        return g1.at[pl.ds(shard(k, o) * part, part), columns]

    def part2(quarter, k, o):
        return g2.at[pl.ds(shard(k, o) * 4 * part + quarter * part, part), :]

    pieces = {1: part1, 2: part2}
    greet(where)
    copies = Copies(send, recv)
    own = {}

    def load(name, src, dst):
        copy = pltpu.make_async_copy(src, dst, own_sem.at[len(own)])
        copy.start()
        own[name] = copy

    def load_either(name, sources, dst):
        turn = own_sem.at[len(own)]
        for which in (0, 1):

            @pl.when(c == which)
            def _():
                pltpu.make_async_copy(sources[which], dst, turn).start()

        own[name] = pltpu.make_async_copy(sources[0], dst, turn)

    for side in (1, 0):
        quarter_row = (1 - y) if side else y
        for pair in flat:
            i = slot[pair]
            for g in (1, 2):
                piece = pieces[g]
                copies.start(
                    (g, "core", side, i), piece(quarter_row * 2 + 1 - c, *pair),
                    c1.at[g - 1, side, i], where["core"],
                )
                load((g, side, i), piece(quarter_row * 2 + c, *pair), k1.at[g - 1, side, i])
            if side:
                for j in range(2):
                    near = [part0(grad, *pair) for grad in ((gq, gw), (gk, go))[j]]
                    copies.start_either(
                        (0, "core", j, i), c, near[::-1], c0.at[i, j], where["core"]
                    )
                    load_either((0, j, i), near, k0.at[i, j])
    for k in (1, 2, 3):
        copies.start(("v", "z", k), gv.at[shard(k, 0)], got.at[k], where["z", k])
        copies.start(("v", "zx", k), gv.at[shard(k, 1)], got.at[3 + k], where["zx", k])
    copies.start(("v", "x", 0), gv.at[shard(0, 1)], got.at[7], where["x"])

    def ready(g, *rest):
        for name in [(0,) + rest, (1,) + rest] if g == 0 else [rest]:
            own[(g,) + name].wait()
            copies.arrived((g, "core") + name)

    for pair in flat:
        i = slot[pair]
        for g in (1, 2):
            ready(g, 1, i)
            k1[g - 1, 1, i] = total(k1.at[g - 1, 1, i], c1.at[g - 1, 1, i]).astype(low)
            copies.start((g, "y", i), k1.at[g - 1, 1, i], y1.at[g - 1, i], where["y"])
        if pair[1] == 1:
            ready(0, i)
            k0[i] = total(k0.at[i], c0.at[i]).astype(low)
            copies.start((0, "x", i), k0.at[i], x0.at[i], where["x"])
    for pair in flat:
        k, o = pair
        i = slot[pair]
        j = slot[k, 1]
        if o == 1:
            for g in (1, 2):
                ready(g, 0, i)
                copies.arrived((g, "y", i))
                k1[g - 1, 0, i] = total(
                    k1.at[g - 1, 0, i], c1.at[g - 1, 0, i], y1.at[g - 1, i]
                ).astype(low)
                copies.start((g, "x", i), k1.at[g - 1, 0, i], x1.at[g - 1, i], where["x"])
        elif k > 0:
            ready(0, i)
            copies.arrived((0, "x", j))
            k0[i] = total(k0.at[i], c0.at[i], x0.at[j]).astype(low)
            copies.start((0, "z", k), k0.at[i], z0.at[k - 1], where["z", k])
            for g in (1, 2):
                ready(g, 0, i)
                copies.arrived((g, "y", i))
                copies.arrived((g, "x", j))
                k1[g - 1, 0, i] = total(
                    k1.at[g - 1, 0, i], c1.at[g - 1, 0, i], y1.at[g - 1, i], x1.at[g - 1, j]
                ).astype(low)
                copies.start((g, "z", k), k1.at[g - 1, 0, i], z1.at[g - 1, k - 1], where["z", k])
    for k in (1, 2, 3):
        copies.arrived(("v", "z", k))
        copies.arrived(("v", "zx", k))
    copies.arrived(("v", "x", 0))
    load("v", gv.at[owner], got.at[0])
    own["v"].wait()
    value = got[0]
    for i in range(1, 8):
        value = value + got[i]
    vec[0] = value
    copies.start(("v", "core"), vec.at[0], vec.at[1], where["core"])
    i, j = slot[0, 0], slot[0, 1]
    ready(0, i)
    copies.arrived((0, "x", j))
    for k in (1, 2, 3):
        copies.arrived((0, "z", k))
    e0[0] = total(k0.at[i], c0.at[i], x0.at[j], z0.at[0], z0.at[1], z0.at[2]).astype(low)
    copies.start((0, "y"), e0.at[0], e0.at[1], where["y"])
    for g in (1, 2):
        ready(g, 0, i)
        copies.arrived((g, "y", i))
        copies.arrived((g, "x", j))
        for k in (1, 2, 3):
            copies.arrived((g, "z", k))
        e1[g - 1, 0] = total(
            k1.at[g - 1, 0, i], c1.at[g - 1, 0, i], y1.at[g - 1, i], x1.at[g - 1, j],
            z1.at[g - 1, 0], z1.at[g - 1, 1], z1.at[g - 1, 2],
        ).astype(low)
        copies.start((g, "ey"), e1.at[g - 1, 0], e1.at[g - 1, 1], where["y"])
        copies.start((g, "ecore"), e1.at[g - 1, 0], e1.at[g - 1, 2], where["core"])
    copies.arrived(("v", "core"))
    vec[2] = vec[0] + vec[1]
    copies.start(("v", "y"), vec.at[2], vec.at[3], where["y"])
    copies.arrived((0, "y"))
    e0[2] = total(e0.at[0], e0.at[1]).astype(low)
    copies.start((0, "ecore"), e0.at[2], e0.at[3], where["core"])
    for g in (1, 2):
        copies.arrived((g, "ey"))
        copies.start((g, "ediagonal"), e1.at[g - 1, 1], e1.at[g - 1, 3], where["core"])
    for core in (0, 1):

        @pl.when(c == core)
        def _():
            for j, ref in enumerate(((rq, rk), (rw, ro))[core]):
                ref[...] = e0[2, j].astype(jnp.float32)

    outs = (rep, (1 - y) * 2 + c, y * 2 + 1 - c, (1 - y) * 2 + 1 - c)

    def put(g, i):
        value = e1[g - 1, i].astype(jnp.float32)
        if g == 1:
            r1[:, pl.ds(pl.multiple_of(outs[i] * W, W), W)] = value
        else:
            r2[pl.ds(outs[i] * part, part), :] = value

    for g in (1, 2):
        put(g, 0)
        put(g, 1)
        copies.arrived((g, "ecore"))
        put(g, 2)
    copies.arrived(("v", "y"))
    rv[...] = vec[2] + vec[3]
    copies.arrived((0, "ecore"))
    for core in (0, 1):

        @pl.when(c == core)
        def _():
            for j, ref in enumerate(((rw, ro), (rq, rk))[core]):
                ref[...] = e0[3, j].astype(jnp.float32)

    for g in (1, 2):
        copies.arrived((g, "ediagonal"))
        put(g, 3)
    copies.drain()


REDUCE_COPIES = 2 * 16 + 16 + 7 + 16 + 4 + 8 + 9 + 1 + 1 + 4 + 1 + 1 + 2


def reduce_all(gq, gk, gw, go, inner, outer, vectors):
    low, full = jnp.bfloat16, jnp.float32
    part = W // 8
    anywhere, near = pl.BlockSpec(memory_space=pl.ANY), pl.BlockSpec(memory_space=pltpu.VMEM)
    return pl.pallas_call(
        reduce_kernel,
        out_shape=(
            jax.ShapeDtypeStruct((part, W), full),
            jax.ShapeDtypeStruct((part, W), full),
            jax.ShapeDtypeStruct((part, W), full),
            jax.ShapeDtypeStruct((part, W), full),
            jax.ShapeDtypeStruct((part, 4 * W), full),
            jax.ShapeDtypeStruct((4 * part, W), full),
            jax.ShapeDtypeStruct(vectors.shape[1:], full),
        ),
        in_specs=[anywhere] * 7,
        out_specs=[near] * 7,
        scratch_shapes=[
            pltpu.VMEM((8, 2, part, W), low),
            pltpu.VMEM((8, 2, part, W), low),
            pltpu.VMEM((4, 2, part, W), low),
            pltpu.VMEM((3, 2, part, W), low),
            pltpu.VMEM((4, 2, part, W), low),
            pltpu.VMEM((2, 2, 8, part, W), low),
            pltpu.VMEM((2, 2, 8, part, W), low),
            pltpu.VMEM((2, 8, part, W), low),
            pltpu.VMEM((2, 4, part, W), low),
            pltpu.VMEM((2, 3, part, W), low),
            pltpu.VMEM((2, 4, part, W), low),
            pltpu.VMEM(vectors.shape, full),
            pltpu.VMEM((4,) + vectors.shape[1:], full),
            pltpu.SemaphoreType.DMA((REDUCE_COPIES,)),
            pltpu.SemaphoreType.DMA((REDUCE_COPIES,)),
            pltpu.SemaphoreType.DMA((2 * 16 + 16 + 1,)),
            pltpu.SemaphoreType.DMA((1,)),
        ],
        compiler_params=pltpu.CompilerParams(
            collective_id=1, has_side_effects=True, vmem_limit_bytes=56 << 20
        ),
        name="reduce_gradients",
    )(gq, gk, gw, go, inner, outer, vectors)


def inner_lines(part):
    return -(-4 * part // 128)


def pack(vectors, inner):
    owners, _, part = vectors.shape
    lines = inner_lines(part)
    first = jnp.pad(vectors, ((0, 0), (0, 0), (0, 128 - part)))
    second = jnp.pad(inner, ((0, 0), (0, lines * 128 - 4 * part)))
    second = second.reshape(owners, lines, 128)
    return jnp.pad(jnp.concatenate([first, second], axis=1), ((0, 0), (0, 8 - lines), (0, 0)))


def unpack(packed, part):
    owners = packed.shape[0]
    lines = inner_lines(part)
    first = packed[:, :8, :part].transpose(1, 0, 2).reshape(8, owners * part)
    second = packed[:, 8 : 8 + lines].reshape(owners, lines * 128)[:, : 4 * part]
    return first, second.reshape(4, owners * part)


def plain_gather(wq, wk, wv, wo, inner, outer, vectors):
    gathered = lax.all_gather(inner, "fsdp", axis=0, tiled=True)
    return (
        lax.all_gather(jnp.stack([wq, wk, wv, wo]), "fsdp", axis=1, tiled=True),
        gathered.reshape(W, 4, W).transpose(1, 0, 2),
        lax.all_gather(outer, "fsdp", axis=0, tiled=True),
        lax.all_gather(vectors, "fsdp", axis=0),
    )


def plain_reduce(*grads):
    def over_all(value):
        part = lax.psum_scatter(value, "fsdp", scatter_dimension=0, tiled=True)
        return lax.psum(part, "rep").astype(jnp.float32)

    return tuple(over_all(grad) for grad in grads[:-1]) + (over_all(grads[-1])[0],)


def product(left, right):
    return jnp.dot(left, right, preferred_element_type=jnp.float32)


def inner_rows(left, right):
    return lax.dot_general(
        left, right, (((0,), (0,)), ((), ())), preferred_element_type=jnp.float32
    )


def against(left, right):
    return lax.dot_general(
        left, right, (((1,), (1,)), ((), ())), preferred_element_type=jnp.float32
    )


def column_sum(values):
    return jnp.sum(values.astype(jnp.float32), axis=0)


TILE = 128
HEAD_DIM = 64
FACTOR = HEAD_DIM ** (-0.5)
HIDDEN = -1e30


def spans(i, count):
    last = count - 1
    if i == last:
        return [(0, count * TILE)]
    low, high = max(0, i - 2), min(last, i + 2)
    if high == last:
        return [(low * TILE, count * TILE)]
    return [(low * TILE, (high + 1) * TILE), (last * TILE, count * TILE)]


def two_heads(block):
    lanes = lax.broadcasted_iota(jnp.int32, block.shape, 1)
    zero = jnp.zeros_like(block)
    first = jnp.where(lanes < HEAD_DIM, block, zero)
    second = jnp.where(lanes < HEAD_DIM, zero, block)
    return jnp.concatenate([first, second], axis=0)


def own_head(value):
    rows = lax.broadcasted_iota(jnp.int32, (TILE, TILE), 0)
    return jnp.where(rows < HEAD_DIM, value[:, :TILE], value[:, TILE:]).T


def masked_scores(k_ref, key_ids, query_ids, stacked, i, span, count):
    low, high = span
    scores = against(k_ref[low:high, :], stacked)
    ids = key_ids[low:high, :]
    row = query_ids[i : i + 1, :]
    seen = ids == row
    if high == count * TILE:
        seen = seen | (ids < 0)
    if i == count - 1:
        seen = seen | (row < 0)
    return jnp.concatenate(
        [jnp.where(seen, scores[:, :TILE], HIDDEN), jnp.where(seen, scores[:, TILE:], HIDDEN)], axis=1
    )


def attend_kernel(key_ids, query_ids, q_ref, k_ref, v_ref, out_ref, lse_ref, v_turned):
    count = q_ref.shape[0] // TILE
    v_turned[...] = v_ref[...].T
    for i in range(count):
        rows = slice(i * TILE, (i + 1) * TILE)
        stacked = two_heads(q_ref[rows, :] * jnp.bfloat16(FACTOR))
        parts = spans(i, count)
        scores = [masked_scores(k_ref, key_ids, query_ids, stacked, i, p, count) for p in parts]
        peak = functools.reduce(
            jnp.maximum, [jnp.max(s, axis=0, keepdims=True) for s in scores]
        )
        weights = [jnp.exp(s - peak) for s in scores]
        total = sum(jnp.sum(w, axis=0, keepdims=True) for w in weights)
        mixed = sum(
            product(v_turned[:, low:high], w.astype(jnp.bfloat16)) for (low, high), w in zip(parts, weights)
        )
        out_ref[rows, :] = own_head(mixed * (1.0 / total)).astype(jnp.bfloat16)
        lse_ref[0, i : i + 1, :] = peak + jnp.log(total)


def attend_back_kernel(
    key_ids, query_ids, q_ref, k_ref, v_ref, g_ref, lse_ref, gq_ref, gk_ref, gv_ref,
    k_turned, k_total, v_total,
):
    count = q_ref.shape[0] // TILE
    k_turned[...] = k_ref[...].T
    k_total[...] = jnp.zeros_like(k_total)
    v_total[...] = jnp.zeros_like(v_total)
    for i in range(count):
        rows = slice(i * TILE, (i + 1) * TILE)
        stacked = two_heads(q_ref[rows, :] * jnp.bfloat16(FACTOR))
        grads = two_heads(g_ref[rows, :])
        lse = lse_ref[0, i : i + 1, :]
        parts = spans(i, count)
        probs, pulls = [], []
        for low, high in parts:
            scores = masked_scores(k_ref, key_ids, query_ids, stacked, i, (low, high), count)
            p = jnp.exp(scores - lse)
            v_total[low:high, :] += product(p.astype(jnp.bfloat16), grads)
            probs.append(p)
            pulls.append(against(v_ref[low:high, :], grads))
        centre = sum(jnp.sum(p * g, axis=0, keepdims=True) for p, g in zip(probs, pulls))
        mixed = 0.0
        for (low, high), p, g in zip(parts, probs, pulls):
            turned = (p * (g - centre)).astype(jnp.bfloat16)
            k_total[low:high, :] += product(turned, stacked)
            mixed = mixed + product(k_turned[:, low:high], turned)
        gq_ref[rows, :] = (own_head(mixed) * FACTOR).astype(jnp.bfloat16)
    gk_ref[...] = k_total[...].astype(jnp.bfloat16)
    gv_ref[...] = v_total[...].astype(jnp.bfloat16)


def attend(key_ids, query_ids, query, keys, values):
    rows, width = query.shape
    pair = 2 * HEAD_DIM
    count = rows // TILE
    column = pl.BlockSpec((rows, pair), lambda h: (0, h))
    whole = lambda a: pl.BlockSpec(a.shape, lambda h: (0, 0))
    return pl.pallas_call(
        attend_kernel,
        grid=(width // pair,),
        out_shape=(
            jax.ShapeDtypeStruct((rows, width), jnp.bfloat16),
            jax.ShapeDtypeStruct((width // pair, count, 2 * TILE), jnp.float32),
        ),
        in_specs=[whole(key_ids), whole(query_ids), column, column, column],
        out_specs=[column, pl.BlockSpec((1, count, 2 * TILE), lambda h: (h, 0, 0))],
        scratch_shapes=[pltpu.VMEM((pair, rows), jnp.bfloat16)],
        compiler_params=pltpu.CompilerParams(vmem_limit_bytes=48 << 20),
        name="attend",
    )(key_ids, query_ids, query, keys, values)


def attend_back(key_ids, query_ids, query, keys, values, grads, lse):
    rows, width = query.shape
    pair = 2 * HEAD_DIM
    count = rows // TILE
    column = pl.BlockSpec((rows, pair), lambda h: (0, h))
    whole = lambda a: pl.BlockSpec(a.shape, lambda h: (0, 0))
    return pl.pallas_call(
        attend_back_kernel,
        grid=(width // pair,),
        out_shape=(jax.ShapeDtypeStruct((rows, width), jnp.bfloat16),) * 3,
        in_specs=[whole(key_ids), whole(query_ids)]
        + [column] * 4
        + [pl.BlockSpec((1, count, 2 * TILE), lambda h: (h, 0, 0))],
        out_specs=[column] * 3,
        scratch_shapes=[
            pltpu.VMEM((pair, rows), jnp.bfloat16),
            pltpu.VMEM((rows, pair), jnp.float32),
            pltpu.VMEM((rows, pair), jnp.float32),
        ],
        compiler_params=pltpu.CompilerParams(vmem_limit_bytes=48 << 20),
        name="attend_back",
    )(key_ids, query_ids, query, keys, values, grads, lse)


ERFC_TERMS = (
    -1.26551223, 1.00002368, 0.37409196, 0.09678418, -0.18628806,
    0.27886807, -1.13520398, 1.48851587, -0.82215223, 0.17087277,
)


def gelu_and_slope(value):
    half_square = value * value * 0.5
    step = 1.0 / (1.0 + jnp.abs(value) * (0.5 * 0.5**0.5))
    power = ERFC_TERMS[-1]
    for term in ERFC_TERMS[-2::-1]:
        power = power * step + term
    tail = 0.5 * step * jnp.exp(power - half_square)
    cover = jnp.where(value < 0, tail, 1.0 - tail)
    density = jnp.exp(-half_square) * ((0.5 / math.pi) ** 0.5)
    return value * cover, cover + value * density


def normalise(value):
    mean = jnp.mean(value, axis=1, keepdims=True)
    centred = value - mean
    scale = lax.rsqrt(jnp.mean(centred * centred, axis=1, keepdims=True) + 1e-05)
    return centred * scale, scale


def normalise_back(grad, unit, scale):
    middle = jnp.mean(grad, axis=1, keepdims=True)
    along = jnp.mean(grad * unit, axis=1, keepdims=True)
    return scale * (grad - middle - unit * along)


def chain_kernel(
    mixed_ref, rows_ref, pull_ref, wo_ref, w1_ref, w2_ref, small_ref, b1_ref,
    out_ref, y1_ref, u_ref, gz_ref, gf_ref, gh_ref, ga_ref, gmix_ref, sums_ref, b1_sum_ref,
    slope_ref,
):
    low = jnp.bfloat16

    @pl.when(pl.program_id(0) == 0)
    def _():
        sums_ref[...] = jnp.zeros_like(sums_ref)
        b1_sum_ref[...] = jnp.zeros_like(b1_sum_ref)

    def small(i):
        return small_ref[i : i + 1, :]

    def gather_sum(ref, i, value):
        ref[i : i + 1, :] += jnp.sum(value, axis=0, keepdims=True)

    hidden = rows_ref[...].astype(jnp.float32) + product(mixed_ref[...], wo_ref[0]) + small(2)
    unit_one, scale_one = normalise(hidden)
    y1 = unit_one * small(3) + small(4)
    y1_low = y1.astype(low)
    y1_ref[...] = y1_low
    second = y1 + small(5)
    for r in range(4):
        inner = product(y1_low, w1_ref[r]) + b1_ref[r : r + 1, :]
        active, slope = gelu_and_slope(inner)
        active = active.astype(low)
        u_ref[:, r * W : (r + 1) * W] = active
        slope_ref[:, r * W : (r + 1) * W] = slope
        second = second + product(active, w2_ref[r * W : (r + 1) * W, :])
    unit_two, scale_two = normalise(second)
    out_ref[...] = (unit_two * small(6) + small(7)).astype(low)
    pull = pull_ref[...].astype(jnp.float32)
    gather_sum(sums_ref, 6, pull * unit_two)
    gather_sum(sums_ref, 7, pull)
    grad_second = normalise_back(pull * small(6), unit_two, scale_two)
    gz = grad_second.astype(low)
    gz_ref[...] = gz
    gather_sum(sums_ref, 5, gz.astype(jnp.float32))
    grad_y1 = grad_second
    for r in range(4):
        gf = against(gz, w2_ref[r * W : (r + 1) * W, :]) * slope_ref[:, r * W : (r + 1) * W]
        gf = gf.astype(low)
        gf_ref[:, r * W : (r + 1) * W] = gf
        gather_sum(b1_sum_ref, r, gf.astype(jnp.float32))
        grad_y1 = grad_y1 + against(gf, w1_ref[r])
    gather_sum(sums_ref, 3, grad_y1 * unit_one)
    gather_sum(sums_ref, 4, grad_y1)
    grad_hidden = normalise_back(grad_y1 * small(3), unit_one, scale_one)
    gh_ref[...] = grad_hidden
    ga = grad_hidden.astype(low)
    ga_ref[...] = ga
    gather_sum(sums_ref, 2, ga.astype(jnp.float32))
    gmix_ref[...] = against(ga, wo_ref[0]).astype(low)


def chain(mixed, rows, pull, weights, inner_blocks, outer_mat, small, inner_bias):
    count, width = rows.shape
    step = 256
    low, full = jnp.bfloat16, jnp.float32
    thin = pl.BlockSpec((step, width), lambda i: (i, 0))
    fat = pl.BlockSpec((step, 4 * width), lambda i: (i, 0))
    held = lambda shape: pl.BlockSpec(shape, lambda i: (0,) * len(shape))
    once = pl.Buffered(1)
    return pl.pallas_call(
        chain_kernel,
        grid=(count // step,),
        out_shape=(
            jax.ShapeDtypeStruct((count, width), low),
            jax.ShapeDtypeStruct((count, width), low),
            jax.ShapeDtypeStruct((count, 4 * width), low),
            jax.ShapeDtypeStruct((count, width), low),
            jax.ShapeDtypeStruct((count, 4 * width), low),
            jax.ShapeDtypeStruct((count, width), full),
            jax.ShapeDtypeStruct((count, width), low),
            jax.ShapeDtypeStruct((count, width), low),
            jax.ShapeDtypeStruct((8, width), full),
            jax.ShapeDtypeStruct((4, width), full),
        ),
        in_specs=[
            thin, thin, thin,
            pl.BlockSpec((1, width, width), lambda i: (3, 0, 0), pipeline_mode=once),
            pl.BlockSpec((4, width, width), lambda i: (0, 0, 0), pipeline_mode=once),
            pl.BlockSpec((4 * width, width), lambda i: (0, 0), pipeline_mode=once),
            held((8, width)), held((4, width)),
        ],
        out_specs=[thin, thin, fat, thin, fat, thin, thin, thin, held((8, width)), held((4, width))],
        scratch_shapes=[pltpu.VMEM((step, 4 * width), full)],
        compiler_params=pltpu.CompilerParams(vmem_limit_bytes=60 << 20),
        name="chain",
    )(mixed, rows, pull, weights, inner_blocks, outer_mat, small, inner_bias)


def on_device(
    tokens,
    read_memory,
    doc_ids,
    w_query,
    w_key,
    w_value,
    w_out,
    query_bias,
    value_bias,
    out_bias,
    norm_one_gain,
    norm_one_bias,
    w_inner,
    inner_bias,
    w_outer,
    outer_bias,
    norm_two_gain,
    norm_two_bias,
    out_grad,
):
    owners = lax.axis_size("fsdp")
    wide = owners == 8 and lax.axis_size("rep") == 4
    part = w_query.shape[0]
    low = jnp.bfloat16
    small = pack(
        jnp.stack(
            [
                query_bias, value_bias, out_bias, norm_one_gain,
                norm_one_bias, outer_bias, norm_two_gain, norm_two_bias,
            ]
        )[None],
        inner_bias[None],
    )[0]
    gather, reduce = (gather_all, reduce_all) if wide else (plain_gather, plain_reduce)
    weights, inner_blocks, outer_mat, packed = gather(
        w_query, w_key, w_value, w_out, w_inner, w_outer, small
    )
    vectors, inner_shift = unpack(packed.astype(jnp.float32), part)
    seqs, seg = doc_ids.shape
    width = tokens.shape[1]
    mem = read_memory.shape[0] // seqs
    length = seg + 2 * mem
    memory_rows = read_memory.reshape(seqs, mem, width)
    rows = jnp.concatenate([tokens.reshape(seqs, seg, width), memory_rows, memory_rows], axis=1)
    rows = rows.reshape(seqs * length, width)
    marks = jnp.full((seqs, 2 * mem), -1, jnp.int32)
    ids = jnp.concatenate([doc_ids, marks], axis=1)
    out_rows = out_grad.reshape(seqs, length, width)
    out_rows = jnp.concatenate(
        [out_rows[:, mem : mem + seg], out_rows[:, :mem], out_rows[:, mem + seg :]], axis=1
    ).reshape(seqs * length, width)

    def each(function, *arrays):
        results = []
        for s in range(seqs):
            own = slice(s * length, (s + 1) * length)
            spread = jnp.broadcast_to(ids[s][:, None], (length, TILE))
            by_block = ids[s].reshape(length // TILE, TILE)
            results.append(function(spread, by_block, *[a[own] for a in arrays]))
        return results

    query = (product(rows, weights[0]) + vectors[0]).astype(low)
    keys = product(rows, weights[1]).astype(low)
    values = (product(rows, weights[2]) + vectors[1]).astype(low)
    pairs = each(attend, query, keys, values)
    mixed = jnp.concatenate([pair[0] for pair in pairs], axis=0)
    output, normed, active, grad_outer, grad_inner, grad_residual, grad_branch, grad_mixed, sums, inner_sums = chain(
        mixed, rows, out_rows, weights, inner_blocks, outer_mat, vectors, inner_shift
    )
    grad_w_outer = inner_rows(active, grad_outer).astype(low)
    grad_w_inner = inner_rows(normed, grad_inner).astype(low)
    grad_w_out = inner_rows(mixed, grad_branch).astype(low)
    triples = [
        attend_back(spread, by_block, q, k, v, g, pairs[s][1])
        for s, (spread, by_block, q, k, v, g) in enumerate(
            each(lambda *a: a, query, keys, values, grad_mixed)
        )
    ]
    grad_query_low, grad_keys_low, grad_values_low = (
        jnp.concatenate([triple[i] for triple in triples], axis=0) for i in range(3)
    )
    grad_w_query = inner_rows(rows, grad_query_low).astype(low)
    grad_w_key = inner_rows(rows, grad_keys_low).astype(low)
    grad_w_value = inner_rows(rows, grad_values_low).astype(low)
    sums = jnp.concatenate(
        [column_sum(grad_query_low)[None], column_sum(grad_values_low)[None], sums[2:]], axis=0
    )
    grad_rows = (
        grad_residual
        + against(grad_query_low, weights[0])
        + against(grad_keys_low, weights[1])
        + against(grad_values_low, weights[2])
    ).reshape(seqs, length, width)
    grad_tokens = grad_rows[:, :seg].reshape(seqs * seg, width).astype(jnp.bfloat16)
    grad_memory = (
        (grad_rows[:, seg : seg + mem] + grad_rows[:, seg + mem :])
        .reshape(seqs * mem, width)
        .astype(jnp.bfloat16)
    )
    layer_out = output.reshape(seqs, length, width)
    layer_out = jnp.concatenate(
        [layer_out[:, seg : seg + mem], layer_out[:, :seg], layer_out[:, seg + mem :]], axis=1
    ).reshape(seqs * length, width)
    share_wq, share_wk, share_wv, share_wo, share_inner, share_outer, share_small = reduce(
        grad_w_query,
        grad_w_key,
        grad_w_value,
        grad_w_out,
        grad_w_inner,
        grad_w_outer,
        pack(
            sums.reshape(8, owners, part).transpose(1, 0, 2),
            inner_sums.reshape(owners, 4 * part),
        ),
    )
    last, last_inner = unpack(share_small[None], part)
    return (
        layer_out,
        grad_tokens,
        grad_memory,
        share_wq,
        share_wk,
        share_wv,
        share_wo,
        *(last[i] for i in range(5)),
        share_inner,
        last_inner.reshape(-1),
        share_outer,
        *(last[i] for i in range(5, 8)),
    )


def solution(mesh):
    return jax.shard_map(
        on_device,
        mesh=mesh,
        in_specs=(
            P(("rep", "fsdp"), None),
            P(("rep", "fsdp"), None),
            P(("rep", "fsdp"), None),
            P("fsdp", None),
            P("fsdp", None),
            P("fsdp", None),
            P("fsdp", None),
            P("fsdp"),
            P("fsdp"),
            P("fsdp"),
            P("fsdp"),
            P("fsdp"),
            P("fsdp", None),
            P("fsdp"),
            P("fsdp", None),
            P("fsdp"),
            P("fsdp"),
            P("fsdp"),
            P(("rep", "fsdp"), None),
        ),
        out_specs=(
            P(("rep", "fsdp"), None),
            P(("rep", "fsdp"), None),
            P(("rep", "fsdp"), None),
            P("fsdp", None),
            P("fsdp", None),
            P("fsdp", None),
            P("fsdp", None),
            P("fsdp"),
            P("fsdp"),
            P("fsdp"),
            P("fsdp"),
            P("fsdp"),
            P("fsdp", None),
            P("fsdp"),
            P("fsdp", None),
            P("fsdp"),
            P("fsdp"),
            P("fsdp"),
        ),
        check_vma=False,
    )
```

```python
import functools
import math

import jax
import jax.numpy as jnp
from jax import lax
from jax.experimental import pallas as pl
from jax.experimental.pallas import tpu as pltpu
from jax.sharding import PartitionSpec as P

MESH_ID = pl.DeviceIdType.MESH
W = 768


class Copies:
    def __init__(self, send, recv):
        self.send, self.recv, self.made = send, recv, {}

    def plan(self, name, src, dst, to):
        slot = len(self.made)

        def describe(src):
            return pltpu.make_async_remote_copy(
                src_ref=src,
                dst_ref=dst,
                send_sem=self.send.at[slot],
                recv_sem=self.recv.at[slot],
                device_id=to,
                device_id_type=MESH_ID,
            )

        self.made[name] = (describe, src)

    def go(self, name):
        describe, src = self.made[name]
        describe(src).start()

    def start(self, name, src, dst, to):
        self.plan(name, src, dst, to)
        self.go(name)

    def start_either(self, name, core, sources, dst, to):
        self.plan(name, dst, dst, to)
        describe, _ = self.made[name]
        for which in (0, 1):

            @pl.when(core == which)
            def _():
                describe(sources[which]).start()

    def arrived(self, name):
        describe, src = self.made[name]
        describe(src).wait_recv()

    def drain(self):
        for describe, src in self.made.values():
            describe(src).wait_send()


def place():
    rep, owner = lax.axis_index("rep"), lax.axis_index("fsdp")
    y, c, z, x = rep // 2, rep % 2, owner // 2, owner % 2
    where = {
        "core": (y * 2 + 1 - c, owner),
        "y": ((1 - y) * 2 + c, owner),
        "x": (rep, z * 2 + 1 - x),
    }
    for k in (1, 2, 3):
        where["z", k] = (rep, ((z + k) % 4) * 2 + x)
        where["zx", k] = (rep, ((z + k) % 4) * 2 + 1 - x)
    return rep, owner, y, c, z, x, where


def greet(where):
    barrier = pltpu.get_barrier_semaphore()
    for to in where.values():
        pl.semaphore_signal(barrier, inc=1, device_id=to, device_id_type=MESH_ID)
    pl.semaphore_wait(barrier, len(where))


def total(*refs):
    value = refs[0][...].astype(jnp.float32)
    for ref in refs[1:]:
        value = value + ref[...].astype(jnp.float32)
    return value


def reduce_kernel(
    gq, gk, gw, go, g1, g2, gv, rq, rk, rw, ro, r1, r2, rv,
    k0, c0, x0, z0, e0, k1, c1, y1, x1, z1, e1, got, vec, send, recv, own_sem, out_sem,
):
    rep, owner, y, c, z, x, where = place()
    part = W // 8
    low = jnp.bfloat16
    flat = [(k, o) for o in (1, 0) for k in (1, 3, 2, 0)]
    slot = {pair: i for i, pair in enumerate(flat)}

    def shard(k, o):
        return ((z + k) % 4) * 2 + (1 - x if o else x)

    def part0(grad, k, o):
        return grad.at[pl.ds(shard(k, o) * part, part), :]

    def part1(quarter, k, o):
        columns = pl.ds(pl.multiple_of(quarter * W, W), W)
        return g1.at[pl.ds(shard(k, o) * part, part), columns]

    def part2(quarter, k, o):
        return g2.at[pl.ds(shard(k, o) * 4 * part + quarter * part, part), :]

    pieces = {1: part1, 2: part2}
    greet(where)
    copies = Copies(send, recv)
    own = {}

    def load(name, src, dst):
        copy = pltpu.make_async_copy(src, dst, own_sem.at[len(own)])
        copy.start()
        own[name] = copy

    def load_either(name, sources, dst):
        turn = own_sem.at[len(own)]
        for which in (0, 1):

            @pl.when(c == which)
            def _():
                pltpu.make_async_copy(sources[which], dst, turn).start()

        own[name] = pltpu.make_async_copy(sources[0], dst, turn)

    for side in (1, 0):
        quarter_row = (1 - y) if side else y
        for pair in flat:
            i = slot[pair]
            for g in (1, 2):
                piece = pieces[g]
                copies.start(
                    (g, "core", side, i), piece(quarter_row * 2 + 1 - c, *pair),
                    c1.at[g - 1, side, i], where["core"],
                )
                load((g, side, i), piece(quarter_row * 2 + c, *pair), k1.at[g - 1, side, i])
            if side:
                for j in range(2):
                    near = [part0(grad, *pair) for grad in ((gq, gw), (gk, go))[j]]
                    copies.start_either(
                        (0, "core", j, i), c, near[::-1], c0.at[i, j], where["core"]
                    )
                    load_either((0, j, i), near, k0.at[i, j])
    for k in (1, 2, 3):
        copies.start(("v", "z", k), gv.at[shard(k, 0)], got.at[k], where["z", k])
        copies.start(("v", "zx", k), gv.at[shard(k, 1)], got.at[3 + k], where["zx", k])
    copies.start(("v", "x", 0), gv.at[shard(0, 1)], got.at[7], where["x"])

    def ready(g, *rest):
        for name in [(0,) + rest, (1,) + rest] if g == 0 else [rest]:
            own[(g,) + name].wait()
            copies.arrived((g, "core") + name)

    for pair in flat:
        i = slot[pair]
        for g in (1, 2):
            ready(g, 1, i)
            k1[g - 1, 1, i] = total(k1.at[g - 1, 1, i], c1.at[g - 1, 1, i]).astype(low)
            copies.start((g, "y", i), k1.at[g - 1, 1, i], y1.at[g - 1, i], where["y"])
        if pair[1] == 1:
            ready(0, i)
            k0[i] = total(k0.at[i], c0.at[i]).astype(low)
            copies.start((0, "x", i), k0.at[i], x0.at[i], where["x"])
    for pair in flat:
        k, o = pair
        i = slot[pair]
        j = slot[k, 1]
        if o == 1:
            for g in (1, 2):
                ready(g, 0, i)
                copies.arrived((g, "y", i))
                k1[g - 1, 0, i] = total(
                    k1.at[g - 1, 0, i], c1.at[g - 1, 0, i], y1.at[g - 1, i]
                ).astype(low)
                copies.start((g, "x", i), k1.at[g - 1, 0, i], x1.at[g - 1, i], where["x"])
        elif k > 0:
            ready(0, i)
            copies.arrived((0, "x", j))
            k0[i] = total(k0.at[i], c0.at[i], x0.at[j]).astype(low)
            copies.start((0, "z", k), k0.at[i], z0.at[k - 1], where["z", k])
            for g in (1, 2):
                ready(g, 0, i)
                copies.arrived((g, "y", i))
                copies.arrived((g, "x", j))
                k1[g - 1, 0, i] = total(
                    k1.at[g - 1, 0, i], c1.at[g - 1, 0, i], y1.at[g - 1, i], x1.at[g - 1, j]
                ).astype(low)
                copies.start((g, "z", k), k1.at[g - 1, 0, i], z1.at[g - 1, k - 1], where["z", k])
    for k in (1, 2, 3):
        copies.arrived(("v", "z", k))
        copies.arrived(("v", "zx", k))
    copies.arrived(("v", "x", 0))
    load("v", gv.at[owner], got.at[0])
    own["v"].wait()
    value = got[0]
    for i in range(1, 8):
        value = value + got[i]
    vec[0] = value
    copies.start(("v", "core"), vec.at[0], vec.at[1], where["core"])
    i, j = slot[0, 0], slot[0, 1]
    ready(0, i)
    copies.arrived((0, "x", j))
    for k in (1, 2, 3):
        copies.arrived((0, "z", k))
    e0[0] = total(k0.at[i], c0.at[i], x0.at[j], z0.at[0], z0.at[1], z0.at[2]).astype(low)
    copies.start((0, "y"), e0.at[0], e0.at[1], where["y"])
    for g in (1, 2):
        ready(g, 0, i)
        copies.arrived((g, "y", i))
        copies.arrived((g, "x", j))
        for k in (1, 2, 3):
            copies.arrived((g, "z", k))
        e1[g - 1, 0] = total(
            k1.at[g - 1, 0, i], c1.at[g - 1, 0, i], y1.at[g - 1, i], x1.at[g - 1, j],
            z1.at[g - 1, 0], z1.at[g - 1, 1], z1.at[g - 1, 2],
        ).astype(low)
        copies.start((g, "ey"), e1.at[g - 1, 0], e1.at[g - 1, 1], where["y"])
        copies.start((g, "ecore"), e1.at[g - 1, 0], e1.at[g - 1, 2], where["core"])
    copies.arrived(("v", "core"))
    vec[2] = vec[0] + vec[1]
    copies.start(("v", "y"), vec.at[2], vec.at[3], where["y"])
    copies.arrived((0, "y"))
    e0[2] = total(e0.at[0], e0.at[1]).astype(low)
    copies.start((0, "ecore"), e0.at[2], e0.at[3], where["core"])
    for g in (1, 2):
        copies.arrived((g, "ey"))
        copies.start((g, "ediagonal"), e1.at[g - 1, 1], e1.at[g - 1, 3], where["core"])
    for core in (0, 1):

        @pl.when(c == core)
        def _():
            for j, ref in enumerate(((rq, rk), (rw, ro))[core]):
                ref[...] = e0[2, j].astype(jnp.float32)

    outs = (rep, (1 - y) * 2 + c, y * 2 + 1 - c, (1 - y) * 2 + 1 - c)

    def put(g, i):
        value = e1[g - 1, i].astype(jnp.float32)
        if g == 1:
            r1[:, pl.ds(pl.multiple_of(outs[i] * W, W), W)] = value
        else:
            r2[pl.ds(outs[i] * part, part), :] = value

    for g in (1, 2):
        put(g, 0)
        put(g, 1)
        copies.arrived((g, "ecore"))
        put(g, 2)
    copies.arrived(("v", "y"))
    rv[...] = vec[2] + vec[3]
    copies.arrived((0, "ecore"))
    for core in (0, 1):

        @pl.when(c == core)
        def _():
            for j, ref in enumerate(((rw, ro), (rq, rk))[core]):
                ref[...] = e0[3, j].astype(jnp.float32)

    for g in (1, 2):
        copies.arrived((g, "ediagonal"))
        put(g, 3)
    copies.drain()


REDUCE_COPIES = 2 * 16 + 16 + 7 + 16 + 4 + 8 + 9 + 1 + 1 + 4 + 1 + 1 + 2


def reduce_all(gq, gk, gw, go, inner, outer, vectors):
    low, full = jnp.bfloat16, jnp.float32
    part = W // 8
    anywhere, near = pl.BlockSpec(memory_space=pl.ANY), pl.BlockSpec(memory_space=pltpu.VMEM)
    return pl.pallas_call(
        reduce_kernel,
        out_shape=(
            jax.ShapeDtypeStruct((part, W), full),
            jax.ShapeDtypeStruct((part, W), full),
            jax.ShapeDtypeStruct((part, W), full),
            jax.ShapeDtypeStruct((part, W), full),
            jax.ShapeDtypeStruct((part, 4 * W), full),
            jax.ShapeDtypeStruct((4 * part, W), full),
            jax.ShapeDtypeStruct(vectors.shape[1:], full),
        ),
        in_specs=[anywhere] * 7,
        out_specs=[near] * 7,
        scratch_shapes=[
            pltpu.VMEM((8, 2, part, W), low),
            pltpu.VMEM((8, 2, part, W), low),
            pltpu.VMEM((4, 2, part, W), low),
            pltpu.VMEM((3, 2, part, W), low),
            pltpu.VMEM((4, 2, part, W), low),
            pltpu.VMEM((2, 2, 8, part, W), low),
            pltpu.VMEM((2, 2, 8, part, W), low),
            pltpu.VMEM((2, 8, part, W), low),
            pltpu.VMEM((2, 4, part, W), low),
            pltpu.VMEM((2, 3, part, W), low),
            pltpu.VMEM((2, 4, part, W), low),
            pltpu.VMEM(vectors.shape, full),
            pltpu.VMEM((4,) + vectors.shape[1:], full),
            pltpu.SemaphoreType.DMA((REDUCE_COPIES,)),
            pltpu.SemaphoreType.DMA((REDUCE_COPIES,)),
            pltpu.SemaphoreType.DMA((2 * 16 + 16 + 1,)),
            pltpu.SemaphoreType.DMA((1,)),
        ],
        compiler_params=pltpu.CompilerParams(
            collective_id=1, has_side_effects=True, vmem_limit_bytes=56 << 20
        ),
        name="reduce_gradients",
    )(gq, gk, gw, go, inner, outer, vectors)


def inner_lines(part):
    return -(-4 * part // 128)


def pack(vectors, inner):
    owners, _, part = vectors.shape
    lines = inner_lines(part)
    first = jnp.pad(vectors, ((0, 0), (0, 0), (0, 128 - part)))
    second = jnp.pad(inner, ((0, 0), (0, lines * 128 - 4 * part)))
    second = second.reshape(owners, lines, 128)
    return jnp.pad(jnp.concatenate([first, second], axis=1), ((0, 0), (0, 8 - lines), (0, 0)))


def unpack(packed, part):
    owners = packed.shape[0]
    lines = inner_lines(part)
    first = packed[:, :8, :part].transpose(1, 0, 2).reshape(8, owners * part)
    second = packed[:, 8 : 8 + lines].reshape(owners, lines * 128)[:, : 4 * part]
    return first, second.reshape(4, owners * part)


def plain_gather(wq, wk, wv, wo, inner, outer, vectors):
    gathered = lax.all_gather(inner, "fsdp", axis=0, tiled=True)
    return (
        lax.all_gather(jnp.stack([wq, wk, wv, wo]), "fsdp", axis=1, tiled=True),
        gathered.reshape(W, 4, W).transpose(1, 0, 2),
        lax.all_gather(outer, "fsdp", axis=0, tiled=True),
        lax.all_gather(vectors, "fsdp", axis=0),
    )


def plain_reduce(*grads):
    def over_all(value):
        part = lax.psum_scatter(value, "fsdp", scatter_dimension=0, tiled=True)
        return lax.psum(part, "rep").astype(jnp.float32)

    return tuple(over_all(grad) for grad in grads[:-1]) + (over_all(grads[-1])[0],)


def product(left, right):
    return jnp.dot(left, right, preferred_element_type=jnp.float32)


def inner_rows(left, right):
    return lax.dot_general(
        left, right, (((0,), (0,)), ((), ())), preferred_element_type=jnp.float32
    )


def against(left, right):
    return lax.dot_general(
        left, right, (((1,), (1,)), ((), ())), preferred_element_type=jnp.float32
    )


def column_sum(values):
    return jnp.sum(values.astype(jnp.float32), axis=0)


TILE = 128
HEAD_DIM = 64
FACTOR = HEAD_DIM ** (-0.5)
HIDDEN = -1e30


def spans(i, count):
    last = count - 1
    if i == last:
        return [(0, count * TILE)]
    low, high = max(0, i - 2), min(last, i + 2)
    if high == last:
        return [(low * TILE, count * TILE)]
    return [(low * TILE, (high + 1) * TILE), (last * TILE, count * TILE)]


def two_heads(block):
    lanes = lax.broadcasted_iota(jnp.int32, block.shape, 1)
    zero = jnp.zeros_like(block)
    first = jnp.where(lanes < HEAD_DIM, block, zero)
    second = jnp.where(lanes < HEAD_DIM, zero, block)
    return jnp.concatenate([first, second], axis=0)


def own_head(value):
    rows = lax.broadcasted_iota(jnp.int32, (TILE, TILE), 0)
    return jnp.where(rows < HEAD_DIM, value[:, :TILE], value[:, TILE:]).T


def masked_scores(k_ref, key_ids, query_ids, stacked, i, span, count):
    low, high = span
    scores = against(k_ref[low:high, :], stacked)
    ids = key_ids[low:high, :]
    row = query_ids[i : i + 1, :]
    seen = ids == row
    if high == count * TILE:
        seen = seen | (ids < 0)
    if i == count - 1:
        seen = seen | (row < 0)
    return jnp.concatenate(
        [jnp.where(seen, scores[:, :TILE], HIDDEN), jnp.where(seen, scores[:, TILE:], HIDDEN)], axis=1
    )


def attend_kernel(key_ids, query_ids, q_ref, k_ref, v_ref, out_ref, lse_ref, v_turned):
    attend_pair(key_ids, query_ids, q_ref, k_ref, v_ref, out_ref, lse_ref.at[0], v_turned)


def attend_pair(key_ids, query_ids, q_ref, k_ref, v_ref, out_ref, lse_ref, v_turned):
    count = q_ref.shape[0] // TILE
    v_turned[...] = v_ref[:, :].T
    for i in range(count):
        rows = slice(i * TILE, (i + 1) * TILE)
        stacked = two_heads(q_ref[rows, :] * jnp.bfloat16(FACTOR))
        parts = spans(i, count)
        scores = [masked_scores(k_ref, key_ids, query_ids, stacked, i, p, count) for p in parts]
        peak = functools.reduce(
            jnp.maximum, [jnp.max(s, axis=0, keepdims=True) for s in scores]
        )
        weights = [jnp.exp(s - peak) for s in scores]
        total = sum(jnp.sum(w, axis=0, keepdims=True) for w in weights)
        mixed = sum(
            product(v_turned[:, low:high], w.astype(jnp.bfloat16)) for (low, high), w in zip(parts, weights)
        )
        out_ref[rows, :] = own_head(mixed * (1.0 / total)).astype(jnp.bfloat16)
        lse_ref[i : i + 1, :] = peak + jnp.log(total)


def attend_back_kernel(
    key_ids, query_ids, q_ref, k_ref, v_ref, g_ref, lse_ref, gq_ref, gk_ref, gv_ref,
    k_turned, k_total, v_total,
):
    count = q_ref.shape[0] // TILE
    k_turned[...] = k_ref[...].T
    k_total[...] = jnp.zeros_like(k_total)
    v_total[...] = jnp.zeros_like(v_total)
    for i in range(count):
        rows = slice(i * TILE, (i + 1) * TILE)
        stacked = two_heads(q_ref[rows, :] * jnp.bfloat16(FACTOR))
        grads = two_heads(g_ref[rows, :])
        lse = lse_ref[0, i : i + 1, :]
        parts = spans(i, count)
        probs, pulls = [], []
        for low, high in parts:
            scores = masked_scores(k_ref, key_ids, query_ids, stacked, i, (low, high), count)
            p = jnp.exp(scores - lse)
            v_total[low:high, :] += product(p.astype(jnp.bfloat16), grads)
            probs.append(p)
            pulls.append(against(v_ref[low:high, :], grads))
        centre = sum(jnp.sum(p * g, axis=0, keepdims=True) for p, g in zip(probs, pulls))
        mixed = 0.0
        for (low, high), p, g in zip(parts, probs, pulls):
            turned = (p * (g - centre)).astype(jnp.bfloat16)
            k_total[low:high, :] += product(turned, stacked)
            mixed = mixed + product(k_turned[:, low:high], turned)
        gq_ref[rows, :] = (own_head(mixed) * FACTOR).astype(jnp.bfloat16)
    gk_ref[...] = k_total[...].astype(jnp.bfloat16)
    gv_ref[...] = v_total[...].astype(jnp.bfloat16)


def attend(key_ids, query_ids, query, keys, values):
    rows, width = query.shape
    pair = 2 * HEAD_DIM
    count = rows // TILE
    column = pl.BlockSpec((rows, pair), lambda h: (0, h))
    whole = lambda a: pl.BlockSpec(a.shape, lambda h: (0, 0))
    return pl.pallas_call(
        attend_kernel,
        grid=(width // pair,),
        out_shape=(
            jax.ShapeDtypeStruct((rows, width), jnp.bfloat16),
            jax.ShapeDtypeStruct((width // pair, count, 2 * TILE), jnp.float32),
        ),
        in_specs=[whole(key_ids), whole(query_ids), column, column, column],
        out_specs=[column, pl.BlockSpec((1, count, 2 * TILE), lambda h: (h, 0, 0))],
        scratch_shapes=[pltpu.VMEM((pair, rows), jnp.bfloat16)],
        compiler_params=pltpu.CompilerParams(vmem_limit_bytes=48 << 20),
        name="attend",
    )(key_ids, query_ids, query, keys, values)


def gather_attend_kernel(
    wq, wk, wv, wo, w1, w2, vec, x_ref, key_ids, query_ids,
    o0, o1, o2, small, inner, q_ref, k_ref, v_ref, out_ref, lse_ref,
    w0, a1, a2, av, got, v_turned, send, recv, own_sem, load_sem,
):
    rep, owner, y, c, z, x, where = place()
    part = W // 8
    low = jnp.bfloat16
    across = (1 - y) * 2 + c
    mine0 = pl.ds(owner * part, part)
    loads = [
        pltpu.make_async_copy(source, into, load_sem.at[i])
        for i, (source, into) in enumerate(
            [
                (wq, w0.at[0, mine0, :]),
                (wk, w0.at[1, mine0, :]),
                (wv, w0.at[2, mine0, :]),
                (wo, w0.at[3, mine0, :]),
                (w1, a1),
                (w2, a2),
                (vec, av),
            ]
        )
    ]
    for load in loads:
        load.start()

    def shard(k, other_x):
        return ((z - k + 4) % 4) * 2 + (1 - x if other_x else x)

    def in0(k, other_x):
        return w0.at[pl.ds(c * 2, 2), pl.ds(shard(k, other_x) * part, part), :]

    def in1(k, other_x, quarter):
        return o1.at[quarter, pl.ds(shard(k, other_x) * part, part), :]

    def in2(k, other_x, quarter):
        return o2.at[pl.ds(shard(k, other_x) * 4 * part + quarter * part, part), :]

    greet(where)
    for load in loads:
        load.wait()
    own = [pltpu.make_async_copy(a2, o2.at[pl.ds(owner * 4 * part, 4 * part), :], own_sem.at[0])]
    for r in range(4):
        own.append(
            pltpu.make_async_copy(
                a1.at[:, r * W : (r + 1) * W], o1.at[r, mine0, :], own_sem.at[1 + r]
            )
        )
    kept = pltpu.make_async_copy(w0, o0, own_sem.at[5])
    note = pltpu.make_async_copy(av, got.at[owner], own_sem.at[6])

    copies = Copies(send, recv)
    from1 = a1.at[:, pl.ds(pl.multiple_of(rep * W, W), W)]
    from2 = a2.at[pl.ds(rep * part, part), :]

    def first(g, stage, k):
        source = (in0(0, False), from1, from2)[g]
        into = (in0(0, False), in1(0, False, rep), in2(0, False, rep))[g]
        copies.start((g, stage, k), source, into, where["x"] if stage == "x" else where["z", k])

    first(0, "x", 0)
    for g, k in FIRST_SENDS:
        first(g, "z", k)
        if (g, k) == (0, 2):
            first(1, "x", 0)
            first(2, "x", 0)
    for k in (1, 2, 3):
        copies.start(("v", "z", k), av, got.at[owner], where["z", k])
        copies.start(("v", "zx", k), av, got.at[owner], where["zx", k])
    copies.start(("v", "x", 0), av, got.at[owner], where["x"])
    note.start()
    for copy in own:
        copy.start()

    steps = [
        (0, True, "x"), (1, False, "z"), (3, False, "z"), (1, True, "x"),
        (2, False, "z"), (3, True, "x"), (2, True, "x"),
    ]
    for k, other_x, stage in steps:
        for g in (0, 1, 2):
            here = (in0(k, other_x), in1(k, other_x, rep), in2(k, other_x, rep))[g]
            if stage == "z":
                copies.plan((g, "x", k), here, here, where["x"])
            if g > 0:
                copies.plan((g, "y", k, other_x), here, here, where["y"])
            copies.plan((g, "core", k, other_x), here, here, where["core"])
    for k, other_x, _ in steps:
        for g in (1, 2):
            there = (in1(k, other_x, across), in2(k, other_x, across))[g - 1]
            copies.plan((g, "diagonal", k, other_x), there, there, where["core"])

    def pass_on(step, groups):
        k, other_x, stage = steps[step]
        for g in groups:
            copies.arrived((g, stage, k))
            if stage == "z":
                copies.go((g, "x", k))
            if g > 0:
                copies.go((g, "y", k, other_x))
            copies.go((g, "core", k, other_x))

    def pass_core(step):
        k, other_x, _ = steps[step]
        for g in (1, 2):
            copies.arrived((g, "y", k, other_x))
            copies.go((g, "diagonal", k, other_x))

    for step, groups in EARLY_STEPS:
        pass_on(step, groups)
    for k, other_x, _ in steps:
        copies.arrived((0, "core", k, other_x))
    for k in (1, 2, 3):
        copies.arrived(("v", "z", k))
        copies.arrived(("v", "zx", k))
    copies.arrived(("v", "x", 0))
    note.wait()
    kept.start()

    lanes = lax.broadcasted_iota(jnp.int32, (TILE, W), 1)
    rows = lax.broadcasted_iota(jnp.int32, (TILE, W), 0)
    joined = jnp.zeros((16, W), jnp.float32)
    for o in range(8):
        pick = ((lanes == rows + o * part) & (rows < part)).astype(low)
        joined = joined + product(got[o], pick)
        for j in range(3):
            i = o * 3 + j
            inner[i // 6 : i // 6 + 1, (i % 6) * TILE : (i % 6 + 1) * TILE] = got[
                o, 8 + j : 9 + j, :
            ].astype(jnp.float32)
    small[...] = joined[:8]

    @pl.loop(0, 4)
    def _(block):
        span = pl.ds(pl.multiple_of(block * 256, 256), 256)
        value = x_ref[span, :]
        q_ref[span, :] = (product(value, w0[0]) + small[0:1, :]).astype(low)
        k_ref[span, :] = product(value, w0[1]).astype(low)
        v_ref[span, :] = (product(value, w0[2]) + small[1:2, :]).astype(low)
        for which, late in enumerate(PROJECTION_STEPS):

            @pl.when(block == which)
            def _():
                for step in late:
                    pass_on(step, (1, 2))

    @pl.loop(0, 6)
    def _(pair):
        columns = pl.ds(pl.multiple_of(pair * TILE, TILE), TILE)
        attend_pair(
            key_ids, query_ids, q_ref.at[:, columns], k_ref.at[:, columns], v_ref.at[:, columns],
            out_ref.at[:, columns], lse_ref.at[pair], v_turned,
        )
        for which, (late, cores) in enumerate(ATTEND_STEPS):

            @pl.when(pair == which)
            def _():
                for step in late:
                    pass_on(step, (1, 2))
                for step in cores:
                    pass_core(step)

    for step in LAST_CORE_STEPS:
        pass_core(step)
    for k, other_x, _ in steps:
        for g in (1, 2):
            copies.arrived((g, "core", k, other_x))
            copies.arrived((g, "diagonal", k, other_x))
    copies.drain()
    for copy in own:
        copy.wait()
    kept.wait()


GATHER_COPIES = 3 * 3 + 3 + 7 + (3 * 3 + 2 * 7 + 3 * 7 + 2 * 7)
FIRST_SENDS = ((0, 1), (0, 3), (0, 2), (1, 1), (2, 1), (1, 3), (2, 3), (1, 2), (2, 2))
EARLY_STEPS = (
    (0, (0,)), (1, (0,)), (2, (0,)), (0, (1, 2)), (3, (0,)), (4, (0,)), (5, (0,)), (6, (0,)),
)
PROJECTION_STEPS = ((1,), (), (2,), ())
ATTEND_STEPS = (((3,), (0,)), ((4,), (1,)), ((5,), (2,)), ((6,), (3,)), ((), (4,)), ((), (5,)))
LAST_CORE_STEPS = (6,)


def gather_attend(shards, rows, key_ids, query_ids):
    low, full = jnp.bfloat16, jnp.float32
    count = rows.shape[0]
    vectors = shards[-1]
    anywhere, near = pl.BlockSpec(memory_space=pl.ANY), pl.BlockSpec(memory_space=pltpu.VMEM)
    thin = jax.ShapeDtypeStruct((count, W), low)
    return pl.pallas_call(
        gather_attend_kernel,
        out_shape=(
            jax.ShapeDtypeStruct((4, W, W), low),
            jax.ShapeDtypeStruct((4, W, W), low),
            jax.ShapeDtypeStruct((4 * W, W), low),
            jax.ShapeDtypeStruct((8, W), full),
            jax.ShapeDtypeStruct((4, W), full),
            thin,
            thin,
            thin,
            thin,
            jax.ShapeDtypeStruct((W // TILE, count // TILE, 2 * TILE), full),
        ),
        in_specs=[anywhere] * 7 + [near] * 3,
        out_specs=[anywhere] * 3 + [near] * 7,
        scratch_shapes=[
            pltpu.VMEM((4, W, W), low),
            pltpu.VMEM(shards[4].shape, low),
            pltpu.VMEM(shards[5].shape, low),
            pltpu.VMEM(vectors.shape, low),
            pltpu.VMEM((8,) + vectors.shape, low),
            pltpu.VMEM((TILE, count), low),
            pltpu.SemaphoreType.DMA((GATHER_COPIES,)),
            pltpu.SemaphoreType.DMA((GATHER_COPIES,)),
            pltpu.SemaphoreType.DMA((7,)),
            pltpu.SemaphoreType.DMA((7,)),
        ],
        compiler_params=pltpu.CompilerParams(
            collective_id=0, has_side_effects=True, vmem_limit_bytes=48 << 20
        ),
        name="gather_attend",
    )(*shards, rows, key_ids, query_ids)


def attend_back(key_ids, query_ids, query, keys, values, grads, lse):
    rows, width = query.shape
    pair = 2 * HEAD_DIM
    count = rows // TILE
    column = pl.BlockSpec((rows, pair), lambda h: (0, h))
    whole = lambda a: pl.BlockSpec(a.shape, lambda h: (0, 0))
    return pl.pallas_call(
        attend_back_kernel,
        grid=(width // pair,),
        out_shape=(jax.ShapeDtypeStruct((rows, width), jnp.bfloat16),) * 3,
        in_specs=[whole(key_ids), whole(query_ids)]
        + [column] * 4
        + [pl.BlockSpec((1, count, 2 * TILE), lambda h: (h, 0, 0))],
        out_specs=[column] * 3,
        scratch_shapes=[
            pltpu.VMEM((pair, rows), jnp.bfloat16),
            pltpu.VMEM((rows, pair), jnp.float32),
            pltpu.VMEM((rows, pair), jnp.float32),
        ],
        compiler_params=pltpu.CompilerParams(vmem_limit_bytes=48 << 20),
        name="attend_back",
    )(key_ids, query_ids, query, keys, values, grads, lse)


ERFC_TERMS = (
    -1.26551223, 1.00002368, 0.37409196, 0.09678418, -0.18628806,
    0.27886807, -1.13520398, 1.48851587, -0.82215223, 0.17087277,
)


def gelu_and_slope(value):
    half_square = value * value * 0.5
    step = 1.0 / (1.0 + jnp.abs(value) * (0.5 * 0.5**0.5))
    power = ERFC_TERMS[-1]
    for term in ERFC_TERMS[-2::-1]:
        power = power * step + term
    tail = 0.5 * step * jnp.exp(power - half_square)
    cover = jnp.where(value < 0, tail, 1.0 - tail)
    density = jnp.exp(-half_square) * ((0.5 / math.pi) ** 0.5)
    return value * cover, cover + value * density


def normalise(value):
    mean = jnp.mean(value, axis=1, keepdims=True)
    centred = value - mean
    scale = lax.rsqrt(jnp.mean(centred * centred, axis=1, keepdims=True) + 1e-05)
    return centred * scale, scale


def normalise_back(grad, unit, scale):
    middle = jnp.mean(grad, axis=1, keepdims=True)
    along = jnp.mean(grad * unit, axis=1, keepdims=True)
    return scale * (grad - middle - unit * along)


def chain_kernel(
    mixed_ref, rows_ref, pull_ref, wo_ref, w1_ref, w2_ref, small_ref, b1_ref,
    out_ref, y1_ref, u_ref, gz_ref, gf_ref, gh_ref, ga_ref, gmix_ref, sums_ref, b1_sum_ref,
    slope_ref,
):
    low = jnp.bfloat16

    @pl.when(pl.program_id(0) == 0)
    def _():
        sums_ref[...] = jnp.zeros_like(sums_ref)
        b1_sum_ref[...] = jnp.zeros_like(b1_sum_ref)

    def small(i):
        return small_ref[i : i + 1, :]

    def gather_sum(ref, i, value):
        ref[i : i + 1, :] += jnp.sum(value, axis=0, keepdims=True)

    hidden = rows_ref[...].astype(jnp.float32) + product(mixed_ref[...], wo_ref[0]) + small(2)
    unit_one, scale_one = normalise(hidden)
    y1 = unit_one * small(3) + small(4)
    y1_low = y1.astype(low)
    y1_ref[...] = y1_low
    second = y1 + small(5)
    for r in range(4):
        inner = product(y1_low, w1_ref[r]) + b1_ref[r : r + 1, :]
        active, slope = gelu_and_slope(inner)
        active = active.astype(low)
        u_ref[:, r * W : (r + 1) * W] = active
        slope_ref[:, r * W : (r + 1) * W] = slope
        second = second + product(active, w2_ref[r * W : (r + 1) * W, :])
    unit_two, scale_two = normalise(second)
    out_ref[...] = (unit_two * small(6) + small(7)).astype(low)
    pull = pull_ref[...].astype(jnp.float32)
    gather_sum(sums_ref, 6, pull * unit_two)
    gather_sum(sums_ref, 7, pull)
    grad_second = normalise_back(pull * small(6), unit_two, scale_two)
    gz = grad_second.astype(low)
    gz_ref[...] = gz
    gather_sum(sums_ref, 5, gz.astype(jnp.float32))
    grad_y1 = grad_second
    for r in range(4):
        gf = against(gz, w2_ref[r * W : (r + 1) * W, :]) * slope_ref[:, r * W : (r + 1) * W]
        gf = gf.astype(low)
        gf_ref[:, r * W : (r + 1) * W] = gf
        gather_sum(b1_sum_ref, r, gf.astype(jnp.float32))
        grad_y1 = grad_y1 + against(gf, w1_ref[r])
    gather_sum(sums_ref, 3, grad_y1 * unit_one)
    gather_sum(sums_ref, 4, grad_y1)
    grad_hidden = normalise_back(grad_y1 * small(3), unit_one, scale_one)
    gh_ref[...] = grad_hidden
    ga = grad_hidden.astype(low)
    ga_ref[...] = ga
    gather_sum(sums_ref, 2, ga.astype(jnp.float32))
    gmix_ref[...] = against(ga, wo_ref[0]).astype(low)


def chain(mixed, rows, pull, weights, inner_blocks, outer_mat, small, inner_bias):
    count, width = rows.shape
    step = 256
    low, full = jnp.bfloat16, jnp.float32
    thin = pl.BlockSpec((step, width), lambda i: (i, 0))
    fat = pl.BlockSpec((step, 4 * width), lambda i: (i, 0))
    held = lambda shape: pl.BlockSpec(shape, lambda i: (0,) * len(shape))
    once = pl.Buffered(1)
    return pl.pallas_call(
        chain_kernel,
        grid=(count // step,),
        out_shape=(
            jax.ShapeDtypeStruct((count, width), low),
            jax.ShapeDtypeStruct((count, width), low),
            jax.ShapeDtypeStruct((count, 4 * width), low),
            jax.ShapeDtypeStruct((count, width), low),
            jax.ShapeDtypeStruct((count, 4 * width), low),
            jax.ShapeDtypeStruct((count, width), full),
            jax.ShapeDtypeStruct((count, width), low),
            jax.ShapeDtypeStruct((count, width), low),
            jax.ShapeDtypeStruct((8, width), full),
            jax.ShapeDtypeStruct((4, width), full),
        ),
        in_specs=[
            thin, thin, thin,
            pl.BlockSpec((1, width, width), lambda i: (3, 0, 0), pipeline_mode=once),
            pl.BlockSpec((4, width, width), lambda i: (0, 0, 0), pipeline_mode=once),
            pl.BlockSpec((4 * width, width), lambda i: (0, 0), pipeline_mode=once),
            held((8, width)), held((4, width)),
        ],
        out_specs=[thin, thin, fat, thin, fat, thin, thin, thin, held((8, width)), held((4, width))],
        scratch_shapes=[pltpu.VMEM((step, 4 * width), full)],
        compiler_params=pltpu.CompilerParams(vmem_limit_bytes=60 << 20),
        name="chain",
    )(mixed, rows, pull, weights, inner_blocks, outer_mat, small, inner_bias)


def on_device(
    tokens,
    read_memory,
    doc_ids,
    w_query,
    w_key,
    w_value,
    w_out,
    query_bias,
    value_bias,
    out_bias,
    norm_one_gain,
    norm_one_bias,
    w_inner,
    inner_bias,
    w_outer,
    outer_bias,
    norm_two_gain,
    norm_two_bias,
    out_grad,
):
    owners = lax.axis_size("fsdp")
    wide = owners == 8 and lax.axis_size("rep") == 4
    part = w_query.shape[0]
    low = jnp.bfloat16
    small = pack(
        jnp.stack(
            [
                query_bias, value_bias, out_bias, norm_one_gain,
                norm_one_bias, outer_bias, norm_two_gain, norm_two_bias,
            ]
        )[None],
        inner_bias[None],
    )[0]
    reduce = reduce_all if wide else plain_reduce
    seqs, seg = doc_ids.shape
    width = tokens.shape[1]
    mem = read_memory.shape[0] // seqs
    length = seg + 2 * mem
    memory_rows = read_memory.reshape(seqs, mem, width)
    rows = jnp.concatenate([tokens.reshape(seqs, seg, width), memory_rows, memory_rows], axis=1)
    rows = rows.reshape(seqs * length, width)
    marks = jnp.full((seqs, 2 * mem), -1, jnp.int32)
    ids = jnp.concatenate([doc_ids, marks], axis=1)
    out_rows = out_grad.reshape(seqs, length, width)
    out_rows = jnp.concatenate(
        [out_rows[:, mem : mem + seg], out_rows[:, :mem], out_rows[:, mem + seg :]], axis=1
    ).reshape(seqs * length, width)

    def each(function, *arrays):
        results = []
        for s in range(seqs):
            own = slice(s * length, (s + 1) * length)
            spread = jnp.broadcast_to(ids[s][:, None], (length, TILE))
            by_block = ids[s].reshape(length // TILE, TILE)
            results.append(function(spread, by_block, *[a[own] for a in arrays]))
        return results

    shards = (w_query, w_key, w_value, w_out, w_inner, w_outer, small)
    if wide and seqs == 1:
        spread, by_block = each(lambda *a: a)[0]
        weights, inner_blocks, outer_mat, vectors, inner_shift, query, keys, values, mixed, sums = (
            gather_attend(shards, rows, spread, by_block)
        )
        pairs = [(mixed, sums)]
    else:
        weights, inner_blocks, outer_mat, packed = plain_gather(*shards)
        vectors, inner_shift = unpack(packed.astype(jnp.float32), part)
        query = (product(rows, weights[0]) + vectors[0]).astype(low)
        keys = product(rows, weights[1]).astype(low)
        values = (product(rows, weights[2]) + vectors[1]).astype(low)
        pairs = each(attend, query, keys, values)
        mixed = jnp.concatenate([pair[0] for pair in pairs], axis=0)
    output, normed, active, grad_outer, grad_inner, grad_residual, grad_branch, grad_mixed, sums, inner_sums = chain(
        mixed, rows, out_rows, weights, inner_blocks, outer_mat, vectors, inner_shift
    )
    grad_w_outer = inner_rows(active, grad_outer).astype(low)
    grad_w_inner = inner_rows(normed, grad_inner).astype(low)
    grad_w_out = inner_rows(mixed, grad_branch).astype(low)
    triples = [
        attend_back(spread, by_block, q, k, v, g, pairs[s][1])
        for s, (spread, by_block, q, k, v, g) in enumerate(
            each(lambda *a: a, query, keys, values, grad_mixed)
        )
    ]
    grad_query_low, grad_keys_low, grad_values_low = (
        jnp.concatenate([triple[i] for triple in triples], axis=0) for i in range(3)
    )
    grad_w_query = inner_rows(rows, grad_query_low).astype(low)
    grad_w_key = inner_rows(rows, grad_keys_low).astype(low)
    grad_w_value = inner_rows(rows, grad_values_low).astype(low)
    sums = jnp.concatenate(
        [column_sum(grad_query_low)[None], column_sum(grad_values_low)[None], sums[2:]], axis=0
    )
    grad_rows = (
        grad_residual
        + against(grad_query_low, weights[0])
        + against(grad_keys_low, weights[1])
        + against(grad_values_low, weights[2])
    ).reshape(seqs, length, width)
    grad_tokens = grad_rows[:, :seg].reshape(seqs * seg, width).astype(jnp.bfloat16)
    grad_memory = (
        (grad_rows[:, seg : seg + mem] + grad_rows[:, seg + mem :])
        .reshape(seqs * mem, width)
        .astype(jnp.bfloat16)
    )
    layer_out = output.reshape(seqs, length, width)
    layer_out = jnp.concatenate(
        [layer_out[:, seg : seg + mem], layer_out[:, :seg], layer_out[:, seg + mem :]], axis=1
    ).reshape(seqs * length, width)
    share_wq, share_wk, share_wv, share_wo, share_inner, share_outer, share_small = reduce(
        grad_w_query,
        grad_w_key,
        grad_w_value,
        grad_w_out,
        grad_w_inner,
        grad_w_outer,
        pack(
            sums.reshape(8, owners, part).transpose(1, 0, 2),
            inner_sums.reshape(owners, 4 * part),
        ),
    )
    last, last_inner = unpack(share_small[None], part)
    return (
        layer_out,
        grad_tokens,
        grad_memory,
        share_wq,
        share_wk,
        share_wv,
        share_wo,
        *(last[i] for i in range(5)),
        share_inner,
        last_inner.reshape(-1),
        share_outer,
        *(last[i] for i in range(5, 8)),
    )


def solution(mesh):
    return jax.shard_map(
        on_device,
        mesh=mesh,
        in_specs=(
            P(("rep", "fsdp"), None),
            P(("rep", "fsdp"), None),
            P(("rep", "fsdp"), None),
            P("fsdp", None),
            P("fsdp", None),
            P("fsdp", None),
            P("fsdp", None),
            P("fsdp"),
            P("fsdp"),
            P("fsdp"),
            P("fsdp"),
            P("fsdp"),
            P("fsdp", None),
            P("fsdp"),
            P("fsdp", None),
            P("fsdp"),
            P("fsdp"),
            P("fsdp"),
            P(("rep", "fsdp"), None),
        ),
        out_specs=(
            P(("rep", "fsdp"), None),
            P(("rep", "fsdp"), None),
            P(("rep", "fsdp"), None),
            P("fsdp", None),
            P("fsdp", None),
            P("fsdp", None),
            P("fsdp", None),
            P("fsdp"),
            P("fsdp"),
            P("fsdp"),
            P("fsdp"),
            P("fsdp"),
            P("fsdp", None),
            P("fsdp"),
            P("fsdp", None),
            P("fsdp"),
            P("fsdp"),
            P("fsdp"),
        ),
        check_vma=False,
    )
```

```python
import functools
import math

import jax
import jax.numpy as jnp
from jax import lax
from jax.experimental import pallas as pl
from jax.experimental.pallas import tpu as pltpu
from jax.sharding import PartitionSpec as P

MESH_ID = pl.DeviceIdType.MESH
W = 768


class Copies:
    def __init__(self, send, recv):
        self.send, self.recv, self.made = send, recv, {}

    def plan(self, name, src, dst, to):
        slot = len(self.made)

        def describe(src):
            return pltpu.make_async_remote_copy(
                src_ref=src,
                dst_ref=dst,
                send_sem=self.send.at[slot],
                recv_sem=self.recv.at[slot],
                device_id=to,
                device_id_type=MESH_ID,
            )

        self.made[name] = (describe, src)

    def go(self, name):
        describe, src = self.made[name]
        describe(src).start()

    def start(self, name, src, dst, to):
        self.plan(name, src, dst, to)
        self.go(name)

    def start_either(self, name, core, sources, dst, to):
        self.plan(name, dst, dst, to)
        describe, _ = self.made[name]
        for which in (0, 1):

            @pl.when(core == which)
            def _():
                describe(sources[which]).start()

    def arrived(self, name):
        describe, src = self.made[name]
        describe(src).wait_recv()

    def drain(self):
        for describe, src in self.made.values():
            describe(src).wait_send()


def place():
    rep, owner = lax.axis_index("rep"), lax.axis_index("fsdp")
    y, c, z, x = rep // 2, rep % 2, owner // 2, owner % 2
    where = {
        "core": (y * 2 + 1 - c, owner),
        "y": ((1 - y) * 2 + c, owner),
        "x": (rep, z * 2 + 1 - x),
    }
    for k in (1, 2, 3):
        where["z", k] = (rep, ((z + k) % 4) * 2 + x)
        where["zx", k] = (rep, ((z + k) % 4) * 2 + 1 - x)
    return rep, owner, y, c, z, x, where


def greet(where):
    barrier = pltpu.get_barrier_semaphore()
    for to in where.values():
        pl.semaphore_signal(barrier, inc=1, device_id=to, device_id_type=MESH_ID)
    pl.semaphore_wait(barrier, len(where))


def total(*refs):
    value = refs[0][...].astype(jnp.float32)
    for ref in refs[1:]:
        value = value + ref[...].astype(jnp.float32)
    return value


def inner_lines(part):
    return -(-4 * part // 128)


def pack(vectors, inner):
    owners, _, part = vectors.shape
    lines = inner_lines(part)
    first = jnp.pad(vectors, ((0, 0), (0, 0), (0, 128 - part)))
    second = jnp.pad(inner, ((0, 0), (0, lines * 128 - 4 * part)))
    second = second.reshape(owners, lines, 128)
    return jnp.pad(jnp.concatenate([first, second], axis=1), ((0, 0), (0, 8 - lines), (0, 0)))


def unpack(packed, part):
    owners = packed.shape[0]
    lines = inner_lines(part)
    first = packed[:, :8, :part].transpose(1, 0, 2).reshape(8, owners * part)
    second = packed[:, 8 : 8 + lines].reshape(owners, lines * 128)[:, : 4 * part]
    return first, second.reshape(4, owners * part)


def plain_gather(wq, wk, wv, wo, inner, outer, vectors):
    gathered = lax.all_gather(inner, "fsdp", axis=0, tiled=True)
    return (
        lax.all_gather(jnp.stack([wq, wk, wv, wo]), "fsdp", axis=1, tiled=True),
        gathered.reshape(W, 4, W).transpose(1, 0, 2),
        lax.all_gather(outer, "fsdp", axis=0, tiled=True),
        lax.all_gather(vectors, "fsdp", axis=0),
    )


def plain_reduce(*grads):
    def over_all(value):
        part = lax.psum_scatter(value, "fsdp", scatter_dimension=0, tiled=True)
        return lax.psum(part, "rep").astype(jnp.float32)

    return tuple(over_all(grad) for grad in grads[:-1]) + (over_all(grads[-1])[0],)


def product(left, right):
    return jnp.dot(left, right, preferred_element_type=jnp.float32)


def inner_rows(left, right):
    return lax.dot_general(
        left, right, (((0,), (0,)), ((), ())), preferred_element_type=jnp.float32
    )


def against(left, right):
    return lax.dot_general(
        left, right, (((1,), (1,)), ((), ())), preferred_element_type=jnp.float32
    )


def column_sum(values):
    return jnp.sum(values.astype(jnp.float32), axis=0)


TILE = 128
HEAD_DIM = 64
FACTOR = HEAD_DIM ** (-0.5)
HIDDEN = -1e30


def spans(i, count):
    last = count - 1
    if i == last:
        return [(0, count * TILE)]
    low, high = max(0, i - 2), min(last, i + 2)
    if high == last:
        return [(low * TILE, count * TILE)]
    return [(low * TILE, (high + 1) * TILE), (last * TILE, count * TILE)]


def two_heads(block):
    lanes = lax.broadcasted_iota(jnp.int32, block.shape, 1)
    zero = jnp.zeros_like(block)
    first = jnp.where(lanes < HEAD_DIM, block, zero)
    second = jnp.where(lanes < HEAD_DIM, zero, block)
    return jnp.concatenate([first, second], axis=0)


def own_head(value):
    rows = lax.broadcasted_iota(jnp.int32, (TILE, TILE), 0)
    return jnp.where(rows < HEAD_DIM, value[:, :TILE], value[:, TILE:]).T


def masked_scores(k_ref, key_ids, query_ids, stacked, i, span, count):
    low, high = span
    scores = against(k_ref[low:high, :], stacked)
    ids = key_ids[low:high, :]
    row = query_ids[i : i + 1, :]
    seen = ids == row
    if high == count * TILE:
        seen = seen | (ids < 0)
    if i == count - 1:
        seen = seen | (row < 0)
    return jnp.concatenate(
        [jnp.where(seen, scores[:, :TILE], HIDDEN), jnp.where(seen, scores[:, TILE:], HIDDEN)], axis=1
    )


def attend_kernel(key_ids, query_ids, q_ref, k_ref, v_ref, out_ref, lse_ref, v_turned):
    attend_pair(key_ids, query_ids, q_ref, k_ref, v_ref, out_ref, lse_ref.at[0], v_turned)


def attend_pair(key_ids, query_ids, q_ref, k_ref, v_ref, out_ref, lse_ref, v_turned):
    count = q_ref.shape[0] // TILE
    v_turned[...] = v_ref[:, :].T
    for i in range(count):
        rows = slice(i * TILE, (i + 1) * TILE)
        stacked = two_heads(q_ref[rows, :] * jnp.bfloat16(FACTOR))
        parts = spans(i, count)
        scores = [masked_scores(k_ref, key_ids, query_ids, stacked, i, p, count) for p in parts]
        peak = functools.reduce(
            jnp.maximum, [jnp.max(s, axis=0, keepdims=True) for s in scores]
        )
        weights = [jnp.exp(s - peak) for s in scores]
        total = sum(jnp.sum(w, axis=0, keepdims=True) for w in weights)
        mixed = sum(
            product(v_turned[:, low:high], w.astype(jnp.bfloat16)) for (low, high), w in zip(parts, weights)
        )
        out_ref[rows, :] = own_head(mixed * (1.0 / total)).astype(jnp.bfloat16)
        lse_ref[i : i + 1, :] = peak + jnp.log(total)


def attend_back_kernel(
    key_ids, query_ids, q_ref, k_ref, v_ref, g_ref, lse_ref, gq_ref, gk_ref, gv_ref,
    k_turned, k_total, v_total,
):
    attend_back_pair(
        key_ids, query_ids, q_ref, k_ref, v_ref, g_ref, lse_ref.at[0], gq_ref, gk_ref, gv_ref,
        k_turned, k_total, v_total,
    )


def attend_back_pair(
    key_ids, query_ids, q_ref, k_ref, v_ref, g_ref, lse_ref, gq_ref, gk_ref, gv_ref,
    k_turned, k_total, v_total,
):
    count = q_ref.shape[0] // TILE
    k_turned[...] = k_ref[:, :].T
    k_total[...] = jnp.zeros_like(k_total)
    v_total[...] = jnp.zeros_like(v_total)
    for i in range(count):
        rows = slice(i * TILE, (i + 1) * TILE)
        stacked = two_heads(q_ref[rows, :] * jnp.bfloat16(FACTOR))
        grads = two_heads(g_ref[rows, :])
        lse = lse_ref[i : i + 1, :]
        parts = spans(i, count)
        probs, pulls = [], []
        for low, high in parts:
            scores = masked_scores(k_ref, key_ids, query_ids, stacked, i, (low, high), count)
            p = jnp.exp(scores - lse)
            v_total[low:high, :] += product(p.astype(jnp.bfloat16), grads)
            probs.append(p)
            pulls.append(against(v_ref[low:high, :], grads))
        centre = sum(jnp.sum(p * g, axis=0, keepdims=True) for p, g in zip(probs, pulls))
        mixed = 0.0
        for (low, high), p, g in zip(parts, probs, pulls):
            turned = (p * (g - centre)).astype(jnp.bfloat16)
            k_total[low:high, :] += product(turned, stacked)
            mixed = mixed + product(k_turned[:, low:high], turned)
        gq_ref[rows, :] = (own_head(mixed) * FACTOR).astype(jnp.bfloat16)
    gk_ref[:, :] = k_total[...].astype(jnp.bfloat16)
    gv_ref[:, :] = v_total[...].astype(jnp.bfloat16)


def attend(key_ids, query_ids, query, keys, values):
    rows, width = query.shape
    pair = 2 * HEAD_DIM
    count = rows // TILE
    column = pl.BlockSpec((rows, pair), lambda h: (0, h))
    whole = lambda a: pl.BlockSpec(a.shape, lambda h: (0, 0))
    return pl.pallas_call(
        attend_kernel,
        grid=(width // pair,),
        out_shape=(
            jax.ShapeDtypeStruct((rows, width), jnp.bfloat16),
            jax.ShapeDtypeStruct((width // pair, count, 2 * TILE), jnp.float32),
        ),
        in_specs=[whole(key_ids), whole(query_ids), column, column, column],
        out_specs=[column, pl.BlockSpec((1, count, 2 * TILE), lambda h: (h, 0, 0))],
        scratch_shapes=[pltpu.VMEM((pair, rows), jnp.bfloat16)],
        compiler_params=pltpu.CompilerParams(vmem_limit_bytes=48 << 20),
        name="attend",
    )(key_ids, query_ids, query, keys, values)


def gather_attend_kernel(
    wq, wk, wv, wo, w1, w2, vec, x_ref, key_ids, query_ids,
    o0, o1, o2, small, inner, q_ref, k_ref, v_ref, out_ref, lse_ref,
    w0, a1, a2, av, got, v_turned, send, recv, own_sem, load_sem,
):
    rep, owner, y, c, z, x, where = place()
    part = W // 8
    low = jnp.bfloat16
    across = (1 - y) * 2 + c
    mine0 = pl.ds(owner * part, part)
    loads = [
        pltpu.make_async_copy(source, into, load_sem.at[i])
        for i, (source, into) in enumerate(
            [(source, w0.at[i, mine0, :]) for i, source in enumerate((wq, wk, wv, wo))]
            + [(w1.at[:, i * W : (i + 1) * W], a1.at[i]) for i in range(4)]
            + [(w2, a2), (vec, av)]
        )
    ]
    for load in loads:
        load.start()

    def shard(k, other_x):
        return ((z - k + 4) % 4) * 2 + (1 - x if other_x else x)

    def spot(g, kind, k, other_x, quarter):
        at = 2 * TILE + quarter * TILE if kind else c * TILE
        lanes = pl.ds(pl.multiple_of(at, TILE), TILE)
        if g == 2:
            return o2.at[pl.ds(shard(k, other_x) * 4 * part, 4 * part), lanes]
        return (w0, o1)[g].at[:, pl.ds(shard(k, other_x) * part, part), lanes]

    greet(where)
    for load in loads:
        load.wait()
    own = [
        pltpu.make_async_copy(a1, o1.at[:, mine0, :], own_sem.at[0]),
        pltpu.make_async_copy(a2, o2.at[pl.ds(owner * 4 * part, 4 * part), :], own_sem.at[1]),
    ]
    kept = pltpu.make_async_copy(w0, o0, own_sem.at[2])
    note = pltpu.make_async_copy(av, got.at[owner], own_sem.at[3])
    copies = Copies(send, recv)

    def first(g, stage, k):
        for kind in (1, 0):
            at = 2 * TILE + rep * TILE if kind else c * TILE
            lanes = pl.ds(pl.multiple_of(at, TILE), TILE)
            source = (w0.at[:, mine0, lanes], a1.at[:, :, lanes], a2.at[:, lanes])[g]
            to = where["x"] if stage == "x" else where["z", k]
            copies.plan((g, kind, stage, k), source, spot(g, kind, 0, False, rep), to)

    def send(g, stage, k):
        for kind in (1, 0):
            copies.go((g, kind, stage, k))

    for k in (1, 2, 3):
        copies.start(("v", "z", k), av, got.at[owner], where["z", k])
        copies.start(("v", "zx", k), av, got.at[owner], where["zx", k])
    copies.start(("v", "x", 0), av, got.at[owner], where["x"])
    for g in (0, 1, 2):
        first(g, "x", 0)
        for k in (1, 3, 2):
            first(g, "z", k)
    send(0, "x", 0)
    for g in (0, 1, 2):
        for k in (1, 3, 2):
            send(g, "z", k)
    note.start()
    for copy in own:
        copy.start()

    steps = [
        (0, True, "x"), (1, False, "z"), (3, False, "z"), (1, True, "x"),
        (2, False, "z"), (3, True, "x"), (2, True, "x"),
    ]
    for g in (0, 1, 2):
        for k, other_x, stage in steps:
            for kind in (0, 1):
                here = spot(g, kind, k, other_x, rep)
                if stage == "z":
                    copies.plan((g, kind, "x", k), here, here, where["x"])
                if kind:
                    copies.plan((g, "y", k, other_x), here, here, where["y"])
                    there = spot(g, kind, k, other_x, across)
                    copies.plan((g, "diagonal", k, other_x), there, there, where["core"])
                copies.plan((g, kind, "core", k, other_x), here, here, where["core"])

    def pass_on(g, step):
        k, other_x, stage = steps[step]
        for kind in (1, 0):
            copies.arrived((g, kind, stage, k))
            if kind:
                copies.go((g, "y", k, other_x))
            if stage == "z":
                copies.go((g, kind, "x", k))
            copies.go((g, kind, "core", k, other_x))
        if step == 4 and g < 2:
            send(g + 1, "x", 0)

    def pass_core(g, step):
        k, other_x, _ = steps[step]
        copies.arrived((g, "y", k, other_x))
        copies.go((g, "diagonal", k, other_x))

    def settle(g):
        for k, other_x, _ in steps:
            copies.arrived((g, 0, "core", k, other_x))
            copies.arrived((g, 1, "core", k, other_x))
            copies.arrived((g, "diagonal", k, other_x))

    def pump(events):
        for kind, g, step in events:
            (pass_core if kind == "c" else pass_on)(g, step)

    pump(EARLY)
    settle(0)
    for k in (1, 2, 3):
        copies.arrived(("v", "z", k))
        copies.arrived(("v", "zx", k))
    copies.arrived(("v", "x", 0))
    note.wait()
    kept.start()

    lanes = lax.broadcasted_iota(jnp.int32, (TILE, W), 1)
    rows = lax.broadcasted_iota(jnp.int32, (TILE, W), 0)
    joined = jnp.zeros((16, W), jnp.float32)
    for o in range(8):
        pick = ((lanes == rows + o * part) & (rows < part)).astype(low)
        joined = joined + product(got[o], pick)
        for j in range(3):
            i = o * 3 + j
            inner[i // 6 : i // 6 + 1, (i % 6) * TILE : (i % 6 + 1) * TILE] = got[
                o, 8 + j : 9 + j, :
            ].astype(jnp.float32)
    small[...] = joined[:8]

    @pl.loop(0, 4)
    def _(block):
        span = pl.ds(pl.multiple_of(block * 256, 256), 256)
        value = x_ref[span, :]
        q_ref[span, :] = (product(value, w0[0]) + small[0:1, :]).astype(low)
        k_ref[span, :] = product(value, w0[1]).astype(low)
        v_ref[span, :] = (product(value, w0[2]) + small[1:2, :]).astype(low)
        for which, events in enumerate(DURING_PROJECTIONS):

            @pl.when(block == which)
            def _():
                pump(events)

    @pl.loop(0, 6)
    def _(pair):
        columns = pl.ds(pl.multiple_of(pair * TILE, TILE), TILE)
        attend_pair(
            key_ids, query_ids, q_ref.at[:, columns], k_ref.at[:, columns], v_ref.at[:, columns],
            out_ref.at[:, columns], lse_ref.at[pair], v_turned,
        )
        for which, events in enumerate(DURING_ATTENTION):

            @pl.when(pair == which)
            def _():
                pump(events)

    pump(LATE)
    settle(1)
    settle(2)
    copies.drain()
    for copy in own:
        copy.wait()
    kept.wait()


GATHER_COPIES = 7 + 3 * (2 * 4 + 2 * 3 + 7 * 4)


def run(g, *order):
    return [(name[0], g, int(name[1])) for name in order]


EARLY = run(0, "p0", "p1", "p2", "c0", "p3", "p4", "c1", "p5", "c2", "p6", "c3", "c4", "c5", "c6")
DURING_PROJECTIONS = [run(1, "p0"), run(1, "p1"), run(1, "p2", "c0"), run(1, "p3", "c1")]
DURING_ATTENTION = [
    run(1, "p4", "c2"),
    run(1, "p5", "c3", "p6", "c4") + run(2, "p0"),
    run(2, "p1") + run(1, "c5", "c6"),
    run(2, "p2", "c0"),
    run(2, "p3", "c1", "p4"),
    run(2, "c2", "p5", "c3"),
]
LATE = run(2, "p6", "c4", "c5", "c6")


def gather_attend(shards, rows, key_ids, query_ids):
    low, full = jnp.bfloat16, jnp.float32
    count = rows.shape[0]
    vectors = shards[-1]
    anywhere, near = pl.BlockSpec(memory_space=pl.ANY), pl.BlockSpec(memory_space=pltpu.VMEM)
    thin = jax.ShapeDtypeStruct((count, W), low)
    return pl.pallas_call(
        gather_attend_kernel,
        out_shape=(
            jax.ShapeDtypeStruct((4, W, W), low),
            jax.ShapeDtypeStruct((4, W, W), low),
            jax.ShapeDtypeStruct((4 * W, W), low),
            jax.ShapeDtypeStruct((8, W), full),
            jax.ShapeDtypeStruct((4, W), full),
            thin,
            thin,
            thin,
            thin,
            jax.ShapeDtypeStruct((W // TILE, count // TILE, 2 * TILE), full),
        ),
        in_specs=[anywhere] * 7 + [near] * 3,
        out_specs=[anywhere] * 3 + [near] * 7,
        scratch_shapes=[
            pltpu.VMEM((4, W, W), low),
            pltpu.VMEM((4, W // 8, W), low),
            pltpu.VMEM(shards[5].shape, low),
            pltpu.VMEM(vectors.shape, low),
            pltpu.VMEM((8,) + vectors.shape, low),
            pltpu.VMEM((TILE, count), low),
            pltpu.SemaphoreType.DMA((GATHER_COPIES,)),
            pltpu.SemaphoreType.DMA((GATHER_COPIES,)),
            pltpu.SemaphoreType.DMA((4,)),
            pltpu.SemaphoreType.DMA((10,)),
        ],
        compiler_params=pltpu.CompilerParams(
            collective_id=0, has_side_effects=True, vmem_limit_bytes=48 << 20
        ),
        name="gather_attend",
    )(*shards, rows, key_ids, query_ids)


def attend_back(key_ids, query_ids, query, keys, values, grads, lse):
    rows, width = query.shape
    pair = 2 * HEAD_DIM
    count = rows // TILE
    column = pl.BlockSpec((rows, pair), lambda h: (0, h))
    whole = lambda a: pl.BlockSpec(a.shape, lambda h: (0, 0))
    return pl.pallas_call(
        attend_back_kernel,
        grid=(width // pair,),
        out_shape=(jax.ShapeDtypeStruct((rows, width), jnp.bfloat16),) * 3,
        in_specs=[whole(key_ids), whole(query_ids)]
        + [column] * 4
        + [pl.BlockSpec((1, count, 2 * TILE), lambda h: (h, 0, 0))],
        out_specs=[column] * 3,
        scratch_shapes=[
            pltpu.VMEM((pair, rows), jnp.bfloat16),
            pltpu.VMEM((rows, pair), jnp.float32),
            pltpu.VMEM((rows, pair), jnp.float32),
        ],
        compiler_params=pltpu.CompilerParams(vmem_limit_bytes=48 << 20),
        name="attend_back",
    )(key_ids, query_ids, query, keys, values, grads, lse)


ERFC_TERMS = (
    -1.26551223, 1.00002368, 0.37409196, 0.09678418, -0.18628806,
    0.27886807, -1.13520398, 1.48851587, -0.82215223, 0.17087277,
)


def gelu_and_slope(value):
    half_square = value * value * 0.5
    step = 1.0 / (1.0 + jnp.abs(value) * (0.5 * 0.5**0.5))
    power = ERFC_TERMS[-1]
    for term in ERFC_TERMS[-2::-1]:
        power = power * step + term
    tail = 0.5 * step * jnp.exp(power - half_square)
    cover = jnp.where(value < 0, tail, 1.0 - tail)
    density = jnp.exp(-half_square) * ((0.5 / math.pi) ** 0.5)
    return value * cover, cover + value * density


def reduce_attend_kernel(
    q_in, k_in, v_in, g_in, x_in, gh_in, w_in, go, g1, g2, lse_ref, key_ids, query_ids, sums_in,
    inner_in, gx, rq, rk, rw, ro, r1, r2, rv,
    held, x_kept, x_turned, grads, dw, k_turned, k_total, v_total,
    keep0, keep1, keep2, core0, core1, core2, got_y, got_x, got_z, ends, vec,
    send, recv, load_sem, own_sem,
):
    rep, owner, y, c, z, x, where = place()
    part = W // 8
    low = jnp.bfloat16
    loads = [
        pltpu.make_async_copy(source, into, load_sem.at[i])
        for i, (source, into) in enumerate(
            [(source, held.at[i]) for i, source in enumerate((q_in, k_in, v_in, g_in))]
            + [(x_in, x_kept), (gh_in, gx), (go, dw.at[3])]
        )
    ]
    for load in loads:
        load.start()
    copies = Copies(send, recv)
    keep, core = (keep0, keep1, keep2), (core0, core1, core2)
    order = (1, 3, 2, 0)
    flat = [(k, o) for o in (1, 0) for k in order]

    def shard(k, o):
        return ((z + k) % 4) * 2 + (1 - x if o else x)

    def lanes(kind, this_core):
        which = 0 if this_core else 1
        own_core = c if which == 0 else 1 - c
        at = {
            0: 2 * TILE + ((1 - y) * 2 + own_core) * TILE,
            1: own_core * TILE,
            2: 2 * TILE + (y * 2 + own_core) * TILE,
        }[kind]
        return at

    def columns(kind, this_core, block=0):
        return pl.ds(pl.multiple_of(block * W + lanes(kind, this_core), TILE), TILE)

    def sources(g, kind, this_core):
        if g == 0:
            return [dw.at[:, :, columns(kind, this_core)]]
        if g == 1:
            return [g1.at[:, columns(kind, this_core, j)] for j in range(4)]
        return [g2.at[:, :, columns(kind, this_core)]]

    def targets(g, kind, refs):
        return [refs[g].at[kind, j] for j in range(4)] if g == 1 else [refs[g].at[kind]]

    def cut(g, kind, refs, k, o):
        if g == 2:
            return refs[g].at[kind, pl.ds(shard(k, o) * 4, 4), :, :]
        return refs[g].at[kind, :, pl.ds(shard(k, o) * part, part), :]

    own = {}
    for g in (2, 1, 0):
        for kind in (0, 1, 2):
            pairs = zip(sources(g, kind, False), targets(g, kind, core))
            for j, (source, into) in enumerate(pairs):
                copies.plan((g, "core", kind, j), source, into, where["core"])
            pairs = zip(sources(g, kind, True), targets(g, kind, keep))
            for j, (source, into) in enumerate(pairs):
                own[g, kind, j] = pltpu.make_async_copy(source, into, own_sem.at[len(own)])
        for i, (k, o) in enumerate(flat):
            copies.plan((g, "y", k, o), cut(g, 0, keep, k, o), got_y.at[g, i], where["y"])
        for k in order:
            for s, kind in enumerate((1, 2)):
                copies.plan(
                    (g, kind, "x", k), cut(g, kind, keep, k, 1), got_x.at[g, s, k], where["x"]
                )
                if k:
                    copies.plan(
                        (g, kind, "z", k), cut(g, kind, keep, k, 0), got_z.at[g, s, k - 1],
                        where["z", k],
                    )
        copies.plan((g, 1, "ey"), ends.at[g, 0, 0], ends.at[g, 0, 1], where["y"])
        copies.plan((g, 1, "ecore"), ends.at[g, 0, 2], ends.at[g, 0, 3], where["core"])
        copies.plan((g, 2, "ey"), ends.at[g, 1, 0], ends.at[g, 1, 1], where["y"])
        copies.plan((g, 2, "ecore"), ends.at[g, 1, 0], ends.at[g, 1, 2], where["core"])
        copies.plan((g, 2, "ediagonal"), ends.at[g, 1, 1], ends.at[g, 1, 3], where["core"])
    copies.plan(("v", "core"), vec.at[0], vec.at[1], where["core"])
    copies.plan(("v", "y"), vec.at[2], vec.at[3], where["y"])
    copies.plan(("v", "x"), vec.at[4], vec.at[5], where["x"])
    for k in (1, 2, 3):
        copies.plan(("v", "z", k), vec.at[6], vec.at[6 + k], where["z", k])

    def begin(g):
        for kind in (0, 1, 2):
            for j in range(4 if g == 1 else 1):
                copies.go((g, "core", kind, j))
                own[g, kind, j].start()

    def ready(g, kind):
        for j in range(4 if g == 1 else 1):
            own[g, kind, j].wait()
            copies.arrived((g, "core", kind, j))

    def put(target, *refs):
        target[...] = total(*refs).astype(low)

    def cores(g):
        ready(g, 0)
        for k, o in flat:
            here = cut(g, 0, keep, k, o)
            put(here, here, cut(g, 0, core, k, o))
            copies.go((g, "y", k, o))
        ready(g, 1)
        for k in order:
            here = cut(g, 1, keep, k, 1)
            put(here, here, cut(g, 1, core, k, 1))
            copies.go((g, 1, "x", k))
        ready(g, 2)

    def over_y(g, k):
        copies.arrived((g, "y", k, 1))
        here = cut(g, 2, keep, k, 1)
        put(here, here, cut(g, 2, core, k, 1), got_y.at[g, flat.index((k, 1))])
        copies.go((g, 2, "x", k))

    def over_x(g, k):
        copies.arrived((g, 1, "x", k))
        here = cut(g, 1, keep, k, 0)
        put(here, here, cut(g, 1, core, k, 0), got_x.at[g, 0, k])
        copies.go((g, 1, "z", k))
        copies.arrived((g, "y", k, 0))
        copies.arrived((g, 2, "x", k))
        here = cut(g, 2, keep, k, 0)
        put(
            here, here, cut(g, 2, core, k, 0), got_y.at[g, flat.index((k, 0))], got_x.at[g, 1, k]
        )
        copies.go((g, 2, "z", k))

    def over_z(g):
        for s, kind in enumerate((1, 2)):
            copies.arrived((g, kind, "x", 0))
            extra = []
            if kind == 2:
                copies.arrived((g, "y", 0, 0))
                extra = [got_y.at[g, flat.index((0, 0))]]
            for k in (1, 2, 3):
                copies.arrived((g, kind, "z", k))
            put(
                ends.at[g, s, 0], cut(g, kind, keep, 0, 0), cut(g, kind, core, 0, 0),
                got_x.at[g, s, 0], *extra, *(got_z.at[g, s, k] for k in range(3)),
            )
            copies.go((g, kind, "ey"))
            if kind == 2:
                copies.go((g, 2, "ecore"))

    def write(g, s, slot, at):
        value = ends[g, s, slot].astype(jnp.float32)
        for j in range(4):
            if g == 0:
                (rq, rk, rw, ro)[j][:, pl.ds(pl.multiple_of(at, TILE), TILE)] = value[j]
            elif g == 1:
                r1[:, pl.ds(pl.multiple_of(j * W + at, TILE), TILE)] = value[j]
            else:
                r2[j * part : (j + 1) * part, pl.ds(pl.multiple_of(at, TILE), TILE)] = value[j]

    def finish(g):
        copies.arrived((g, 1, "ey"))
        put(ends.at[g, 0, 2], ends.at[g, 0, 0], ends.at[g, 0, 1])
        copies.go((g, 1, "ecore"))
        copies.arrived((g, 2, "ey"))
        copies.go((g, 2, "ediagonal"))
        write(g, 0, 2, lanes(1, True))
        write(g, 1, 0, lanes(2, True))
        write(g, 1, 1, lanes(0, True))

    def close(g):
        copies.arrived((g, 2, "ecore"))
        write(g, 1, 2, lanes(2, False))
        copies.arrived((g, 1, "ecore"))
        write(g, 0, 3, lanes(1, False))
        copies.arrived((g, 2, "ediagonal"))
        write(g, 1, 3, lanes(0, False))

    acts = {"a": cores, "b": over_y, "c": over_x, "d": over_z, "f": finish, "g": close}

    def pump(events):
        for event in events:
            act = acts[event[0]]
            if len(event) == 3:
                act(int(event[1]), int(event[2]))
            else:
                act(int(event[1]))

    greet(where)
    begin(2)
    begin(1)
    for load in loads:
        load.wait()
    x_turned[...] = x_kept[...].T
    pump(BEFORE_BACK)

    @pl.loop(0, 6)
    def _(pair):
        at = pl.ds(pl.multiple_of(pair * TILE, TILE), TILE)
        attend_back_pair(
            key_ids, query_ids, *(held.at[i, :, at] for i in range(4)), lse_ref.at[pair],
            *(grads.at[i, :, at] for i in range(3)), k_turned, k_total, v_total,
        )
        for which, events in enumerate(DURING_BACK):

            @pl.when(pair == which)
            def _():
                pump(events)

    fetch = [pltpu.make_async_copy(w_in.at[i], held.at[i, 0:W, :], load_sem.at[i]) for i in range(3)]
    for copy in fetch:
        copy.start()
    for i in range(3):

        @pl.loop(0, 3)
        def _(block):
            span = pl.ds(pl.multiple_of(block * 256, 256), 256)
            dw[i, span, :] = product(x_turned[span, :], grads[i]).astype(low)

    begin(0)
    vec[0, 0:1, :] = column_sum(grads[0])[None]
    vec[0, 1:2, :] = column_sum(grads[2])[None]
    vec[0, 2:8, :] = sums_in[2:8, :]
    vec[0, 8:12, :] = inner_in[...]
    vec[0, 12:16, :] = jnp.zeros((4, W), jnp.float32)
    copies.go(("v", "core"))
    pump(("a0",))
    copies.arrived(("v", "core"))
    vec[2] = vec[0] + vec[1]
    copies.go(("v", "y"))
    for copy in fetch:
        copy.wait()

    @pl.loop(0, 4)
    def _(block):
        span = pl.ds(pl.multiple_of(block * 256, 256), 256)
        value = gx[span, :]
        for i in range(3):
            value = value + against(grads[i, span, :], held[i, 0:W, :])
        gx[span, :] = value
        for which, events in enumerate(DURING_ROWS):

            @pl.when(block == which)
            def _():
                pump(events)

    copies.arrived(("v", "y"))
    vec[4] = vec[2] + vec[3]
    copies.go(("v", "x"))
    pump(AFTER_ROWS)
    copies.arrived(("v", "x"))
    vec[6] = vec[4] + vec[5]
    for k in (1, 2, 3):
        copies.go(("v", "z", k))
    pump(LAST)
    for k in (1, 2, 3):
        copies.arrived(("v", "z", k))
    rv[...] = (vec[6] + vec[7]) + (vec[8] + vec[9])
    pump(("g2", "g1", "g0"))
    copies.drain()


REDUCE_COPIES = 3 + 3 + 12 + 3 * (8 + 4 + 4 + 3 + 3 + 5) + 6
BEFORE_BACK = ("a2",)
DURING_BACK = (
    ("a1", "b21", "b23",),
    ("b22", "b20", "c21", "c23",),
    ("c22", "b11", "b13",),
    ("b12", "b10", "c11",),
    ("d2", "c13", "c12",),
    ("f2",),
)
DURING_ROWS = (("d1",), ("b01",), ("b03",), ("f1", "b02", "b00",))
AFTER_ROWS = ("c01", "c03", "c02",)
LAST = ("d0", "f0",)


def reduce_attend(
    query, keys, values, grad_mixed, rows, grad_hidden, weights, grad_out, grad_inner, grad_outer,
    lse, key_ids, query_ids, sums, inner_sums,
):
    low, full = jnp.bfloat16, jnp.float32
    count = rows.shape[0]
    part = W // 8
    anywhere, near = pl.BlockSpec(memory_space=pl.ANY), pl.BlockSpec(memory_space=pltpu.VMEM)
    slab = jax.ShapeDtypeStruct((part, W), full)
    piece = (4, part, TILE)
    wide, tall = pltpu.VMEM((3, 4, W, TILE), low), pltpu.VMEM((3, 32, part, TILE), low)
    return pl.pallas_call(
        reduce_attend_kernel,
        out_shape=(
            jax.ShapeDtypeStruct((count, W), full),
            slab,
            slab,
            slab,
            slab,
            jax.ShapeDtypeStruct((part, 4 * W), full),
            jax.ShapeDtypeStruct((4 * part, W), full),
            jax.ShapeDtypeStruct((16, W), full),
        ),
        in_specs=[anywhere] * 10 + [near] * 5,
        out_specs=[near] * 8,
        scratch_shapes=[
            pltpu.VMEM((4, count, W), low),
            pltpu.VMEM((count, W), low),
            pltpu.VMEM((W, count), low),
            pltpu.VMEM((3, count, W), low),
            pltpu.VMEM((4, W, W), low),
            pltpu.VMEM((TILE, count), low),
            pltpu.VMEM((count, TILE), full),
            pltpu.VMEM((count, TILE), full),
            wide,
            wide,
            tall,
            wide,
            wide,
            tall,
            pltpu.VMEM((3, 8) + piece, low),
            pltpu.VMEM((3, 2, 4) + piece, low),
            pltpu.VMEM((3, 2, 3) + piece, low),
            pltpu.VMEM((3, 2, 4) + piece, low),
            pltpu.VMEM((10, 16, W), full),
            pltpu.SemaphoreType.DMA((REDUCE_COPIES,)),
            pltpu.SemaphoreType.DMA((REDUCE_COPIES,)),
            pltpu.SemaphoreType.DMA((7,)),
            pltpu.SemaphoreType.DMA((18,)),
        ],
        compiler_params=pltpu.CompilerParams(
            collective_id=1, has_side_effects=True, vmem_limit_bytes=62 << 20
        ),
        name="reduce_attend",
    )(
        query, keys, values, grad_mixed, rows, grad_hidden, weights, grad_out, grad_inner,
        grad_outer.reshape(32, part, W), lse, key_ids, query_ids, sums, inner_sums,
    )


def normalise(value):
    mean = jnp.mean(value, axis=1, keepdims=True)
    centred = value - mean
    scale = lax.rsqrt(jnp.mean(centred * centred, axis=1, keepdims=True) + 1e-05)
    return centred * scale, scale


def normalise_back(grad, unit, scale):
    middle = jnp.mean(grad, axis=1, keepdims=True)
    along = jnp.mean(grad * unit, axis=1, keepdims=True)
    return scale * (grad - middle - unit * along)


def chain_kernel(
    mixed_ref, rows_ref, pull_ref, wo_ref, w1_ref, w2_ref, small_ref, b1_ref,
    out_ref, y1_ref, u_ref, gz_ref, gf_ref, gh_ref, ga_ref, gmix_ref, sums_ref, b1_sum_ref,
    slope_ref,
):
    low = jnp.bfloat16

    @pl.when(pl.program_id(0) == 0)
    def _():
        sums_ref[...] = jnp.zeros_like(sums_ref)
        b1_sum_ref[...] = jnp.zeros_like(b1_sum_ref)

    def small(i):
        return small_ref[i : i + 1, :]

    def gather_sum(ref, i, value):
        ref[i : i + 1, :] += jnp.sum(value, axis=0, keepdims=True)

    hidden = rows_ref[...].astype(jnp.float32) + product(mixed_ref[...], wo_ref[0]) + small(2)
    unit_one, scale_one = normalise(hidden)
    y1 = unit_one * small(3) + small(4)
    y1_low = y1.astype(low)
    y1_ref[...] = y1_low
    second = y1 + small(5)
    for r in range(4):
        inner = product(y1_low, w1_ref[r]) + b1_ref[r : r + 1, :]
        active, slope = gelu_and_slope(inner)
        active = active.astype(low)
        u_ref[:, r * W : (r + 1) * W] = active
        slope_ref[:, r * W : (r + 1) * W] = slope
        second = second + product(active, w2_ref[r * W : (r + 1) * W, :])
    unit_two, scale_two = normalise(second)
    out_ref[...] = (unit_two * small(6) + small(7)).astype(low)
    pull = pull_ref[...].astype(jnp.float32)
    gather_sum(sums_ref, 6, pull * unit_two)
    gather_sum(sums_ref, 7, pull)
    grad_second = normalise_back(pull * small(6), unit_two, scale_two)
    gz = grad_second.astype(low)
    gz_ref[...] = gz
    gather_sum(sums_ref, 5, gz.astype(jnp.float32))
    grad_y1 = grad_second
    for r in range(4):
        gf = against(gz, w2_ref[r * W : (r + 1) * W, :]) * slope_ref[:, r * W : (r + 1) * W]
        gf = gf.astype(low)
        gf_ref[:, r * W : (r + 1) * W] = gf
        gather_sum(b1_sum_ref, r, gf.astype(jnp.float32))
        grad_y1 = grad_y1 + against(gf, w1_ref[r])
    gather_sum(sums_ref, 3, grad_y1 * unit_one)
    gather_sum(sums_ref, 4, grad_y1)
    grad_hidden = normalise_back(grad_y1 * small(3), unit_one, scale_one)
    gh_ref[...] = grad_hidden
    ga = grad_hidden.astype(low)
    ga_ref[...] = ga
    gather_sum(sums_ref, 2, ga.astype(jnp.float32))
    gmix_ref[...] = against(ga, wo_ref[0]).astype(low)


def chain(mixed, rows, pull, weights, inner_blocks, outer_mat, small, inner_bias):
    count, width = rows.shape
    step = 256
    low, full = jnp.bfloat16, jnp.float32
    thin = pl.BlockSpec((step, width), lambda i: (i, 0))
    fat = pl.BlockSpec((step, 4 * width), lambda i: (i, 0))
    held = lambda shape: pl.BlockSpec(shape, lambda i: (0,) * len(shape))
    once = pl.Buffered(1)
    return pl.pallas_call(
        chain_kernel,
        grid=(count // step,),
        out_shape=(
            jax.ShapeDtypeStruct((count, width), low),
            jax.ShapeDtypeStruct((count, width), low),
            jax.ShapeDtypeStruct((count, 4 * width), low),
            jax.ShapeDtypeStruct((count, width), low),
            jax.ShapeDtypeStruct((count, 4 * width), low),
            jax.ShapeDtypeStruct((count, width), full),
            jax.ShapeDtypeStruct((count, width), low),
            jax.ShapeDtypeStruct((count, width), low),
            jax.ShapeDtypeStruct((8, width), full),
            jax.ShapeDtypeStruct((4, width), full),
        ),
        in_specs=[
            thin, thin, thin,
            pl.BlockSpec((1, width, width), lambda i: (3, 0, 0), pipeline_mode=once),
            pl.BlockSpec((4, width, width), lambda i: (0, 0, 0), pipeline_mode=once),
            pl.BlockSpec((4 * width, width), lambda i: (0, 0), pipeline_mode=once),
            held((8, width)), held((4, width)),
        ],
        out_specs=[thin, thin, fat, thin, fat, thin, thin, thin, held((8, width)), held((4, width))],
        scratch_shapes=[pltpu.VMEM((step, 4 * width), full)],
        compiler_params=pltpu.CompilerParams(vmem_limit_bytes=60 << 20),
        name="chain",
    )(mixed, rows, pull, weights, inner_blocks, outer_mat, small, inner_bias)


def on_device(
    tokens,
    read_memory,
    doc_ids,
    w_query,
    w_key,
    w_value,
    w_out,
    query_bias,
    value_bias,
    out_bias,
    norm_one_gain,
    norm_one_bias,
    w_inner,
    inner_bias,
    w_outer,
    outer_bias,
    norm_two_gain,
    norm_two_bias,
    out_grad,
):
    owners = lax.axis_size("fsdp")
    wide = owners == 8 and lax.axis_size("rep") == 4
    part = w_query.shape[0]
    low = jnp.bfloat16
    small = pack(
        jnp.stack(
            [
                query_bias, value_bias, out_bias, norm_one_gain,
                norm_one_bias, outer_bias, norm_two_gain, norm_two_bias,
            ]
        )[None],
        inner_bias[None],
    )[0]
    seqs, seg = doc_ids.shape
    width = tokens.shape[1]
    mem = read_memory.shape[0] // seqs
    length = seg + 2 * mem
    memory_rows = read_memory.reshape(seqs, mem, width)
    rows = jnp.concatenate([tokens.reshape(seqs, seg, width), memory_rows, memory_rows], axis=1)
    rows = rows.reshape(seqs * length, width)
    marks = jnp.full((seqs, 2 * mem), -1, jnp.int32)
    ids = jnp.concatenate([doc_ids, marks], axis=1)
    out_rows = out_grad.reshape(seqs, length, width)
    out_rows = jnp.concatenate(
        [out_rows[:, mem : mem + seg], out_rows[:, :mem], out_rows[:, mem + seg :]], axis=1
    ).reshape(seqs * length, width)

    def each(function, *arrays):
        results = []
        for s in range(seqs):
            own = slice(s * length, (s + 1) * length)
            spread = jnp.broadcast_to(ids[s][:, None], (length, TILE))
            by_block = ids[s].reshape(length // TILE, TILE)
            results.append(function(spread, by_block, *[a[own] for a in arrays]))
        return results

    shards = (w_query, w_key, w_value, w_out, w_inner, w_outer, small)
    wide = wide and seqs == 1
    if wide:
        spread, by_block = each(lambda *a: a)[0]
        weights, inner_blocks, outer_mat, vectors, inner_shift, query, keys, values, mixed, sums = (
            gather_attend(shards, rows, spread, by_block)
        )
        pairs = [(mixed, sums)]
    else:
        weights, inner_blocks, outer_mat, packed = plain_gather(*shards)
        vectors, inner_shift = unpack(packed.astype(jnp.float32), part)
        query = (product(rows, weights[0]) + vectors[0]).astype(low)
        keys = product(rows, weights[1]).astype(low)
        values = (product(rows, weights[2]) + vectors[1]).astype(low)
        pairs = each(attend, query, keys, values)
        mixed = jnp.concatenate([pair[0] for pair in pairs], axis=0)
    output, normed, active, grad_outer, grad_inner, grad_residual, grad_branch, grad_mixed, sums, inner_sums = chain(
        mixed, rows, out_rows, weights, inner_blocks, outer_mat, vectors, inner_shift
    )
    grad_w_outer = inner_rows(active, grad_outer).astype(low)
    grad_w_inner = inner_rows(normed, grad_inner).astype(low)
    grad_w_out = inner_rows(mixed, grad_branch).astype(low)
    if wide:
        grad_rows, *shares, joined = reduce_attend(
            query, keys, values, grad_mixed, rows, grad_residual, weights, grad_w_out,
            grad_w_inner, grad_w_outer, pairs[0][1], spread, by_block, sums, inner_sums,
        )
        place_of = lax.axis_index("fsdp")
        last = lax.dynamic_slice(joined[:8], (0, place_of * part), (8, part))
        last_inner = lax.dynamic_slice(
            joined[8:12].reshape(-1), (place_of * 4 * part,), (4 * part,)
        )
    else:
        triples = [
            attend_back(spread, by_block, q, k, v, g, pairs[s][1])
            for s, (spread, by_block, q, k, v, g) in enumerate(
                each(lambda *a: a, query, keys, values, grad_mixed)
            )
        ]
        grad_query_low, grad_keys_low, grad_values_low = (
            jnp.concatenate([triple[i] for triple in triples], axis=0) for i in range(3)
        )
        grad_w_query = inner_rows(rows, grad_query_low).astype(low)
        grad_w_key = inner_rows(rows, grad_keys_low).astype(low)
        grad_w_value = inner_rows(rows, grad_values_low).astype(low)
        sums = jnp.concatenate(
            [column_sum(grad_query_low)[None], column_sum(grad_values_low)[None], sums[2:]], axis=0
        )
        grad_rows = (
            grad_residual
            + against(grad_query_low, weights[0])
            + against(grad_keys_low, weights[1])
            + against(grad_values_low, weights[2])
        )
        *shares, share_small = plain_reduce(
            grad_w_query,
            grad_w_key,
            grad_w_value,
            grad_w_out,
            grad_w_inner,
            grad_w_outer,
            pack(
                sums.reshape(8, owners, part).transpose(1, 0, 2),
                inner_sums.reshape(owners, 4 * part),
            ),
        )
        last, last_inner = unpack(share_small[None], part)
    grad_rows = grad_rows.reshape(seqs, length, width)
    grad_tokens = grad_rows[:, :seg].reshape(seqs * seg, width).astype(jnp.bfloat16)
    grad_memory = (
        (grad_rows[:, seg : seg + mem] + grad_rows[:, seg + mem :])
        .reshape(seqs * mem, width)
        .astype(jnp.bfloat16)
    )
    layer_out = output.reshape(seqs, length, width)
    layer_out = jnp.concatenate(
        [layer_out[:, seg : seg + mem], layer_out[:, :seg], layer_out[:, seg + mem :]], axis=1
    ).reshape(seqs * length, width)
    return (
        layer_out,
        grad_tokens,
        grad_memory,
        *shares[:4],
        *(last[i] for i in range(5)),
        shares[4],
        last_inner.reshape(-1),
        shares[5],
        *(last[i] for i in range(5, 8)),
    )


def solution(mesh):
    return jax.shard_map(
        on_device,
        mesh=mesh,
        in_specs=(
            P(("rep", "fsdp"), None),
            P(("rep", "fsdp"), None),
            P(("rep", "fsdp"), None),
            P("fsdp", None),
            P("fsdp", None),
            P("fsdp", None),
            P("fsdp", None),
            P("fsdp"),
            P("fsdp"),
            P("fsdp"),
            P("fsdp"),
            P("fsdp"),
            P("fsdp", None),
            P("fsdp"),
            P("fsdp", None),
            P("fsdp"),
            P("fsdp"),
            P("fsdp"),
            P(("rep", "fsdp"), None),
        ),
        out_specs=(
            P(("rep", "fsdp"), None),
            P(("rep", "fsdp"), None),
            P(("rep", "fsdp"), None),
            P("fsdp", None),
            P("fsdp", None),
            P("fsdp", None),
            P("fsdp", None),
            P("fsdp"),
            P("fsdp"),
            P("fsdp"),
            P("fsdp"),
            P("fsdp"),
            P("fsdp", None),
            P("fsdp"),
            P("fsdp", None),
            P("fsdp"),
            P("fsdp"),
            P("fsdp"),
        ),
        check_vma=False,
    )
```

```python
import functools
import math

import jax
import jax.numpy as jnp
from jax import lax
from jax.experimental import pallas as pl
from jax.experimental.pallas import tpu as pltpu
from jax.sharding import PartitionSpec as P

MESH_ID = pl.DeviceIdType.MESH
W = 768


def only_if(condition, act):
    if condition is None:
        act()
    else:
        pl.when(condition)(act)


class Copies:
    def __init__(self, send, recv):
        self.send, self.recv, self.made = send, recv, {}

    def plan(self, name, src, dst, to, leaves=None, comes=None):
        slot = len(self.made)

        def describe(src):
            return pltpu.make_async_remote_copy(
                src_ref=src,
                dst_ref=dst,
                send_sem=self.send.at[slot],
                recv_sem=self.recv.at[slot],
                device_id=to,
                device_id_type=MESH_ID,
            )

        self.made[name] = (describe, src, leaves, comes)

    def go(self, name):
        describe, src, leaves, _ = self.made[name]
        only_if(leaves, lambda: describe(src).start())

    def start(self, name, src, dst, to):
        self.plan(name, src, dst, to)
        self.go(name)

    def arrived(self, name):
        describe, src, _, comes = self.made[name]
        only_if(comes, lambda: describe(src).wait_recv())

    def drain(self):
        for describe, src, leaves, _ in self.made.values():
            only_if(leaves, functools.partial(lambda describe, src: describe(src).wait_send(), describe, src))


def place():
    rep, owner = lax.axis_index("rep"), lax.axis_index("fsdp")
    y, c, z, x = rep // 2, rep % 2, owner // 2, owner % 2
    where = {
        "core": (y * 2 + 1 - c, owner),
        "y": ((1 - y) * 2 + c, owner),
        "x": (rep, z * 2 + 1 - x),
    }
    for k in (1, 2, 3):
        where["z", k] = (rep, ((z + k) % 4) * 2 + x)
        where["zx", k] = (rep, ((z + k) % 4) * 2 + 1 - x)
    return rep, owner, y, c, z, x, where


def greet(where):
    barrier = pltpu.get_barrier_semaphore()
    for to in where.values():
        pl.semaphore_signal(barrier, inc=1, device_id=to, device_id_type=MESH_ID)
    pl.semaphore_wait(barrier, len(where))


def total(*refs):
    value = refs[0][...].astype(jnp.float32)
    for ref in refs[1:]:
        value = value + ref[...].astype(jnp.float32)
    return value


def inner_lines(part):
    return -(-4 * part // 128)


def pack(vectors, inner):
    owners, _, part = vectors.shape
    lines = inner_lines(part)
    first = jnp.pad(vectors, ((0, 0), (0, 0), (0, 128 - part)))
    second = jnp.pad(inner, ((0, 0), (0, lines * 128 - 4 * part)))
    second = second.reshape(owners, lines, 128)
    return jnp.pad(jnp.concatenate([first, second], axis=1), ((0, 0), (0, 8 - lines), (0, 0)))


def unpack(packed, part):
    owners = packed.shape[0]
    lines = inner_lines(part)
    first = packed[:, :8, :part].transpose(1, 0, 2).reshape(8, owners * part)
    second = packed[:, 8 : 8 + lines].reshape(owners, lines * 128)[:, : 4 * part]
    return first, second.reshape(4, owners * part)


def plain_gather(wq, wk, wv, wo, inner, outer, vectors):
    gathered = lax.all_gather(inner, "fsdp", axis=0, tiled=True)
    return (
        lax.all_gather(jnp.stack([wq, wk, wv, wo]), "fsdp", axis=1, tiled=True),
        gathered.reshape(W, 4, W).transpose(1, 0, 2),
        lax.all_gather(outer, "fsdp", axis=0, tiled=True),
        lax.all_gather(vectors, "fsdp", axis=0),
    )


def plain_reduce(*grads):
    def over_all(value):
        part = lax.psum_scatter(value, "fsdp", scatter_dimension=0, tiled=True)
        return lax.psum(part, "rep").astype(jnp.float32)

    return tuple(over_all(grad) for grad in grads[:-1]) + (over_all(grads[-1])[0],)


def product(left, right):
    return jnp.dot(left, right, preferred_element_type=jnp.float32)


def inner_rows(left, right):
    return lax.dot_general(
        left, right, (((0,), (0,)), ((), ())), preferred_element_type=jnp.float32
    )


def against(left, right):
    return lax.dot_general(
        left, right, (((1,), (1,)), ((), ())), preferred_element_type=jnp.float32
    )


def column_sum(values):
    return jnp.sum(values.astype(jnp.float32), axis=0)


TILE = 128
HEAD_DIM = 64
FACTOR = HEAD_DIM ** (-0.5)
HIDDEN = -1e30


def spans(i, count):
    last = count - 1
    if i == last:
        return [(0, count * TILE)]
    low, high = max(0, i - 2), min(last, i + 2)
    if high == last:
        return [(low * TILE, count * TILE)]
    return [(low * TILE, (high + 1) * TILE), (last * TILE, count * TILE)]


def two_heads(block):
    lanes = lax.broadcasted_iota(jnp.int32, block.shape, 1)
    zero = jnp.zeros_like(block)
    first = jnp.where(lanes < HEAD_DIM, block, zero)
    second = jnp.where(lanes < HEAD_DIM, zero, block)
    return jnp.concatenate([first, second], axis=0)


def own_head(value):
    rows = lax.broadcasted_iota(jnp.int32, (TILE, TILE), 0)
    return jnp.where(rows < HEAD_DIM, value[:, :TILE], value[:, TILE:]).T


def masked_scores(k_ref, key_ids, query_ids, stacked, i, span, count):
    low, high = span
    scores = against(k_ref[low:high, :], stacked)
    ids = key_ids[low:high, :]
    row = query_ids[i : i + 1, :]
    seen = ids == row
    if high == count * TILE:
        seen = seen | (ids < 0)
    if i == count - 1:
        seen = seen | (row < 0)
    return jnp.concatenate(
        [jnp.where(seen, scores[:, :TILE], HIDDEN), jnp.where(seen, scores[:, TILE:], HIDDEN)], axis=1
    )


def attend_kernel(key_ids, query_ids, q_ref, k_ref, v_ref, out_ref, lse_ref, v_turned):
    attend_pair(key_ids, query_ids, q_ref, k_ref, v_ref, out_ref, lse_ref.at[0], v_turned)


def attend_pair(
    key_ids, query_ids, q_ref, k_ref, v_ref, out_ref, lse_ref, v_turned, middle=lambda: None
):
    count = q_ref.shape[0] // TILE
    v_turned[...] = v_ref[:, :].T
    for i in range(count):
        rows = slice(i * TILE, (i + 1) * TILE)
        stacked = two_heads(q_ref[rows, :] * jnp.bfloat16(FACTOR))
        parts = spans(i, count)
        scores = [masked_scores(k_ref, key_ids, query_ids, stacked, i, p, count) for p in parts]
        peak = functools.reduce(
            jnp.maximum, [jnp.max(s, axis=0, keepdims=True) for s in scores]
        )
        weights = [jnp.exp(s - peak) for s in scores]
        total = sum(jnp.sum(w, axis=0, keepdims=True) for w in weights)
        mixed = sum(
            product(v_turned[:, low:high], w.astype(jnp.bfloat16)) for (low, high), w in zip(parts, weights)
        )
        out_ref[rows, :] = own_head(mixed * (1.0 / total)).astype(jnp.bfloat16)
        lse_ref[i : i + 1, :] = peak + jnp.log(total)
        if i == count // 2 - 1:
            middle()


def attend_back_kernel(
    key_ids, query_ids, q_ref, k_ref, v_ref, g_ref, lse_ref, gq_ref, gk_ref, gv_ref,
    k_turned, k_total, v_total,
):
    attend_back_pair(
        key_ids, query_ids, q_ref, k_ref, v_ref, g_ref, lse_ref.at[0], gq_ref, gk_ref, gv_ref,
        k_turned, k_total, v_total,
    )


def attend_back_pair(
    key_ids, query_ids, q_ref, k_ref, v_ref, g_ref, lse_ref, gq_ref, gk_ref, gv_ref,
    k_turned, k_total, v_total, middle=lambda: None,
):
    count = q_ref.shape[0] // TILE
    k_turned[...] = k_ref[:, :].T
    k_total[...] = jnp.zeros_like(k_total)
    v_total[...] = jnp.zeros_like(v_total)
    for i in range(count):
        rows = slice(i * TILE, (i + 1) * TILE)
        stacked = two_heads(q_ref[rows, :] * jnp.bfloat16(FACTOR))
        grads = two_heads(g_ref[rows, :])
        lse = lse_ref[i : i + 1, :]
        parts = spans(i, count)
        probs, pulls = [], []
        for low, high in parts:
            scores = masked_scores(k_ref, key_ids, query_ids, stacked, i, (low, high), count)
            p = jnp.exp(scores - lse)
            v_total[low:high, :] += product(p.astype(jnp.bfloat16), grads)
            probs.append(p)
            pulls.append(against(v_ref[low:high, :], grads))
        centre = sum(jnp.sum(p * g, axis=0, keepdims=True) for p, g in zip(probs, pulls))
        mixed = 0.0
        for (low, high), p, g in zip(parts, probs, pulls):
            turned = (p * (g - centre)).astype(jnp.bfloat16)
            k_total[low:high, :] += product(turned, stacked)
            mixed = mixed + product(k_turned[:, low:high], turned)
        gq_ref[rows, :] = (own_head(mixed) * FACTOR).astype(jnp.bfloat16)
        if i == count // 2 - 1:
            middle()
    gk_ref[:, :] = k_total[...].astype(jnp.bfloat16)
    gv_ref[:, :] = v_total[...].astype(jnp.bfloat16)


def attend(key_ids, query_ids, query, keys, values):
    rows, width = query.shape
    pair = 2 * HEAD_DIM
    count = rows // TILE
    column = pl.BlockSpec((rows, pair), lambda h: (0, h))
    whole = lambda a: pl.BlockSpec(a.shape, lambda h: (0, 0))
    return pl.pallas_call(
        attend_kernel,
        grid=(width // pair,),
        out_shape=(
            jax.ShapeDtypeStruct((rows, width), jnp.bfloat16),
            jax.ShapeDtypeStruct((width // pair, count, 2 * TILE), jnp.float32),
        ),
        in_specs=[whole(key_ids), whole(query_ids), column, column, column],
        out_specs=[column, pl.BlockSpec((1, count, 2 * TILE), lambda h: (h, 0, 0))],
        scratch_shapes=[pltpu.VMEM((pair, rows), jnp.bfloat16)],
        compiler_params=pltpu.CompilerParams(vmem_limit_bytes=48 << 20),
        name="attend",
    )(key_ids, query_ids, query, keys, values)


def gather_attend_kernel(
    wq, wk, wv, wo, w1, w2, vec, x_ref, key_ids, query_ids,
    o0, o1, o2, small, inner, q_ref, k_ref, v_ref, out_ref, lse_ref,
    w0, a1, a2, av, got, v_turned, send, recv, own_sem, load_sem,
):
    rep, owner, y, c, z, x, where = place()
    part = W // 8
    low = jnp.bfloat16
    across = (1 - y) * 2 + c
    mine0 = pl.ds(owner * part, part)
    loads = [
        pltpu.make_async_copy(source, into, load_sem.at[i])
        for i, (source, into) in enumerate(
            [(source, w0.at[i, mine0, :]) for i, source in enumerate((wq, wk, wv, wo))]
            + [(w1.at[:, i * W : (i + 1) * W], a1.at[i]) for i in range(4)]
            + [(w2, a2), (vec, av)]
        )
    ]
    for load in loads:
        load.start()

    near = (z + 3) % 4 - 2 * ((3 - z) // 3)
    far = 3 * (1 - z // 2)
    owners_z = (z, near, 6 - z - near - far, far)

    def shard(turn, other_x):
        return owners_z[turn] * 2 + (1 - x if other_x else x)

    def spot(g, kind, turn, other_x, quarter):
        at = 2 * TILE + quarter * TILE if kind else c * TILE
        lanes = pl.ds(pl.multiple_of(at, TILE), TILE)
        if g == 2:
            return o2.at[pl.ds(shard(turn, other_x) * 4 * part, 4 * part), lanes]
        return (w0, o1)[g].at[:, pl.ds(shard(turn, other_x) * part, part), lanes]

    greet(where)
    for load in loads:
        load.wait()
    own = [
        pltpu.make_async_copy(a1, o1.at[:, mine0, :], own_sem.at[0]),
        pltpu.make_async_copy(a2, o2.at[pl.ds(owner * 4 * part, 4 * part), :], own_sem.at[1]),
    ]
    kept = pltpu.make_async_copy(w0, o0, own_sem.at[2])
    note = pltpu.make_async_copy(av, got.at[owner], own_sem.at[3])
    copies = Copies(send, recv)

    for k in (1, 2, 3):
        copies.start(("v", "z", k), av, got.at[owner], where["z", k])
        copies.start(("v", "zx", k), av, got.at[owner], where["zx", k])
    copies.start(("v", "x", 0), av, got.at[owner], where["x"])
    for g in (0, 1, 2):
        for kind in (1, 0):
            at = 2 * TILE + rep * TILE if kind else c * TILE
            lanes = pl.ds(pl.multiple_of(at, TILE), TILE)
            source = (w0.at[:, mine0, lanes], a1.at[:, :, lanes], a2.at[:, lanes])[g]
            here = spot(g, kind, 0, False, rep)
            copies.plan((g, kind, "x", 0), source, here, where["x"])
            for start, end, turn in Z_ROUTES:
                through = (rep, end * 2 + x)
                relayed = turn == 3 and start in (1, 2) and end in (0, 3)
                from_here = spot(g, kind, 3, False, rep) if relayed else source
                into = spot(g, kind, 3, False, rep) if relayed else here
                copies.plan(
                    (g, kind, "z", start, end, turn), from_here, into, through, z == start, z == end
                )
    steps = [
        (0, True, "x"), (1, False, "z"), (2, False, "z"), (1, True, "x"),
        (3, False, "z"), (2, True, "x"), (3, True, "x"),
    ]
    for g in (0, 1, 2):
        for turn, other_x, stage in steps:
            for kind in (0, 1):
                here = spot(g, kind, turn, other_x, rep)
                if stage == "z":
                    copies.plan((g, kind, "x", turn), here, here, where["x"])
                if kind:
                    copies.plan((g, "y", turn, other_x), here, here, where["y"])
                    there = spot(g, kind, turn, other_x, across)
                    copies.plan((g, "diagonal", turn, other_x), there, there, where["core"])
                copies.plan((g, kind, "core", turn, other_x), here, here, where["core"])

    def begin(g, turns):
        for start, end, turn in Z_ROUTES:
            if turn in turns and not (turn == 3 and start in (1, 2)):
                for kind in (1, 0):
                    copies.go((g, kind, "z", start, end, turn))

    copies.go((0, 1, "x", 0))
    copies.go((0, 0, "x", 0))
    for g in (0, 1, 2):
        begin(g, (1, 2, 3))
    note.start()
    for copy in own:
        copy.start()

    def pass_on(g, step):
        turn, other_x, stage = steps[step]
        for kind in (1, 0):
            if stage == "x":
                copies.arrived((g, kind, "x", turn))
            else:
                for start, end, at_turn in Z_ROUTES:
                    if at_turn == turn:
                        copies.arrived((g, kind, "z", start, end, turn))
                if turn == 3:
                    copies.go((g, kind, "z", 1, 0, 3))
                    copies.go((g, kind, "z", 2, 3, 3))
                copies.go((g, kind, "x", turn))
            if kind:
                copies.go((g, "y", turn, other_x))
            copies.go((g, kind, "core", turn, other_x))
        if step == 4 and g < 2:
            for kind in (1, 0):
                copies.go((g + 1, kind, "x", 0))

    def pass_core(g, step):
        turn, other_x, _ = steps[step]
        copies.arrived((g, "y", turn, other_x))
        copies.go((g, "diagonal", turn, other_x))

    def settle(g):
        for k, other_x, _ in steps:
            copies.arrived((g, 0, "core", k, other_x))
            copies.arrived((g, 1, "core", k, other_x))
            copies.arrived((g, "diagonal", k, other_x))

    def pump(events):
        for kind, g, step in events:
            (pass_core if kind == "c" else pass_on)(g, step)

    pump(EARLY)
    settle(0)
    for k in (1, 2, 3):
        copies.arrived(("v", "z", k))
        copies.arrived(("v", "zx", k))
    copies.arrived(("v", "x", 0))
    note.wait()
    kept.start()

    lanes = lax.broadcasted_iota(jnp.int32, (TILE, W), 1)
    rows = lax.broadcasted_iota(jnp.int32, (TILE, W), 0)
    joined = jnp.zeros((16, W), jnp.float32)
    for o in range(8):
        pick = ((lanes == rows + o * part) & (rows < part)).astype(low)
        joined = joined + product(got[o], pick)
        for j in range(3):
            i = o * 3 + j
            inner[i // 6 : i // 6 + 1, (i % 6) * TILE : (i % 6 + 1) * TILE] = got[
                o, 8 + j : 9 + j, :
            ].astype(jnp.float32)
    small[...] = joined[:8]

    @pl.loop(0, 4)
    def _(block):
        span = pl.ds(pl.multiple_of(block * 256, 256), 256)
        value = x_ref[span, :]
        q_ref[span, :] = (product(value, w0[0]) + small[0:1, :]).astype(low)
        k_ref[span, :] = product(value, w0[1]).astype(low)
        v_ref[span, :] = (product(value, w0[2]) + small[1:2, :]).astype(low)
        for which, events in enumerate(DURING_PROJECTIONS):

            @pl.when(block == which)
            def _():
                pump(events)

    def at_half(pair, half):
        for which, events in enumerate(DURING_ATTENTION[half::2]):
            if events:
                pl.when(pair == which)(functools.partial(pump, events))

    @pl.loop(0, 6)
    def _(pair):
        columns = pl.ds(pl.multiple_of(pair * TILE, TILE), TILE)
        attend_pair(
            key_ids, query_ids, q_ref.at[:, columns], k_ref.at[:, columns], v_ref.at[:, columns],
            out_ref.at[:, columns], lse_ref.at[pair], v_turned, lambda: at_half(pair, 0),
        )
        at_half(pair, 1)

    pump(LATE)
    settle(1)
    settle(2)
    copies.drain()
    for copy in own:
        copy.wait()
    kept.wait()


Z_ROUTES = (
    (0, 1, 1), (1, 0, 1), (1, 2, 1), (2, 3, 1), (2, 1, 2), (3, 2, 2), (1, 3, 2), (2, 0, 2),
    (0, 2, 3), (3, 1, 3), (1, 0, 3), (2, 3, 3),
)
GATHER_COPIES = 7 + 3 * (2 * (1 + 12) + 2 * 3 + 7 * 4)


def run(g, *order):
    return [(name[0], g, int(name[1])) for name in order]


EARLY = run(0, "p0", "p1", "p2", "c0", "p3", "p4", "c1", "p5", "c2", "p6", "c3", "c4", "c5", "c6")
DURING_PROJECTIONS = [run(1, "p0"), run(1, "p1"), run(1, "p2", "c0"), run(1, "p3", "c1")]
DURING_ATTENTION = [
    run(1, "p4"),
    run(1, "c2"),
    run(1, "p5", "c3", "p6"),
    run(2, "p0") + run(1, "c4"),
    run(2, "p1"),
    run(1, "c5", "c6"),
    run(2, "p2", "c0"),
    run(2, "p3"),
    run(2, "c1"),
    run(2, "p4"),
    run(2, "c2", "p5"),
    run(2, "c3"),
]
LATE = run(2, "p6", "c4", "c5", "c6")


def gather_attend(shards, rows, key_ids, query_ids):
    low, full = jnp.bfloat16, jnp.float32
    count = rows.shape[0]
    vectors = shards[-1]
    anywhere, near = pl.BlockSpec(memory_space=pl.ANY), pl.BlockSpec(memory_space=pltpu.VMEM)
    thin = jax.ShapeDtypeStruct((count, W), low)
    return pl.pallas_call(
        gather_attend_kernel,
        out_shape=(
            jax.ShapeDtypeStruct((4, W, W), low),
            jax.ShapeDtypeStruct((4, W, W), low),
            jax.ShapeDtypeStruct((4 * W, W), low),
            jax.ShapeDtypeStruct((8, W), full),
            jax.ShapeDtypeStruct((4, W), full),
            thin,
            thin,
            thin,
            thin,
            jax.ShapeDtypeStruct((W // TILE, count // TILE, 2 * TILE), full),
        ),
        in_specs=[anywhere] * 7 + [near] * 3,
        out_specs=[anywhere] * 3 + [near] * 7,
        scratch_shapes=[
            pltpu.VMEM((4, W, W), low),
            pltpu.VMEM((4, W // 8, W), low),
            pltpu.VMEM(shards[5].shape, low),
            pltpu.VMEM(vectors.shape, low),
            pltpu.VMEM((8,) + vectors.shape, low),
            pltpu.VMEM((TILE, count), low),
            pltpu.SemaphoreType.DMA((GATHER_COPIES,)),
            pltpu.SemaphoreType.DMA((GATHER_COPIES,)),
            pltpu.SemaphoreType.DMA((4,)),
            pltpu.SemaphoreType.DMA((10,)),
        ],
        compiler_params=pltpu.CompilerParams(
            collective_id=0, has_side_effects=True, vmem_limit_bytes=48 << 20
        ),
        name="gather_attend",
    )(*shards, rows, key_ids, query_ids)


def attend_back(key_ids, query_ids, query, keys, values, grads, lse):
    rows, width = query.shape
    pair = 2 * HEAD_DIM
    count = rows // TILE
    column = pl.BlockSpec((rows, pair), lambda h: (0, h))
    whole = lambda a: pl.BlockSpec(a.shape, lambda h: (0, 0))
    return pl.pallas_call(
        attend_back_kernel,
        grid=(width // pair,),
        out_shape=(jax.ShapeDtypeStruct((rows, width), jnp.bfloat16),) * 3,
        in_specs=[whole(key_ids), whole(query_ids)]
        + [column] * 4
        + [pl.BlockSpec((1, count, 2 * TILE), lambda h: (h, 0, 0))],
        out_specs=[column] * 3,
        scratch_shapes=[
            pltpu.VMEM((pair, rows), jnp.bfloat16),
            pltpu.VMEM((rows, pair), jnp.float32),
            pltpu.VMEM((rows, pair), jnp.float32),
        ],
        compiler_params=pltpu.CompilerParams(vmem_limit_bytes=48 << 20),
        name="attend_back",
    )(key_ids, query_ids, query, keys, values, grads, lse)


ERFC_TERMS = (
    -1.26551223, 1.00002368, 0.37409196, 0.09678418, -0.18628806,
    0.27886807, -1.13520398, 1.48851587, -0.82215223, 0.17087277,
)


def gelu_and_slope(value):
    half_square = value * value * 0.5
    step = 1.0 / (1.0 + jnp.abs(value) * (0.5 * 0.5**0.5))
    power = ERFC_TERMS[-1]
    for term in ERFC_TERMS[-2::-1]:
        power = power * step + term
    tail = 0.5 * step * jnp.exp(power - half_square)
    cover = jnp.where(value < 0, tail, 1.0 - tail)
    density = jnp.exp(-half_square) * ((0.5 / math.pi) ** 0.5)
    return value * cover, cover + value * density


def reduce_attend_kernel(
    q_in, k_in, v_in, g_in, x_in, gh_in, w_in, go, g1, g2, lse_ref, key_ids, query_ids, sums_in,
    inner_in, gx, rq, rk, rw, ro, r1, r2, rv,
    held, x_kept, x_turned, grads, dw, k_turned, k_total, v_total,
    keep0, keep1, keep2, core0, core1, core2, got_y, got_x, got_z, ends, vec,
    send, recv, load_sem, own_sem,
):
    rep, owner, y, c, z, x, where = place()
    part = W // 8
    low = jnp.bfloat16
    loads = [
        pltpu.make_async_copy(source, into, load_sem.at[i])
        for i, (source, into) in enumerate(
            [(source, held.at[i]) for i, source in enumerate((q_in, k_in, v_in, g_in))]
            + [(x_in, x_kept), (gh_in, gx), (go, dw.at[3])]
        )
    ]
    for load in loads:
        load.start()
    copies = Copies(send, recv)
    keep, core = (keep0, keep1, keep2), (core0, core1, core2)
    order = (1, 3, 2, 0)
    flat = [(k, o) for k in order for o in (1, 0)]

    def shard(k, o):
        return ((z + k) % 4) * 2 + (1 - x if o else x)

    def lanes(kind, this_core):
        which = 0 if this_core else 1
        own_core = c if which == 0 else 1 - c
        at = {
            0: 2 * TILE + ((1 - y) * 2 + own_core) * TILE,
            1: own_core * TILE,
            2: 2 * TILE + (y * 2 + own_core) * TILE,
        }[kind]
        return at

    def columns(kind, this_core, block=0):
        return pl.ds(pl.multiple_of(block * W + lanes(kind, this_core), TILE), TILE)

    def sources(g, kind, this_core):
        if g == 0:
            return [dw.at[j, :, columns(kind, this_core)] for j in range(4)]
        if g == 1:
            return [g1.at[:, columns(kind, this_core, j)] for j in range(4)]
        return [g2.at[:, :, columns(kind, this_core)]]

    def targets(g, kind, refs):
        return [refs[g].at[kind, j] for j in range(4)] if g < 2 else [refs[g].at[kind]]

    def cut(g, kind, refs, k, o):
        if g == 2:
            return refs[g].at[kind, pl.ds(shard(k, o) * 4, 4), :, :]
        return refs[g].at[kind, :, pl.ds(shard(k, o) * part, part), :]

    own = {}
    for g in (2, 1, 0):
        for kind in (0, 1, 2):
            pairs = zip(sources(g, kind, False), targets(g, kind, core))
            for j, (source, into) in enumerate(pairs):
                copies.plan((g, "core", kind, j), source, into, where["core"])
            pairs = zip(sources(g, kind, True), targets(g, kind, keep))
            for j, (source, into) in enumerate(pairs):
                own[g, kind, j] = pltpu.make_async_copy(source, into, own_sem.at[len(own)])
        for i, (k, o) in enumerate(flat):
            copies.plan((g, "y", k, o), cut(g, 0, keep, k, o), got_y.at[g, i], where["y"])
        for k in order:
            for s, kind in enumerate((1, 2)):
                copies.plan(
                    (g, kind, "x", k), cut(g, kind, keep, k, 1), got_x.at[g, s, k], where["x"]
                )
                if k:
                    copies.plan(
                        (g, kind, "z", k), cut(g, kind, keep, k, 0), got_z.at[g, s, k - 1],
                        where["z", k],
                    )
        copies.plan((g, 1, "ey"), ends.at[g, 0, 0], ends.at[g, 0, 1], where["y"])
        copies.plan((g, 1, "ecore"), ends.at[g, 0, 2], ends.at[g, 0, 3], where["core"])
        copies.plan((g, 2, "ey"), ends.at[g, 1, 0], ends.at[g, 1, 1], where["y"])
        copies.plan((g, 2, "ecore"), ends.at[g, 1, 0], ends.at[g, 1, 2], where["core"])
        copies.plan((g, 2, "ediagonal"), ends.at[g, 1, 1], ends.at[g, 1, 3], where["core"])
    copies.plan(("v", "core"), vec.at[0], vec.at[1], where["core"])
    copies.plan(("v", "y"), vec.at[2], vec.at[3], where["y"])
    copies.plan(("v", "x"), vec.at[4], vec.at[5], where["x"])
    for k in (1, 2, 3):
        copies.plan(("v", "z", k), vec.at[6], vec.at[6 + k], where["z", k])

    def begin(g, blocks):
        for kind in (0, 1, 2):
            for j in blocks:
                copies.go((g, "core", kind, j))
                own[g, kind, j].start()

    def ready(g, kind):
        for j in range(4 if g < 2 else 1):
            own[g, kind, j].wait()
            copies.arrived((g, "core", kind, j))

    def put(target, *refs):
        target[...] = total(*refs).astype(low)

    def cores(g):
        ready(g, 0)
        for k, o in flat:
            here = cut(g, 0, keep, k, o)
            put(here, here, cut(g, 0, core, k, o))
            copies.go((g, "y", k, o))
        ready(g, 1)
        for k in order:
            here = cut(g, 1, keep, k, 1)
            put(here, here, cut(g, 1, core, k, 1))
            copies.go((g, 1, "x", k))
        ready(g, 2)

    def over_y(g, k):
        copies.arrived((g, "y", k, 1))
        here = cut(g, 2, keep, k, 1)
        put(here, here, cut(g, 2, core, k, 1), got_y.at[g, flat.index((k, 1))])
        copies.go((g, 2, "x", k))

    def half_over_x(g, k):
        copies.arrived((g, 1, "x", k))
        here = cut(g, 1, keep, k, 0)
        put(here, here, cut(g, 1, core, k, 0), got_x.at[g, 0, k])
        copies.go((g, 1, "z", k))

    def over_x(g, k):
        copies.arrived((g, "y", k, 0))
        copies.arrived((g, 2, "x", k))
        here = cut(g, 2, keep, k, 0)
        put(
            here, here, cut(g, 2, core, k, 0), got_y.at[g, flat.index((k, 0))], got_x.at[g, 1, k]
        )
        copies.go((g, 2, "z", k))

    def half_over_z(g):
        copies.arrived((g, 1, "x", 0))
        for k in (1, 2, 3):
            copies.arrived((g, 1, "z", k))
        put(
            ends.at[g, 0, 0], cut(g, 1, keep, 0, 0), cut(g, 1, core, 0, 0), got_x.at[g, 0, 0],
            *(got_z.at[g, 0, k] for k in range(3)),
        )
        copies.go((g, 1, "ey"))

    def over_z(g):
        copies.arrived((g, 2, "x", 0))
        copies.arrived((g, "y", 0, 0))
        for k in (1, 2, 3):
            copies.arrived((g, 2, "z", k))
        put(
            ends.at[g, 1, 0], cut(g, 2, keep, 0, 0), cut(g, 2, core, 0, 0), got_x.at[g, 1, 0],
            got_y.at[g, flat.index((0, 0))], *(got_z.at[g, 1, k] for k in range(3)),
        )
        copies.go((g, 2, "ey"))
        copies.go((g, 2, "ecore"))

    def write(g, s, slot, at):
        value = ends[g, s, slot].astype(jnp.float32)
        for j in range(4):
            if g == 0:
                (rq, rk, rw, ro)[j][:, pl.ds(pl.multiple_of(at, TILE), TILE)] = value[j]
            elif g == 1:
                r1[:, pl.ds(pl.multiple_of(j * W + at, TILE), TILE)] = value[j]
            else:
                r2[j * part : (j + 1) * part, pl.ds(pl.multiple_of(at, TILE), TILE)] = value[j]

    def half_finish(g):
        copies.arrived((g, 1, "ey"))
        put(ends.at[g, 0, 2], ends.at[g, 0, 0], ends.at[g, 0, 1])
        copies.go((g, 1, "ecore"))

    def finish(g):
        copies.arrived((g, 2, "ey"))
        copies.go((g, 2, "ediagonal"))
        write(g, 0, 2, lanes(1, True))
        write(g, 1, 0, lanes(2, True))
        write(g, 1, 1, lanes(0, True))

    def close(g):
        copies.arrived((g, 2, "ecore"))
        write(g, 1, 2, lanes(2, False))
        copies.arrived((g, 1, "ecore"))
        write(g, 0, 3, lanes(1, False))
        copies.arrived((g, 2, "ediagonal"))
        write(g, 1, 3, lanes(0, False))

    acts = {
        "a": cores, "h": half_over_x, "b": over_y, "c": over_x, "s": half_over_z, "d": over_z,
        "t": half_finish, "f": finish, "g": close,
    }

    def pump(events):
        for event in events:
            act = acts[event[0]]
            if len(event) == 3:
                act(int(event[1]), int(event[2]))
            else:
                act(int(event[1]))

    greet(where)
    begin(2, (0,))
    begin(1, range(4))
    for load in loads:
        load.wait()
    begin(0, (3,))
    x_turned[...] = x_kept[...].T
    pump(BEFORE_BACK)

    def at_half(pair, half):
        for which, events in enumerate(DURING_BACK[half::2]):
            if events:
                pl.when(pair == which)(functools.partial(pump, events))

    @pl.loop(0, 6)
    def _(pair):
        at = pl.ds(pl.multiple_of(pair * TILE, TILE), TILE)
        attend_back_pair(
            key_ids, query_ids, *(held.at[i, :, at] for i in range(4)), lse_ref.at[pair],
            *(grads.at[i, :, at] for i in range(3)), k_turned, k_total, v_total,
            lambda: at_half(pair, 0),
        )
        at_half(pair, 1)

    fetch = [pltpu.make_async_copy(w_in.at[i], held.at[i, 0:W, :], load_sem.at[i]) for i in range(3)]
    for copy in fetch:
        copy.start()
    for i in range(3):

        @pl.loop(0, 3)
        def _(block):
            span = pl.ds(pl.multiple_of(block * 256, 256), 256)
            dw[i, span, :] = product(x_turned[span, :], grads[i]).astype(low)

        begin(0, (i,))
        pump(DURING_WEIGHTS[i])
    vec[0, 0:1, :] = column_sum(grads[0])[None]
    vec[0, 1:2, :] = column_sum(grads[2])[None]
    vec[0, 2:8, :] = sums_in[2:8, :]
    vec[0, 8:12, :] = inner_in[...]
    vec[0, 12:16, :] = jnp.zeros((4, W), jnp.float32)
    copies.go(("v", "core"))
    pump(("a0",))
    copies.arrived(("v", "core"))
    vec[2] = vec[0] + vec[1]
    copies.go(("v", "y"))
    for copy in fetch:
        copy.wait()

    @pl.loop(0, 4)
    def _(block):
        span = pl.ds(pl.multiple_of(block * 256, 256), 256)
        value = gx[span, :]
        for i in range(3):
            value = value + against(grads[i, span, :], held[i, 0:W, :])
        gx[span, :] = value
        for which, events in enumerate(DURING_ROWS):

            @pl.when(block == which)
            def _():
                pump(events)

    copies.arrived(("v", "y"))
    vec[4] = vec[2] + vec[3]
    copies.go(("v", "x"))
    pump(AFTER_ROWS)
    copies.arrived(("v", "x"))
    vec[6] = vec[4] + vec[5]
    for k in (1, 2, 3):
        copies.go(("v", "z", k))
    pump(LAST)
    for k in (1, 2, 3):
        copies.arrived(("v", "z", k))
    rv[...] = (vec[6] + vec[7]) + (vec[8] + vec[9])
    pump(("g2", "g1", "g0"))
    copies.drain()


REDUCE_COPIES = 3 + 12 + 12 + 3 * (8 + 4 + 4 + 3 + 3 + 5) + 6
BEFORE_BACK = ("a2",)
DURING_BACK = (
    (),
    ("h21", "b21", "a1", "h23"),
    ("b23", "h22"),
    ("c21", "b22"),
    ("h11", "s2"),
    ("b20", "h13", "h12"),
    ("b11", "c23"),
    ("c22", "b13"),
    ("s1", "c11", "b12"),
    ("c13", "d2"),
    ("b10", "c12"),
    ("t2",),
)
DURING_WEIGHTS = (
    ("t1",),
    ("f2", "d1"),
    (),
)
DURING_ROWS = (
    ("f1",),
    (),
    ("h01", "b01"),
    ("h03",),
)
AFTER_ROWS = ("b03", "h02", "c01", "b02", "c03", "s0")
LAST = ("b00", "c02", "t0", "d0", "f0")


def reduce_attend(
    query, keys, values, grad_mixed, rows, grad_hidden, weights, grad_out, grad_inner, grad_outer,
    lse, key_ids, query_ids, sums, inner_sums,
):
    low, full = jnp.bfloat16, jnp.float32
    count = rows.shape[0]
    part = W // 8
    anywhere, near = pl.BlockSpec(memory_space=pl.ANY), pl.BlockSpec(memory_space=pltpu.VMEM)
    slab = jax.ShapeDtypeStruct((part, W), full)
    piece = (4, part, TILE)
    wide, tall = pltpu.VMEM((3, 4, W, TILE), low), pltpu.VMEM((3, 32, part, TILE), low)
    return pl.pallas_call(
        reduce_attend_kernel,
        out_shape=(
            jax.ShapeDtypeStruct((count, W), full),
            slab,
            slab,
            slab,
            slab,
            jax.ShapeDtypeStruct((part, 4 * W), full),
            jax.ShapeDtypeStruct((4 * part, W), full),
            jax.ShapeDtypeStruct((16, W), full),
        ),
        in_specs=[anywhere] * 10 + [near] * 5,
        out_specs=[near] * 8,
        scratch_shapes=[
            pltpu.VMEM((4, count, W), low),
            pltpu.VMEM((count, W), low),
            pltpu.VMEM((W, count), low),
            pltpu.VMEM((3, count, W), low),
            pltpu.VMEM((4, W, W), low),
            pltpu.VMEM((TILE, count), low),
            pltpu.VMEM((count, TILE), full),
            pltpu.VMEM((count, TILE), full),
            wide,
            wide,
            tall,
            wide,
            wide,
            tall,
            pltpu.VMEM((3, 8) + piece, low),
            pltpu.VMEM((3, 2, 4) + piece, low),
            pltpu.VMEM((3, 2, 3) + piece, low),
            pltpu.VMEM((3, 2, 4) + piece, low),
            pltpu.VMEM((10, 16, W), full),
            pltpu.SemaphoreType.DMA((REDUCE_COPIES,)),
            pltpu.SemaphoreType.DMA((REDUCE_COPIES,)),
            pltpu.SemaphoreType.DMA((7,)),
            pltpu.SemaphoreType.DMA((27,)),
        ],
        compiler_params=pltpu.CompilerParams(
            collective_id=1, has_side_effects=True, vmem_limit_bytes=62 << 20
        ),
        name="reduce_attend",
    )(
        query, keys, values, grad_mixed, rows, grad_hidden, weights, grad_out, grad_inner,
        grad_outer.reshape(32, part, W), lse, key_ids, query_ids, sums, inner_sums,
    )


def normalise(value):
    mean = jnp.mean(value, axis=1, keepdims=True)
    centred = value - mean
    scale = lax.rsqrt(jnp.mean(centred * centred, axis=1, keepdims=True) + 1e-05)
    return centred * scale, scale


def normalise_back(grad, unit, scale):
    middle = jnp.mean(grad, axis=1, keepdims=True)
    along = jnp.mean(grad * unit, axis=1, keepdims=True)
    return scale * (grad - middle - unit * along)


def chain_kernel(
    mixed_ref, rows_ref, pull_ref, wo_ref, w1_ref, w2_ref, small_ref, b1_ref,
    out_ref, y1_ref, u_ref, gz_ref, gf_ref, gh_ref, ga_ref, gmix_ref, sums_ref, b1_sum_ref,
    slope_ref,
):
    low = jnp.bfloat16

    @pl.when(pl.program_id(0) == 0)
    def _():
        sums_ref[...] = jnp.zeros_like(sums_ref)
        b1_sum_ref[...] = jnp.zeros_like(b1_sum_ref)

    def small(i):
        return small_ref[i : i + 1, :]

    def gather_sum(ref, i, value):
        ref[i : i + 1, :] += jnp.sum(value, axis=0, keepdims=True)

    hidden = rows_ref[...].astype(jnp.float32) + product(mixed_ref[...], wo_ref[0]) + small(2)
    unit_one, scale_one = normalise(hidden)
    y1 = unit_one * small(3) + small(4)
    y1_low = y1.astype(low)
    y1_ref[...] = y1_low
    second = y1 + small(5)
    for r in range(4):
        inner = product(y1_low, w1_ref[r]) + b1_ref[r : r + 1, :]
        active, slope = gelu_and_slope(inner)
        active = active.astype(low)
        u_ref[:, r * W : (r + 1) * W] = active
        slope_ref[:, r * W : (r + 1) * W] = slope
        second = second + product(active, w2_ref[r * W : (r + 1) * W, :])
    unit_two, scale_two = normalise(second)
    out_ref[...] = (unit_two * small(6) + small(7)).astype(low)
    pull = pull_ref[...].astype(jnp.float32)
    gather_sum(sums_ref, 6, pull * unit_two)
    gather_sum(sums_ref, 7, pull)
    grad_second = normalise_back(pull * small(6), unit_two, scale_two)
    gz = grad_second.astype(low)
    gz_ref[...] = gz
    gather_sum(sums_ref, 5, gz.astype(jnp.float32))
    grad_y1 = grad_second
    for r in range(4):
        gf = against(gz, w2_ref[r * W : (r + 1) * W, :]) * slope_ref[:, r * W : (r + 1) * W]
        gf = gf.astype(low)
        gf_ref[:, r * W : (r + 1) * W] = gf
        gather_sum(b1_sum_ref, r, gf.astype(jnp.float32))
        grad_y1 = grad_y1 + against(gf, w1_ref[r])
    gather_sum(sums_ref, 3, grad_y1 * unit_one)
    gather_sum(sums_ref, 4, grad_y1)
    grad_hidden = normalise_back(grad_y1 * small(3), unit_one, scale_one)
    gh_ref[...] = grad_hidden
    ga = grad_hidden.astype(low)
    ga_ref[...] = ga
    gather_sum(sums_ref, 2, ga.astype(jnp.float32))
    gmix_ref[...] = against(ga, wo_ref[0]).astype(low)


def chain(mixed, rows, pull, weights, inner_blocks, outer_mat, small, inner_bias):
    count, width = rows.shape
    step = 256
    low, full = jnp.bfloat16, jnp.float32
    thin = pl.BlockSpec((step, width), lambda i: (i, 0))
    fat = pl.BlockSpec((step, 4 * width), lambda i: (i, 0))
    held = lambda shape: pl.BlockSpec(shape, lambda i: (0,) * len(shape))
    once = pl.Buffered(1)
    return pl.pallas_call(
        chain_kernel,
        grid=(count // step,),
        out_shape=(
            jax.ShapeDtypeStruct((count, width), low),
            jax.ShapeDtypeStruct((count, width), low),
            jax.ShapeDtypeStruct((count, 4 * width), low),
            jax.ShapeDtypeStruct((count, width), low),
            jax.ShapeDtypeStruct((count, 4 * width), low),
            jax.ShapeDtypeStruct((count, width), full),
            jax.ShapeDtypeStruct((count, width), low),
            jax.ShapeDtypeStruct((count, width), low),
            jax.ShapeDtypeStruct((8, width), full),
            jax.ShapeDtypeStruct((4, width), full),
        ),
        in_specs=[
            thin, thin, thin,
            pl.BlockSpec((1, width, width), lambda i: (3, 0, 0), pipeline_mode=once),
            pl.BlockSpec((4, width, width), lambda i: (0, 0, 0), pipeline_mode=once),
            pl.BlockSpec((4 * width, width), lambda i: (0, 0), pipeline_mode=once),
            held((8, width)), held((4, width)),
        ],
        out_specs=[thin, thin, fat, thin, fat, thin, thin, thin, held((8, width)), held((4, width))],
        scratch_shapes=[pltpu.VMEM((step, 4 * width), full)],
        compiler_params=pltpu.CompilerParams(vmem_limit_bytes=60 << 20),
        name="chain",
    )(mixed, rows, pull, weights, inner_blocks, outer_mat, small, inner_bias)


def on_device(
    tokens,
    read_memory,
    doc_ids,
    w_query,
    w_key,
    w_value,
    w_out,
    query_bias,
    value_bias,
    out_bias,
    norm_one_gain,
    norm_one_bias,
    w_inner,
    inner_bias,
    w_outer,
    outer_bias,
    norm_two_gain,
    norm_two_bias,
    out_grad,
):
    owners = lax.axis_size("fsdp")
    wide = owners == 8 and lax.axis_size("rep") == 4
    part = w_query.shape[0]
    low = jnp.bfloat16
    small = pack(
        jnp.stack(
            [
                query_bias, value_bias, out_bias, norm_one_gain,
                norm_one_bias, outer_bias, norm_two_gain, norm_two_bias,
            ]
        )[None],
        inner_bias[None],
    )[0]
    seqs, seg = doc_ids.shape
    width = tokens.shape[1]
    mem = read_memory.shape[0] // seqs
    length = seg + 2 * mem
    memory_rows = read_memory.reshape(seqs, mem, width)
    rows = jnp.concatenate([tokens.reshape(seqs, seg, width), memory_rows, memory_rows], axis=1)
    rows = rows.reshape(seqs * length, width)
    marks = jnp.full((seqs, 2 * mem), -1, jnp.int32)
    ids = jnp.concatenate([doc_ids, marks], axis=1)
    out_rows = out_grad.reshape(seqs, length, width)
    out_rows = jnp.concatenate(
        [out_rows[:, mem : mem + seg], out_rows[:, :mem], out_rows[:, mem + seg :]], axis=1
    ).reshape(seqs * length, width)

    def each(function, *arrays):
        results = []
        for s in range(seqs):
            own = slice(s * length, (s + 1) * length)
            spread = jnp.broadcast_to(ids[s][:, None], (length, TILE))
            by_block = ids[s].reshape(length // TILE, TILE)
            results.append(function(spread, by_block, *[a[own] for a in arrays]))
        return results

    shards = (w_query, w_key, w_value, w_out, w_inner, w_outer, small)
    wide = wide and seqs == 1
    if wide:
        spread, by_block = each(lambda *a: a)[0]
        weights, inner_blocks, outer_mat, vectors, inner_shift, query, keys, values, mixed, sums = (
            gather_attend(shards, rows, spread, by_block)
        )
        pairs = [(mixed, sums)]
    else:
        weights, inner_blocks, outer_mat, packed = plain_gather(*shards)
        vectors, inner_shift = unpack(packed.astype(jnp.float32), part)
        query = (product(rows, weights[0]) + vectors[0]).astype(low)
        keys = product(rows, weights[1]).astype(low)
        values = (product(rows, weights[2]) + vectors[1]).astype(low)
        pairs = each(attend, query, keys, values)
        mixed = jnp.concatenate([pair[0] for pair in pairs], axis=0)
    output, normed, active, grad_outer, grad_inner, grad_residual, grad_branch, grad_mixed, sums, inner_sums = chain(
        mixed, rows, out_rows, weights, inner_blocks, outer_mat, vectors, inner_shift
    )
    grad_w_outer = inner_rows(active, grad_outer).astype(low)
    grad_w_inner = inner_rows(normed, grad_inner).astype(low)
    grad_w_out = inner_rows(mixed, grad_branch).astype(low)
    if wide:
        grad_rows, *shares, joined = reduce_attend(
            query, keys, values, grad_mixed, rows, grad_residual, weights, grad_w_out,
            grad_w_inner, grad_w_outer, pairs[0][1], spread, by_block, sums, inner_sums,
        )
        place_of = lax.axis_index("fsdp")
        last = lax.dynamic_slice(joined[:8], (0, place_of * part), (8, part))
        last_inner = lax.dynamic_slice(
            joined[8:12].reshape(-1), (place_of * 4 * part,), (4 * part,)
        )
    else:
        triples = [
            attend_back(spread, by_block, q, k, v, g, pairs[s][1])
            for s, (spread, by_block, q, k, v, g) in enumerate(
                each(lambda *a: a, query, keys, values, grad_mixed)
            )
        ]
        grad_query_low, grad_keys_low, grad_values_low = (
            jnp.concatenate([triple[i] for triple in triples], axis=0) for i in range(3)
        )
        grad_w_query = inner_rows(rows, grad_query_low).astype(low)
        grad_w_key = inner_rows(rows, grad_keys_low).astype(low)
        grad_w_value = inner_rows(rows, grad_values_low).astype(low)
        sums = jnp.concatenate(
            [column_sum(grad_query_low)[None], column_sum(grad_values_low)[None], sums[2:]], axis=0
        )
        grad_rows = (
            grad_residual
            + against(grad_query_low, weights[0])
            + against(grad_keys_low, weights[1])
            + against(grad_values_low, weights[2])
        )
        *shares, share_small = plain_reduce(
            grad_w_query,
            grad_w_key,
            grad_w_value,
            grad_w_out,
            grad_w_inner,
            grad_w_outer,
            pack(
                sums.reshape(8, owners, part).transpose(1, 0, 2),
                inner_sums.reshape(owners, 4 * part),
            ),
        )
        last, last_inner = unpack(share_small[None], part)
    grad_rows = grad_rows.reshape(seqs, length, width)
    grad_tokens = grad_rows[:, :seg].reshape(seqs * seg, width).astype(jnp.bfloat16)
    grad_memory = (
        (grad_rows[:, seg : seg + mem] + grad_rows[:, seg + mem :])
        .reshape(seqs * mem, width)
        .astype(jnp.bfloat16)
    )
    layer_out = output.reshape(seqs, length, width)
    layer_out = jnp.concatenate(
        [layer_out[:, seg : seg + mem], layer_out[:, :seg], layer_out[:, seg + mem :]], axis=1
    ).reshape(seqs * length, width)
    return (
        layer_out,
        grad_tokens,
        grad_memory,
        *shares[:4],
        *(last[i] for i in range(5)),
        shares[4],
        last_inner.reshape(-1),
        shares[5],
        *(last[i] for i in range(5, 8)),
    )


def solution(mesh):
    return jax.shard_map(
        on_device,
        mesh=mesh,
        in_specs=(
            P(("rep", "fsdp"), None),
            P(("rep", "fsdp"), None),
            P(("rep", "fsdp"), None),
            P("fsdp", None),
            P("fsdp", None),
            P("fsdp", None),
            P("fsdp", None),
            P("fsdp"),
            P("fsdp"),
            P("fsdp"),
            P("fsdp"),
            P("fsdp"),
            P("fsdp", None),
            P("fsdp"),
            P("fsdp", None),
            P("fsdp"),
            P("fsdp"),
            P("fsdp"),
            P(("rep", "fsdp"), None),
        ),
        out_specs=(
            P(("rep", "fsdp"), None),
            P(("rep", "fsdp"), None),
            P(("rep", "fsdp"), None),
            P("fsdp", None),
            P("fsdp", None),
            P("fsdp", None),
            P("fsdp", None),
            P("fsdp"),
            P("fsdp"),
            P("fsdp"),
            P("fsdp"),
            P("fsdp"),
            P("fsdp", None),
            P("fsdp"),
            P("fsdp", None),
            P("fsdp"),
            P("fsdp"),
            P("fsdp"),
        ),
        check_vma=False,
    )
```

```python
import functools
import math

import jax
import jax.numpy as jnp
from jax import lax
from jax.experimental import pallas as pl
from jax.experimental.pallas import tpu as pltpu
from jax.sharding import PartitionSpec as P

MESH_ID = pl.DeviceIdType.MESH
W = 768


def only_if(condition, act):
    if condition is None:
        act()
    else:
        pl.when(condition)(act)


class Copies:
    def __init__(self, send, recv):
        self.send, self.recv, self.made = send, recv, {}

    def plan(self, name, src, dst, to, leaves=None, comes=None):
        slot = len(self.made)

        def describe(src):
            return pltpu.make_async_remote_copy(
                src_ref=src,
                dst_ref=dst,
                send_sem=self.send.at[slot],
                recv_sem=self.recv.at[slot],
                device_id=to,
                device_id_type=MESH_ID,
            )

        self.made[name] = (describe, src, leaves, comes)

    def go(self, name):
        describe, src, leaves, _ = self.made[name]
        only_if(leaves, lambda: describe(src).start())

    def start(self, name, src, dst, to):
        self.plan(name, src, dst, to)
        self.go(name)

    def arrived(self, name):
        describe, src, _, comes = self.made[name]
        only_if(comes, lambda: describe(src).wait_recv())

    def drain(self):
        for describe, src, leaves, _ in self.made.values():
            only_if(leaves, functools.partial(lambda describe, src: describe(src).wait_send(), describe, src))


def place():
    rep, owner = lax.axis_index("rep"), lax.axis_index("fsdp")
    y, c, z, x = rep // 2, rep % 2, owner // 2, owner % 2
    where = {
        "core": (y * 2 + 1 - c, owner),
        "y": ((1 - y) * 2 + c, owner),
        "x": (rep, z * 2 + 1 - x),
    }
    for k in (1, 2, 3):
        where["z", k] = (rep, ((z + k) % 4) * 2 + x)
        where["zx", k] = (rep, ((z + k) % 4) * 2 + 1 - x)
    return rep, owner, y, c, z, x, where


def greet(where):
    barrier = pltpu.get_barrier_semaphore()
    for to in where.values():
        pl.semaphore_signal(barrier, inc=1, device_id=to, device_id_type=MESH_ID)
    pl.semaphore_wait(barrier, len(where))


def total(*refs):
    value = refs[0][...].astype(jnp.float32)
    for ref in refs[1:]:
        value = value + ref[...].astype(jnp.float32)
    return value


def inner_lines(part):
    return -(-4 * part // 128)


def pack(vectors, inner):
    owners, _, part = vectors.shape
    lines = inner_lines(part)
    first = jnp.pad(vectors, ((0, 0), (0, 0), (0, 128 - part)))
    second = jnp.pad(inner, ((0, 0), (0, lines * 128 - 4 * part)))
    second = second.reshape(owners, lines, 128)
    return jnp.pad(jnp.concatenate([first, second], axis=1), ((0, 0), (0, 8 - lines), (0, 0)))


def unpack(packed, part):
    owners = packed.shape[0]
    lines = inner_lines(part)
    first = packed[:, :8, :part].transpose(1, 0, 2).reshape(8, owners * part)
    second = packed[:, 8 : 8 + lines].reshape(owners, lines * 128)[:, : 4 * part]
    return first, second.reshape(4, owners * part)


def plain_gather(wq, wk, wv, wo, inner, outer, vectors):
    gathered = lax.all_gather(inner, "fsdp", axis=0, tiled=True)
    return (
        lax.all_gather(jnp.stack([wq, wk, wv, wo]), "fsdp", axis=1, tiled=True),
        gathered.reshape(W, 4, W).transpose(1, 0, 2),
        lax.all_gather(outer, "fsdp", axis=0, tiled=True),
        lax.all_gather(vectors, "fsdp", axis=0),
    )


def plain_reduce(*grads):
    def over_all(value):
        part = lax.psum_scatter(value, "fsdp", scatter_dimension=0, tiled=True)
        return lax.psum(part, "rep").astype(jnp.float32)

    return tuple(over_all(grad) for grad in grads[:-1]) + (over_all(grads[-1])[0],)


def product(left, right):
    return jnp.dot(left, right, preferred_element_type=jnp.float32)


def inner_rows(left, right):
    return lax.dot_general(
        left, right, (((0,), (0,)), ((), ())), preferred_element_type=jnp.float32
    )


def against(left, right):
    return lax.dot_general(
        left, right, (((1,), (1,)), ((), ())), preferred_element_type=jnp.float32
    )


def column_sum(values):
    return jnp.sum(values.astype(jnp.float32), axis=0)


TILE = 128
HEAD_DIM = 64
FACTOR = HEAD_DIM ** (-0.5)
HIDDEN = -1e30


def spans(i, count):
    last = count - 1
    if i == last:
        return [(0, count * TILE)]
    low, high = max(0, i - 2), min(last, i + 2)
    if high == last:
        return [(low * TILE, count * TILE)]
    return [(low * TILE, (high + 1) * TILE), (last * TILE, count * TILE)]


def two_heads(block):
    lanes = lax.broadcasted_iota(jnp.int32, block.shape, 1)
    zero = jnp.zeros_like(block)
    first = jnp.where(lanes < HEAD_DIM, block, zero)
    second = jnp.where(lanes < HEAD_DIM, zero, block)
    return jnp.concatenate([first, second], axis=0)


def own_head(value):
    rows = lax.broadcasted_iota(jnp.int32, (TILE, TILE), 0)
    return jnp.where(rows < HEAD_DIM, value[:, :TILE], value[:, TILE:]).T


def masked_scores(k_ref, key_ids, query_ids, stacked, i, span, count):
    low, high = span
    scores = against(k_ref[low:high, :], stacked)
    ids = key_ids[low:high, :]
    row = query_ids[i : i + 1, :]
    seen = ids == row
    if high == count * TILE:
        seen = seen | (ids < 0)
    if i == count - 1:
        seen = seen | (row < 0)
    return jnp.concatenate(
        [jnp.where(seen, scores[:, :TILE], HIDDEN), jnp.where(seen, scores[:, TILE:], HIDDEN)], axis=1
    )


def attend_kernel(key_ids, query_ids, q_ref, k_ref, v_ref, out_ref, lse_ref, v_turned):
    attend_pair(key_ids, query_ids, q_ref, k_ref, v_ref, out_ref, lse_ref.at[0], v_turned)


def attend_pair(
    key_ids, query_ids, q_ref, k_ref, v_ref, out_ref, lse_ref, v_turned, middle=lambda: None
):
    count = q_ref.shape[0] // TILE
    v_turned[...] = v_ref[:, :].T
    for i in range(count):
        rows = slice(i * TILE, (i + 1) * TILE)
        stacked = two_heads(q_ref[rows, :] * jnp.bfloat16(FACTOR))
        parts = spans(i, count)
        scores = [masked_scores(k_ref, key_ids, query_ids, stacked, i, p, count) for p in parts]
        peak = functools.reduce(
            jnp.maximum, [jnp.max(s, axis=0, keepdims=True) for s in scores]
        )
        weights = [jnp.exp(s - peak) for s in scores]
        total = sum(jnp.sum(w, axis=0, keepdims=True) for w in weights)
        mixed = sum(
            product(v_turned[:, low:high], w.astype(jnp.bfloat16)) for (low, high), w in zip(parts, weights)
        )
        out_ref[rows, :] = own_head(mixed * (1.0 / total)).astype(jnp.bfloat16)
        lse_ref[i : i + 1, :] = peak + jnp.log(total)
        if i == count // 2 - 1:
            middle()


def attend_back_kernel(
    key_ids, query_ids, q_ref, k_ref, v_ref, g_ref, lse_ref, gq_ref, gk_ref, gv_ref,
    k_turned, k_total, v_total,
):
    attend_back_pair(
        key_ids, query_ids, q_ref, k_ref, v_ref, g_ref, lse_ref.at[0], gq_ref, gk_ref, gv_ref,
        k_turned, k_total, v_total,
    )


def attend_back_pair(
    key_ids, query_ids, q_ref, k_ref, v_ref, g_ref, lse_ref, gq_ref, gk_ref, gv_ref,
    k_turned, k_total, v_total, middle=lambda: None,
):
    count = q_ref.shape[0] // TILE
    k_turned[...] = k_ref[:, :].T
    k_total[...] = jnp.zeros_like(k_total)
    v_total[...] = jnp.zeros_like(v_total)
    for i in range(count):
        rows = slice(i * TILE, (i + 1) * TILE)
        stacked = two_heads(q_ref[rows, :] * jnp.bfloat16(FACTOR))
        grads = two_heads(g_ref[rows, :])
        lse = lse_ref[i : i + 1, :]
        parts = spans(i, count)
        probs, pulls = [], []
        for low, high in parts:
            scores = masked_scores(k_ref, key_ids, query_ids, stacked, i, (low, high), count)
            p = jnp.exp(scores - lse)
            v_total[low:high, :] += product(p.astype(jnp.bfloat16), grads)
            probs.append(p)
            pulls.append(against(v_ref[low:high, :], grads))
        centre = sum(jnp.sum(p * g, axis=0, keepdims=True) for p, g in zip(probs, pulls))
        mixed = 0.0
        for (low, high), p, g in zip(parts, probs, pulls):
            turned = (p * (g - centre)).astype(jnp.bfloat16)
            k_total[low:high, :] += product(turned, stacked)
            mixed = mixed + product(k_turned[:, low:high], turned)
        gq_ref[rows, :] = (own_head(mixed) * FACTOR).astype(jnp.bfloat16)
        if i == count // 2 - 1:
            middle()
    gk_ref[:, :] = k_total[...].astype(jnp.bfloat16)
    gv_ref[:, :] = v_total[...].astype(jnp.bfloat16)


def attend(key_ids, query_ids, query, keys, values):
    rows, width = query.shape
    pair = 2 * HEAD_DIM
    count = rows // TILE
    column = pl.BlockSpec((rows, pair), lambda h: (0, h))
    whole = lambda a: pl.BlockSpec(a.shape, lambda h: (0, 0))
    return pl.pallas_call(
        attend_kernel,
        grid=(width // pair,),
        out_shape=(
            jax.ShapeDtypeStruct((rows, width), jnp.bfloat16),
            jax.ShapeDtypeStruct((width // pair, count, 2 * TILE), jnp.float32),
        ),
        in_specs=[whole(key_ids), whole(query_ids), column, column, column],
        out_specs=[column, pl.BlockSpec((1, count, 2 * TILE), lambda h: (h, 0, 0))],
        scratch_shapes=[pltpu.VMEM((pair, rows), jnp.bfloat16)],
        compiler_params=pltpu.CompilerParams(vmem_limit_bytes=48 << 20),
        name="attend",
    )(key_ids, query_ids, query, keys, values)


def picked(ref, low, high, *runs):
    rows = lax.broadcasted_iota(jnp.int32, (TILE, high - low), 0)
    source = lax.broadcasted_iota(jnp.int32, (TILE, high - low), 1)
    choice = None
    for first, last, offset in runs:
        one = (source == rows + offset) & (rows >= first) & (rows < last)
        choice = one if choice is None else choice | one
    return product(choice.astype(jnp.bfloat16), ref[low:high, :])


def to_tokens_first(ref, into, mem):
    count = ref.shape[0] // TILE
    end = TILE - 2 * mem
    for i in range(count - 1):
        value = picked(ref, i * TILE, i * TILE + TILE + 16, (0, TILE, mem))
        into[i * TILE : (i + 1) * TILE, :] = value.astype(jnp.bfloat16)
    last = (count - 1) * TILE
    value = picked(ref, last, last + TILE, (0, end, mem), (end + mem, TILE, 0))
    value = value + picked(ref, 0, 16, (end, end + mem, -end))
    into[last:, :] = value.astype(jnp.bfloat16)


def to_memory_first(ref, into, mem):
    count = ref.shape[0] // TILE
    last = (count - 1) * TILE
    value = picked(ref, 0, TILE, (mem, TILE, -mem))
    value = value + picked(ref, last, last + TILE, (0, mem, TILE - 2 * mem))
    into[:TILE, :] = value.astype(jnp.bfloat16)
    for i in range(1, count):
        runs = [(0, TILE, 16 - mem)]
        if i == count - 1:
            runs = [(0, TILE - mem, 16 - mem), (TILE - mem, TILE, 16)]
        value = picked(ref, i * TILE - 16, (i + 1) * TILE, *runs)
        into[i * TILE : (i + 1) * TILE, :] = value.astype(jnp.bfloat16)


def gather_attend_kernel(
    mem, wq, wk, wv, wo, w1, w2, vec, x_ref, key_ids, query_ids, pull_in,
    o0, o1, o2, small, inner, q_out, k_out, v_out, out_ref, lse_ref, pull_out,
    q_ref, k_ref, v_ref, w0, a1, a2, av, got, v_turned, send, recv, own_sem, load_sem,
):
    rep, owner, y, c, z, x, where = place()
    part = W // 8
    low = jnp.bfloat16
    across = (1 - y) * 2 + c
    mine0 = pl.ds(owner * part, part)
    loads = [
        pltpu.make_async_copy(source, into, load_sem.at[i])
        for i, (source, into) in enumerate(
            [(source, w0.at[i, mine0, :]) for i, source in enumerate((wq, wk, wv, wo))]
            + [(w1.at[:, i * W : (i + 1) * W], a1.at[i]) for i in range(4)]
            + [(w2, a2), (vec, av)]
        )
    ]
    for load in loads:
        load.start()

    near = (z + 3) % 4 - 2 * ((3 - z) // 3)
    far = 3 * (1 - z // 2)
    owners_z = (z, near, 6 - z - near - far, far)

    def shard(turn, other_x):
        return owners_z[turn] * 2 + (1 - x if other_x else x)

    def spot(g, kind, turn, other_x, quarter):
        at = 2 * TILE + quarter * TILE if kind else c * TILE
        lanes = pl.ds(pl.multiple_of(at, TILE), TILE)
        if g == 2:
            return o2.at[pl.ds(shard(turn, other_x) * 4 * part, 4 * part), lanes]
        return (w0, o1)[g].at[:, pl.ds(shard(turn, other_x) * part, part), lanes]

    greet(where)
    for load in loads:
        load.wait()
    own = [
        pltpu.make_async_copy(a1, o1.at[:, mine0, :], own_sem.at[0]),
        pltpu.make_async_copy(a2, o2.at[pl.ds(owner * 4 * part, 4 * part), :], own_sem.at[1]),
    ]
    kept = pltpu.make_async_copy(w0, o0, own_sem.at[2])
    note = pltpu.make_async_copy(av, got.at[owner], own_sem.at[3])
    copies = Copies(send, recv)

    for k in (1, 2, 3):
        copies.start(("v", "z", k), av, got.at[owner], where["z", k])
        copies.start(("v", "zx", k), av, got.at[owner], where["zx", k])
    copies.start(("v", "x", 0), av, got.at[owner], where["x"])
    for g in (0, 1, 2):
        for kind in (1, 0):
            at = 2 * TILE + rep * TILE if kind else c * TILE
            lanes = pl.ds(pl.multiple_of(at, TILE), TILE)
            source = (w0.at[:, mine0, lanes], a1.at[:, :, lanes], a2.at[:, lanes])[g]
            here = spot(g, kind, 0, False, rep)
            copies.plan((g, kind, "x", 0), source, here, where["x"])
            for start, end, turn in Z_ROUTES:
                through = (rep, end * 2 + x)
                relayed = turn == 3 and start in (1, 2) and end in (0, 3)
                from_here = spot(g, kind, 3, False, rep) if relayed else source
                into = spot(g, kind, 3, False, rep) if relayed else here
                copies.plan(
                    (g, kind, "z", start, end, turn), from_here, into, through, z == start, z == end
                )
    steps = [
        (0, True, "x"), (1, False, "z"), (2, False, "z"), (1, True, "x"),
        (3, False, "z"), (2, True, "x"), (3, True, "x"),
    ]
    for g in (0, 1, 2):
        for turn, other_x, stage in steps:
            for kind in (0, 1):
                here = spot(g, kind, turn, other_x, rep)
                if stage == "z":
                    copies.plan((g, kind, "x", turn), here, here, where["x"])
                if kind:
                    copies.plan((g, "y", turn, other_x), here, here, where["y"])
                    there = spot(g, kind, turn, other_x, across)
                    copies.plan((g, "diagonal", turn, other_x), there, there, where["core"])
                copies.plan((g, kind, "core", turn, other_x), here, here, where["core"])

    def begin(g, turns):
        for start, end, turn in Z_ROUTES:
            if turn in turns and not (turn == 3 and start in (1, 2)):
                for kind in (1, 0):
                    copies.go((g, kind, "z", start, end, turn))

    copies.go((0, 1, "x", 0))
    copies.go((0, 0, "x", 0))
    for g in (0, 1, 2):
        begin(g, (1, 2, 3))
    note.start()
    for copy in own:
        copy.start()
    to_tokens_first(pull_in, pull_out, mem)

    def pass_on(g, step):
        turn, other_x, stage = steps[step]
        for kind in (1, 0):
            if stage == "x":
                copies.arrived((g, kind, "x", turn))
            else:
                for start, end, at_turn in Z_ROUTES:
                    if at_turn == turn:
                        copies.arrived((g, kind, "z", start, end, turn))
                if turn == 3:
                    copies.go((g, kind, "z", 1, 0, 3))
                    copies.go((g, kind, "z", 2, 3, 3))
                copies.go((g, kind, "x", turn))
            if kind:
                copies.go((g, "y", turn, other_x))
            copies.go((g, kind, "core", turn, other_x))
        if step == 4 and g < 2:
            for kind in (1, 0):
                copies.go((g + 1, kind, "x", 0))

    def pass_core(g, step):
        turn, other_x, _ = steps[step]
        copies.arrived((g, "y", turn, other_x))
        copies.go((g, "diagonal", turn, other_x))

    def settle(g):
        for k, other_x, _ in steps:
            copies.arrived((g, 0, "core", k, other_x))
            copies.arrived((g, 1, "core", k, other_x))
            copies.arrived((g, "diagonal", k, other_x))

    def pump(events):
        for kind, g, step in events:
            (pass_core if kind == "c" else pass_on)(g, step)

    pump(EARLY)
    settle(0)
    for k in (1, 2, 3):
        copies.arrived(("v", "z", k))
        copies.arrived(("v", "zx", k))
    copies.arrived(("v", "x", 0))
    note.wait()
    kept.start()

    lanes = lax.broadcasted_iota(jnp.int32, (TILE, W), 1)
    rows = lax.broadcasted_iota(jnp.int32, (TILE, W), 0)
    joined = jnp.zeros((16, W), jnp.float32)
    for o in range(8):
        pick = ((lanes == rows + o * part) & (rows < part)).astype(low)
        joined = joined + product(got[o], pick)
        for j in range(3):
            i = o * 3 + j
            inner[i // 6 : i // 6 + 1, (i % 6) * TILE : (i % 6 + 1) * TILE] = got[
                o, 8 + j : 9 + j, :
            ].astype(jnp.float32)
    small[...] = joined[:8]

    @pl.loop(0, 4)
    def _(block):
        span = pl.ds(pl.multiple_of(block * 256, 256), 256)
        value = x_ref[span, :]
        q_ref[span, :] = (product(value, w0[0]) + small[0:1, :]).astype(low)
        k_ref[span, :] = product(value, w0[1]).astype(low)
        v_ref[span, :] = (product(value, w0[2]) + small[1:2, :]).astype(low)
        for which, events in enumerate(DURING_PROJECTIONS):

            @pl.when(block == which)
            def _():
                pump(events)

    leaving = [
        pltpu.make_async_copy(ref, into, own_sem.at[4 + i])
        for i, (ref, into) in enumerate(((q_ref, q_out), (k_ref, k_out), (v_ref, v_out)))
    ]
    for copy in leaving:
        copy.start()

    def at_half(pair, half):
        for which, events in enumerate(DURING_ATTENTION[half::2]):
            if events:
                pl.when(pair == which)(functools.partial(pump, events))

    @pl.loop(0, 6)
    def _(pair):
        columns = pl.ds(pl.multiple_of(pair * TILE, TILE), TILE)
        attend_pair(
            key_ids, query_ids, q_ref.at[:, columns], k_ref.at[:, columns], v_ref.at[:, columns],
            out_ref.at[:, columns], lse_ref.at[pair], v_turned, lambda: at_half(pair, 0),
        )
        at_half(pair, 1)

    pump(LATE)
    settle(1)
    settle(2)
    copies.drain()
    for copy in own:
        copy.wait()
    kept.wait()
    for copy in leaving:
        copy.wait()


Z_ROUTES = (
    (0, 1, 1), (1, 0, 1), (1, 2, 1), (2, 3, 1), (2, 1, 2), (3, 2, 2), (1, 3, 2), (2, 0, 2),
    (0, 2, 3), (3, 1, 3), (1, 0, 3), (2, 3, 3),
)
GATHER_COPIES = 7 + 3 * (2 * (1 + 12) + 2 * 3 + 7 * 4)


def run(g, *order):
    return [(name[0], g, int(name[1])) for name in order]


EARLY = run(0, "p0", "p1", "p2", "c0", "p3", "p4", "c1", "p5", "c2", "p6", "c3", "c4", "c5", "c6")
DURING_PROJECTIONS = [run(1, "p0"), run(1, "p1"), run(1, "p2", "c0"), run(1, "p3", "c1")]
DURING_ATTENTION = [
    run(1, "p4"),
    run(1, "c2"),
    run(1, "p5", "c3", "p6"),
    run(2, "p0") + run(1, "c4"),
    run(2, "p1"),
    run(1, "c5", "c6"),
    run(2, "p2", "c0"),
    run(2, "p3"),
    run(2, "c1"),
    run(2, "p4"),
    run(2, "c2", "p5"),
    run(2, "c3"),
]
LATE = run(2, "p6", "c4", "c5", "c6")


def gather_attend(shards, rows, key_ids, query_ids, pull, mem):
    low, full = jnp.bfloat16, jnp.float32
    count = rows.shape[0]
    vectors = shards[-1]
    anywhere, near = pl.BlockSpec(memory_space=pl.ANY), pl.BlockSpec(memory_space=pltpu.VMEM)
    thin = jax.ShapeDtypeStruct((count, W), low)
    return pl.pallas_call(
        functools.partial(gather_attend_kernel, mem),
        out_shape=(
            jax.ShapeDtypeStruct((4, W, W), low),
            jax.ShapeDtypeStruct((4, W, W), low),
            jax.ShapeDtypeStruct((4 * W, W), low),
            jax.ShapeDtypeStruct((8, W), full),
            jax.ShapeDtypeStruct((4, W), full),
            thin,
            thin,
            thin,
            thin,
            jax.ShapeDtypeStruct((W // TILE, count // TILE, 2 * TILE), full),
            thin,
        ),
        in_specs=[anywhere] * 7 + [near] * 4,
        out_specs=[anywhere] * 3 + [near] * 2 + [anywhere] * 3 + [near] * 3,
        scratch_shapes=[
            pltpu.VMEM((count, W), low),
            pltpu.VMEM((count, W), low),
            pltpu.VMEM((count, W), low),
            pltpu.VMEM((4, W, W), low),
            pltpu.VMEM((4, W // 8, W), low),
            pltpu.VMEM(shards[5].shape, low),
            pltpu.VMEM(vectors.shape, low),
            pltpu.VMEM((8,) + vectors.shape, low),
            pltpu.VMEM((TILE, count), low),
            pltpu.SemaphoreType.DMA((GATHER_COPIES,)),
            pltpu.SemaphoreType.DMA((GATHER_COPIES,)),
            pltpu.SemaphoreType.DMA((7,)),
            pltpu.SemaphoreType.DMA((10,)),
        ],
        compiler_params=pltpu.CompilerParams(
            collective_id=0, has_side_effects=True, vmem_limit_bytes=48 << 20
        ),
        name="gather_attend",
    )(*shards, rows, key_ids, query_ids, pull)


def attend_back(key_ids, query_ids, query, keys, values, grads, lse):
    rows, width = query.shape
    pair = 2 * HEAD_DIM
    count = rows // TILE
    column = pl.BlockSpec((rows, pair), lambda h: (0, h))
    whole = lambda a: pl.BlockSpec(a.shape, lambda h: (0, 0))
    return pl.pallas_call(
        attend_back_kernel,
        grid=(width // pair,),
        out_shape=(jax.ShapeDtypeStruct((rows, width), jnp.bfloat16),) * 3,
        in_specs=[whole(key_ids), whole(query_ids)]
        + [column] * 4
        + [pl.BlockSpec((1, count, 2 * TILE), lambda h: (h, 0, 0))],
        out_specs=[column] * 3,
        scratch_shapes=[
            pltpu.VMEM((pair, rows), jnp.bfloat16),
            pltpu.VMEM((rows, pair), jnp.float32),
            pltpu.VMEM((rows, pair), jnp.float32),
        ],
        compiler_params=pltpu.CompilerParams(vmem_limit_bytes=48 << 20),
        name="attend_back",
    )(key_ids, query_ids, query, keys, values, grads, lse)


ERFC_TERMS = (
    -1.26551223, 1.00002368, 0.37409196, 0.09678418, -0.18628806,
    0.27886807, -1.13520398, 1.48851587, -0.82215223, 0.17087277,
)


def gelu_and_slope(value):
    half_square = value * value * 0.5
    step = 1.0 / (1.0 + jnp.abs(value) * (0.5 * 0.5**0.5))
    power = ERFC_TERMS[-1]
    for term in ERFC_TERMS[-2::-1]:
        power = power * step + term
    tail = 0.5 * step * jnp.exp(power - half_square)
    cover = jnp.where(value < 0, tail, 1.0 - tail)
    density = jnp.exp(-half_square) * ((0.5 / math.pi) ** 0.5)
    return value * cover, cover + value * density


def reduce_attend_kernel(
    mem, q_in, k_in, v_in, g_in, x_in, gh_in, w_in, go, g1, g2, layer_in, lse_ref, key_ids,
    query_ids, sums_in, inner_in, tokens_ref, memory_ref, layer_ref, rq, rk, rw, ro, r1, r2, rv,
    gx, held, x_kept, x_turned, grads, dw, k_turned, k_total, v_total,
    keep0, keep1, keep2, core0, core1, core2, got_y, got_x, got_z, ends, vec,
    send, recv, load_sem, own_sem,
):
    rep, owner, y, c, z, x, where = place()
    part = W // 8
    low = jnp.bfloat16
    loads = [
        pltpu.make_async_copy(source, into, load_sem.at[i])
        for i, (source, into) in enumerate(
            [(source, held.at[i]) for i, source in enumerate((q_in, k_in, v_in, g_in))]
            + [(x_in, x_kept), (gh_in, gx), (go, dw.at[3])]
        )
    ]
    for load in loads:
        load.start()
    copies = Copies(send, recv)
    keep, core = (keep0, keep1, keep2), (core0, core1, core2)
    order = (1, 3, 2, 0)
    flat = [(k, o) for k in order for o in (1, 0)]

    def shard(k, o):
        return ((z + k) % 4) * 2 + (1 - x if o else x)

    def lanes(kind, this_core):
        which = 0 if this_core else 1
        own_core = c if which == 0 else 1 - c
        at = {
            0: 2 * TILE + ((1 - y) * 2 + own_core) * TILE,
            1: own_core * TILE,
            2: 2 * TILE + (y * 2 + own_core) * TILE,
        }[kind]
        return at

    def columns(kind, this_core, block=0):
        return pl.ds(pl.multiple_of(block * W + lanes(kind, this_core), TILE), TILE)

    def sources(g, kind, this_core):
        if g == 0:
            return [dw.at[j, :, columns(kind, this_core)] for j in range(4)]
        if g == 1:
            return [g1.at[:, columns(kind, this_core, j)] for j in range(4)]
        return [g2.at[:, :, columns(kind, this_core)]]

    def targets(g, kind, refs):
        return [refs[g].at[kind, j] for j in range(4)] if g < 2 else [refs[g].at[kind]]

    def cut(g, kind, refs, k, o):
        if g == 2:
            return refs[g].at[kind, pl.ds(shard(k, o) * 4, 4), :, :]
        return refs[g].at[kind, :, pl.ds(shard(k, o) * part, part), :]

    own = {}
    for g in (2, 1, 0):
        for kind in (0, 1, 2):
            pairs = zip(sources(g, kind, False), targets(g, kind, core))
            for j, (source, into) in enumerate(pairs):
                copies.plan((g, "core", kind, j), source, into, where["core"])
            pairs = zip(sources(g, kind, True), targets(g, kind, keep))
            for j, (source, into) in enumerate(pairs):
                own[g, kind, j] = pltpu.make_async_copy(source, into, own_sem.at[len(own)])
        for i, (k, o) in enumerate(flat):
            copies.plan((g, "y", k, o), cut(g, 0, keep, k, o), got_y.at[g, i], where["y"])
        for k in order:
            for s, kind in enumerate((1, 2)):
                copies.plan(
                    (g, kind, "x", k), cut(g, kind, keep, k, 1), got_x.at[g, s, k], where["x"]
                )
                if k:
                    copies.plan(
                        (g, kind, "z", k), cut(g, kind, keep, k, 0), got_z.at[g, s, k - 1],
                        where["z", k],
                    )
        copies.plan((g, 1, "ey"), ends.at[g, 0, 0], ends.at[g, 0, 1], where["y"])
        copies.plan((g, 1, "ecore"), ends.at[g, 0, 2], ends.at[g, 0, 3], where["core"])
        copies.plan((g, 2, "ey"), ends.at[g, 1, 0], ends.at[g, 1, 1], where["y"])
        copies.plan((g, 2, "ecore"), ends.at[g, 1, 0], ends.at[g, 1, 2], where["core"])
        copies.plan((g, 2, "ediagonal"), ends.at[g, 1, 1], ends.at[g, 1, 3], where["core"])
    copies.plan(("v", "core"), vec.at[0], vec.at[1], where["core"])
    copies.plan(("v", "y"), vec.at[2], vec.at[3], where["y"])
    copies.plan(("v", "x"), vec.at[4], vec.at[5], where["x"])
    for k in (1, 2, 3):
        copies.plan(("v", "z", k), vec.at[6], vec.at[6 + k], where["z", k])

    def begin(g, blocks):
        for kind in (0, 1, 2):
            for j in blocks:
                copies.go((g, "core", kind, j))
                own[g, kind, j].start()

    def ready(g, kind):
        for j in range(4 if g < 2 else 1):
            own[g, kind, j].wait()
            copies.arrived((g, "core", kind, j))

    def put(target, *refs):
        target[...] = total(*refs).astype(low)

    def cores(g):
        ready(g, 0)
        for k, o in flat:
            here = cut(g, 0, keep, k, o)
            put(here, here, cut(g, 0, core, k, o))
            copies.go((g, "y", k, o))
        ready(g, 1)
        for k in order:
            here = cut(g, 1, keep, k, 1)
            put(here, here, cut(g, 1, core, k, 1))
            copies.go((g, 1, "x", k))
        ready(g, 2)

    def over_y(g, k):
        copies.arrived((g, "y", k, 1))
        here = cut(g, 2, keep, k, 1)
        put(here, here, cut(g, 2, core, k, 1), got_y.at[g, flat.index((k, 1))])
        copies.go((g, 2, "x", k))

    def half_over_x(g, k):
        copies.arrived((g, 1, "x", k))
        here = cut(g, 1, keep, k, 0)
        put(here, here, cut(g, 1, core, k, 0), got_x.at[g, 0, k])
        copies.go((g, 1, "z", k))

    def over_x(g, k):
        copies.arrived((g, "y", k, 0))
        copies.arrived((g, 2, "x", k))
        here = cut(g, 2, keep, k, 0)
        put(
            here, here, cut(g, 2, core, k, 0), got_y.at[g, flat.index((k, 0))], got_x.at[g, 1, k]
        )
        copies.go((g, 2, "z", k))

    def half_over_z(g):
        copies.arrived((g, 1, "x", 0))
        for k in (1, 2, 3):
            copies.arrived((g, 1, "z", k))
        put(
            ends.at[g, 0, 0], cut(g, 1, keep, 0, 0), cut(g, 1, core, 0, 0), got_x.at[g, 0, 0],
            *(got_z.at[g, 0, k] for k in range(3)),
        )
        copies.go((g, 1, "ey"))

    def over_z(g):
        copies.arrived((g, 2, "x", 0))
        copies.arrived((g, "y", 0, 0))
        for k in (1, 2, 3):
            copies.arrived((g, 2, "z", k))
        put(
            ends.at[g, 1, 0], cut(g, 2, keep, 0, 0), cut(g, 2, core, 0, 0), got_x.at[g, 1, 0],
            got_y.at[g, flat.index((0, 0))], *(got_z.at[g, 1, k] for k in range(3)),
        )
        copies.go((g, 2, "ey"))
        copies.go((g, 2, "ecore"))

    def write(g, s, slot, at):
        value = ends[g, s, slot].astype(jnp.float32)
        for j in range(4):
            if g == 0:
                (rq, rk, rw, ro)[j][:, pl.ds(pl.multiple_of(at, TILE), TILE)] = value[j]
            elif g == 1:
                r1[:, pl.ds(pl.multiple_of(j * W + at, TILE), TILE)] = value[j]
            else:
                r2[j * part : (j + 1) * part, pl.ds(pl.multiple_of(at, TILE), TILE)] = value[j]

    def half_finish(g):
        copies.arrived((g, 1, "ey"))
        put(ends.at[g, 0, 2], ends.at[g, 0, 0], ends.at[g, 0, 1])
        copies.go((g, 1, "ecore"))

    def finish(g):
        copies.arrived((g, 2, "ey"))
        copies.go((g, 2, "ediagonal"))
        write(g, 0, 2, lanes(1, True))
        write(g, 1, 0, lanes(2, True))
        write(g, 1, 1, lanes(0, True))

    def close(g):
        copies.arrived((g, 2, "ecore"))
        write(g, 1, 2, lanes(2, False))
        copies.arrived((g, 1, "ecore"))
        write(g, 0, 3, lanes(1, False))
        copies.arrived((g, 2, "ediagonal"))
        write(g, 1, 3, lanes(0, False))

    acts = {
        "a": cores, "h": half_over_x, "b": over_y, "c": over_x, "s": half_over_z, "d": over_z,
        "t": half_finish, "f": finish, "g": close,
    }

    def pump(events):
        for event in events:
            act = acts[event[0]]
            if len(event) == 3:
                act(int(event[1]), int(event[2]))
            else:
                act(int(event[1]))

    greet(where)
    begin(2, (0,))
    begin(1, range(4))
    for load in loads:
        load.wait()
    begin(0, (3,))
    x_turned[...] = x_kept[...].T
    pump(BEFORE_BACK)

    def at_half(pair, half):
        for which, events in enumerate(DURING_BACK[half::2]):
            if events:
                pl.when(pair == which)(functools.partial(pump, events))

    @pl.loop(0, 6)
    def _(pair):
        at = pl.ds(pl.multiple_of(pair * TILE, TILE), TILE)
        attend_back_pair(
            key_ids, query_ids, *(held.at[i, :, at] for i in range(4)), lse_ref.at[pair],
            *(grads.at[i, :, at] for i in range(3)), k_turned, k_total, v_total,
            lambda: at_half(pair, 0),
        )
        at_half(pair, 1)

    fetch = [pltpu.make_async_copy(w_in.at[i], held.at[i, 0:W, :], load_sem.at[i]) for i in range(3)]
    fetch.append(pltpu.make_async_copy(layer_in, held.at[3], load_sem.at[3]))
    for copy in fetch:
        copy.start()
    for i in range(3):

        @pl.loop(0, 3)
        def _(block):
            span = pl.ds(pl.multiple_of(block * 256, 256), 256)
            dw[i, span, :] = product(x_turned[span, :], grads[i]).astype(low)

        begin(0, (i,))
        pump(DURING_WEIGHTS[i])
    vec[0, 0:1, :] = column_sum(grads[0])[None]
    vec[0, 1:2, :] = column_sum(grads[2])[None]
    vec[0, 2:8, :] = sums_in[2:8, :]
    vec[0, 8:12, :] = inner_in[...]
    vec[0, 12:16, :] = jnp.zeros((4, W), jnp.float32)
    copies.go(("v", "core"))
    pump(("a0",))
    copies.arrived(("v", "core"))
    vec[2] = vec[0] + vec[1]
    copies.go(("v", "y"))
    for copy in fetch:
        copy.wait()

    @pl.loop(0, 4)
    def _(block):
        span = pl.ds(pl.multiple_of(block * 256, 256), 256)
        value = gx[span, :]
        for i in range(3):
            value = value + against(grads[i, span, :], held[i, 0:W, :])
        gx[span, :] = value
        for which, events in enumerate(DURING_ROWS):

            @pl.when(block == which)
            def _():
                pump(events)

    copies.arrived(("v", "y"))
    vec[4] = vec[2] + vec[3]
    copies.go(("v", "x"))
    seg = gx.shape[0] - 2 * mem
    tokens_ref[...] = gx[...].astype(low)
    memory_ref[...] = (gx[seg : seg + mem, :] + gx[seg + mem : seg + 2 * mem, :]).astype(low)
    pump(AFTER_ROWS)
    to_memory_first(held.at[3], layer_ref, mem)
    copies.arrived(("v", "x"))
    vec[6] = vec[4] + vec[5]
    for k in (1, 2, 3):
        copies.go(("v", "z", k))
    pump(LAST)
    for k in (1, 2, 3):
        copies.arrived(("v", "z", k))
    rv[...] = (vec[6] + vec[7]) + (vec[8] + vec[9])
    pump(("g2", "g1", "g0"))
    copies.drain()


REDUCE_COPIES = 3 + 12 + 12 + 3 * (8 + 4 + 4 + 3 + 3 + 5) + 6
BEFORE_BACK = ("a2",)
DURING_BACK = (
    (),
    ("h21", "b21", "a1", "h23"),
    ("b23", "h22"),
    ("c21", "b22"),
    ("h11", "s2"),
    ("b20", "h13", "h12"),
    ("b11", "c23"),
    ("c22", "b13"),
    ("s1", "c11", "b12"),
    ("c13", "d2"),
    ("b10", "c12"),
    ("t2",),
)
DURING_WEIGHTS = (
    ("t1",),
    ("f2", "d1"),
    (),
)
DURING_ROWS = (
    ("f1",),
    (),
    ("h01", "b01"),
    ("h03",),
)
AFTER_ROWS = ("b03", "h02", "c01", "b02", "c03", "s0")
LAST = ("b00", "c02", "t0", "d0", "f0")


def reduce_attend(
    mem, query, keys, values, grad_mixed, rows, grad_hidden, weights, grad_out, grad_inner,
    grad_outer, layer, lse, key_ids, query_ids, sums, inner_sums,
):
    low, full = jnp.bfloat16, jnp.float32
    count = rows.shape[0]
    part = W // 8
    anywhere, near = pl.BlockSpec(memory_space=pl.ANY), pl.BlockSpec(memory_space=pltpu.VMEM)
    slab = jax.ShapeDtypeStruct((part, W), full)
    piece = (4, part, TILE)
    wide, tall = pltpu.VMEM((3, 4, W, TILE), low), pltpu.VMEM((3, 32, part, TILE), low)
    return pl.pallas_call(
        functools.partial(reduce_attend_kernel, mem),
        out_shape=(
            jax.ShapeDtypeStruct((count, W), low),
            jax.ShapeDtypeStruct((mem, W), low),
            jax.ShapeDtypeStruct((count, W), low),
            slab,
            slab,
            slab,
            slab,
            jax.ShapeDtypeStruct((part, 4 * W), full),
            jax.ShapeDtypeStruct((4 * part, W), full),
            jax.ShapeDtypeStruct((16, W), full),
        ),
        in_specs=[anywhere] * 11 + [near] * 5,
        out_specs=[near] * 10,
        scratch_shapes=[
            pltpu.VMEM((count, W), full),
            pltpu.VMEM((4, count, W), low),
            pltpu.VMEM((count, W), low),
            pltpu.VMEM((W, count), low),
            pltpu.VMEM((3, count, W), low),
            pltpu.VMEM((4, W, W), low),
            pltpu.VMEM((TILE, count), low),
            pltpu.VMEM((count, TILE), full),
            pltpu.VMEM((count, TILE), full),
            wide,
            wide,
            tall,
            wide,
            wide,
            tall,
            pltpu.VMEM((3, 8) + piece, low),
            pltpu.VMEM((3, 2, 4) + piece, low),
            pltpu.VMEM((3, 2, 3) + piece, low),
            pltpu.VMEM((3, 2, 4) + piece, low),
            pltpu.VMEM((10, 16, W), full),
            pltpu.SemaphoreType.DMA((REDUCE_COPIES,)),
            pltpu.SemaphoreType.DMA((REDUCE_COPIES,)),
            pltpu.SemaphoreType.DMA((7,)),
            pltpu.SemaphoreType.DMA((27,)),
        ],
        compiler_params=pltpu.CompilerParams(
            collective_id=1, has_side_effects=True, vmem_limit_bytes=62 << 20
        ),
        name="reduce_attend",
    )(
        query, keys, values, grad_mixed, rows, grad_hidden, weights, grad_out, grad_inner,
        grad_outer.reshape(32, part, W), layer, lse, key_ids, query_ids, sums, inner_sums,
    )


def normalise(value):
    mean = jnp.mean(value, axis=1, keepdims=True)
    centred = value - mean
    scale = lax.rsqrt(jnp.mean(centred * centred, axis=1, keepdims=True) + 1e-05)
    return centred * scale, scale


def normalise_back(grad, unit, scale):
    middle = jnp.mean(grad, axis=1, keepdims=True)
    along = jnp.mean(grad * unit, axis=1, keepdims=True)
    return scale * (grad - middle - unit * along)


def chain_kernel(
    mixed_ref, rows_ref, pull_ref, wo_ref, w1_ref, w2_ref, small_ref, b1_ref,
    out_ref, y1_ref, u_ref, gz_ref, gf_ref, gh_ref, ga_ref, gmix_ref, sums_ref, b1_sum_ref,
    slope_ref,
):
    low = jnp.bfloat16

    @pl.when(pl.program_id(0) == 0)
    def _():
        sums_ref[...] = jnp.zeros_like(sums_ref)
        b1_sum_ref[...] = jnp.zeros_like(b1_sum_ref)

    def small(i):
        return small_ref[i : i + 1, :]

    def gather_sum(ref, i, value):
        ref[i : i + 1, :] += jnp.sum(value, axis=0, keepdims=True)

    hidden = rows_ref[...].astype(jnp.float32) + product(mixed_ref[...], wo_ref[0]) + small(2)
    unit_one, scale_one = normalise(hidden)
    y1 = unit_one * small(3) + small(4)
    y1_low = y1.astype(low)
    y1_ref[...] = y1_low
    second = y1 + small(5)
    for r in range(4):
        inner = product(y1_low, w1_ref[r]) + b1_ref[r : r + 1, :]
        active, slope = gelu_and_slope(inner)
        active = active.astype(low)
        u_ref[:, r * W : (r + 1) * W] = active
        slope_ref[:, r * W : (r + 1) * W] = slope
        second = second + product(active, w2_ref[r * W : (r + 1) * W, :])
    unit_two, scale_two = normalise(second)
    out_ref[...] = (unit_two * small(6) + small(7)).astype(low)
    pull = pull_ref[...].astype(jnp.float32)
    gather_sum(sums_ref, 6, pull * unit_two)
    gather_sum(sums_ref, 7, pull)
    grad_second = normalise_back(pull * small(6), unit_two, scale_two)
    gz = grad_second.astype(low)
    gz_ref[...] = gz
    gather_sum(sums_ref, 5, gz.astype(jnp.float32))
    grad_y1 = grad_second
    for r in range(4):
        gf = against(gz, w2_ref[r * W : (r + 1) * W, :]) * slope_ref[:, r * W : (r + 1) * W]
        gf = gf.astype(low)
        gf_ref[:, r * W : (r + 1) * W] = gf
        gather_sum(b1_sum_ref, r, gf.astype(jnp.float32))
        grad_y1 = grad_y1 + against(gf, w1_ref[r])
    gather_sum(sums_ref, 3, grad_y1 * unit_one)
    gather_sum(sums_ref, 4, grad_y1)
    grad_hidden = normalise_back(grad_y1 * small(3), unit_one, scale_one)
    gh_ref[...] = grad_hidden
    ga = grad_hidden.astype(low)
    ga_ref[...] = ga
    gather_sum(sums_ref, 2, ga.astype(jnp.float32))
    gmix_ref[...] = against(ga, wo_ref[0]).astype(low)


def chain(mixed, rows, pull, weights, inner_blocks, outer_mat, small, inner_bias):
    count, width = rows.shape
    step = 256
    low, full = jnp.bfloat16, jnp.float32
    thin = pl.BlockSpec((step, width), lambda i: (i, 0))
    fat = pl.BlockSpec((step, 4 * width), lambda i: (i, 0))
    held = lambda shape: pl.BlockSpec(shape, lambda i: (0,) * len(shape))
    once = pl.Buffered(1)
    return pl.pallas_call(
        chain_kernel,
        grid=(count // step,),
        out_shape=(
            jax.ShapeDtypeStruct((count, width), low),
            jax.ShapeDtypeStruct((count, width), low),
            jax.ShapeDtypeStruct((count, 4 * width), low),
            jax.ShapeDtypeStruct((count, width), low),
            jax.ShapeDtypeStruct((count, 4 * width), low),
            jax.ShapeDtypeStruct((count, width), full),
            jax.ShapeDtypeStruct((count, width), low),
            jax.ShapeDtypeStruct((count, width), low),
            jax.ShapeDtypeStruct((8, width), full),
            jax.ShapeDtypeStruct((4, width), full),
        ),
        in_specs=[
            thin, thin, thin,
            pl.BlockSpec((1, width, width), lambda i: (3, 0, 0), pipeline_mode=once),
            pl.BlockSpec((4, width, width), lambda i: (0, 0, 0), pipeline_mode=once),
            pl.BlockSpec((4 * width, width), lambda i: (0, 0), pipeline_mode=once),
            held((8, width)), held((4, width)),
        ],
        out_specs=[thin, thin, fat, thin, fat, thin, thin, thin, held((8, width)), held((4, width))],
        scratch_shapes=[pltpu.VMEM((step, 4 * width), full)],
        compiler_params=pltpu.CompilerParams(vmem_limit_bytes=60 << 20),
        name="chain",
    )(mixed, rows, pull, weights, inner_blocks, outer_mat, small, inner_bias)


def on_device(
    tokens,
    read_memory,
    doc_ids,
    w_query,
    w_key,
    w_value,
    w_out,
    query_bias,
    value_bias,
    out_bias,
    norm_one_gain,
    norm_one_bias,
    w_inner,
    inner_bias,
    w_outer,
    outer_bias,
    norm_two_gain,
    norm_two_bias,
    out_grad,
):
    owners = lax.axis_size("fsdp")
    wide = owners == 8 and lax.axis_size("rep") == 4
    part = w_query.shape[0]
    low = jnp.bfloat16
    small = pack(
        jnp.stack(
            [
                query_bias, value_bias, out_bias, norm_one_gain,
                norm_one_bias, outer_bias, norm_two_gain, norm_two_bias,
            ]
        )[None],
        inner_bias[None],
    )[0]
    seqs, seg = doc_ids.shape
    width = tokens.shape[1]
    mem = read_memory.shape[0] // seqs
    length = seg + 2 * mem
    memory_rows = read_memory.reshape(seqs, mem, width)
    rows = jnp.concatenate([tokens.reshape(seqs, seg, width), memory_rows, memory_rows], axis=1)
    rows = rows.reshape(seqs * length, width)
    marks = jnp.full((seqs, 2 * mem), -1, jnp.int32)
    ids = jnp.concatenate([doc_ids, marks], axis=1)

    def each(function, *arrays):
        results = []
        for s in range(seqs):
            own = slice(s * length, (s + 1) * length)
            spread = jnp.broadcast_to(ids[s][:, None], (length, TILE))
            by_block = ids[s].reshape(length // TILE, TILE)
            results.append(function(spread, by_block, *[a[own] for a in arrays]))
        return results

    shards = (w_query, w_key, w_value, w_out, w_inner, w_outer, small)
    wide = wide and seqs == 1
    if wide:
        spread, by_block = each(lambda *a: a)[0]
        (
            weights, inner_blocks, outer_mat, vectors, inner_shift, query, keys, values, mixed,
            lse, out_rows,
        ) = gather_attend(shards, rows, spread, by_block, out_grad, mem)
    else:
        out_rows = out_grad.reshape(seqs, length, width)
        out_rows = jnp.concatenate(
            [out_rows[:, mem : mem + seg], out_rows[:, :mem], out_rows[:, mem + seg :]], axis=1
        ).reshape(seqs * length, width)
        weights, inner_blocks, outer_mat, packed = plain_gather(*shards)
        vectors, inner_shift = unpack(packed.astype(jnp.float32), part)
        query = (product(rows, weights[0]) + vectors[0]).astype(low)
        keys = product(rows, weights[1]).astype(low)
        values = (product(rows, weights[2]) + vectors[1]).astype(low)
        pairs = each(attend, query, keys, values)
        mixed = jnp.concatenate([pair[0] for pair in pairs], axis=0)
    output, normed, active, grad_outer, grad_inner, grad_residual, grad_branch, grad_mixed, sums, inner_sums = chain(
        mixed, rows, out_rows, weights, inner_blocks, outer_mat, vectors, inner_shift
    )
    grad_w_outer = inner_rows(active, grad_outer).astype(low)
    grad_w_inner = inner_rows(normed, grad_inner).astype(low)
    grad_w_out = inner_rows(mixed, grad_branch).astype(low)
    if wide:
        grad_tokens, grad_memory, layer_out, *shares, joined = reduce_attend(
            mem, query, keys, values, grad_mixed, rows, grad_residual, weights, grad_w_out,
            grad_w_inner, grad_w_outer, output, lse, spread, by_block, sums, inner_sums,
        )
        grad_tokens = grad_tokens[:seg]
        place_of = lax.axis_index("fsdp")
        last = lax.dynamic_slice(joined[:8], (0, place_of * part), (8, part))
        last_inner = lax.dynamic_slice(
            joined[8:12].reshape(-1), (place_of * 4 * part,), (4 * part,)
        )
    else:
        triples = [
            attend_back(spread, by_block, q, k, v, g, pairs[s][1])
            for s, (spread, by_block, q, k, v, g) in enumerate(
                each(lambda *a: a, query, keys, values, grad_mixed)
            )
        ]
        grad_query_low, grad_keys_low, grad_values_low = (
            jnp.concatenate([triple[i] for triple in triples], axis=0) for i in range(3)
        )
        grad_w_query = inner_rows(rows, grad_query_low).astype(low)
        grad_w_key = inner_rows(rows, grad_keys_low).astype(low)
        grad_w_value = inner_rows(rows, grad_values_low).astype(low)
        sums = jnp.concatenate(
            [column_sum(grad_query_low)[None], column_sum(grad_values_low)[None], sums[2:]], axis=0
        )
        grad_rows = (
            grad_residual
            + against(grad_query_low, weights[0])
            + against(grad_keys_low, weights[1])
            + against(grad_values_low, weights[2])
        )
        *shares, share_small = plain_reduce(
            grad_w_query,
            grad_w_key,
            grad_w_value,
            grad_w_out,
            grad_w_inner,
            grad_w_outer,
            pack(
                sums.reshape(8, owners, part).transpose(1, 0, 2),
                inner_sums.reshape(owners, 4 * part),
            ),
        )
        last, last_inner = unpack(share_small[None], part)
        grad_rows = grad_rows.reshape(seqs, length, width)
        grad_tokens = grad_rows[:, :seg].reshape(seqs * seg, width).astype(jnp.bfloat16)
        grad_memory = (
            (grad_rows[:, seg : seg + mem] + grad_rows[:, seg + mem :])
            .reshape(seqs * mem, width)
            .astype(jnp.bfloat16)
        )
        layer_out = output.reshape(seqs, length, width)
        layer_out = jnp.concatenate(
            [layer_out[:, seg : seg + mem], layer_out[:, :seg], layer_out[:, seg + mem :]], axis=1
        ).reshape(seqs * length, width)
    return (
        layer_out,
        grad_tokens,
        grad_memory,
        *shares[:4],
        *(last[i] for i in range(5)),
        shares[4],
        last_inner.reshape(-1),
        shares[5],
        *(last[i] for i in range(5, 8)),
    )


def solution(mesh):
    return jax.shard_map(
        on_device,
        mesh=mesh,
        in_specs=(
            P(("rep", "fsdp"), None),
            P(("rep", "fsdp"), None),
            P(("rep", "fsdp"), None),
            P("fsdp", None),
            P("fsdp", None),
            P("fsdp", None),
            P("fsdp", None),
            P("fsdp"),
            P("fsdp"),
            P("fsdp"),
            P("fsdp"),
            P("fsdp"),
            P("fsdp", None),
            P("fsdp"),
            P("fsdp", None),
            P("fsdp"),
            P("fsdp"),
            P("fsdp"),
            P(("rep", "fsdp"), None),
        ),
        out_specs=(
            P(("rep", "fsdp"), None),
            P(("rep", "fsdp"), None),
            P(("rep", "fsdp"), None),
            P("fsdp", None),
            P("fsdp", None),
            P("fsdp", None),
            P("fsdp", None),
            P("fsdp"),
            P("fsdp"),
            P("fsdp"),
            P("fsdp"),
            P("fsdp"),
            P("fsdp", None),
            P("fsdp"),
            P("fsdp", None),
            P("fsdp"),
            P("fsdp"),
            P("fsdp"),
        ),
        check_vma=False,
    )
```

```python
import functools
import math

import jax
import jax.numpy as jnp
from jax import lax
from jax.experimental import pallas as pl
from jax.experimental.pallas import tpu as pltpu
from jax.sharding import PartitionSpec as P

MESH_ID = pl.DeviceIdType.MESH
W = 768


def only_if(condition, act):
    if condition is None:
        act()
    else:
        pl.when(condition)(act)


class Copies:
    def __init__(self, send, recv):
        self.send, self.recv, self.made = send, recv, {}

    def plan(self, name, src, dst, to, leaves=None, comes=None):
        slot = len(self.made)

        def describe(src):
            return pltpu.make_async_remote_copy(
                src_ref=src,
                dst_ref=dst,
                send_sem=self.send.at[slot],
                recv_sem=self.recv.at[slot],
                device_id=to,
                device_id_type=MESH_ID,
            )

        self.made[name] = (describe, src, leaves, comes)

    def go(self, name):
        describe, src, leaves, _ = self.made[name]
        only_if(leaves, lambda: describe(src).start())

    def start(self, name, src, dst, to):
        self.plan(name, src, dst, to)
        self.go(name)

    def arrived(self, name):
        describe, src, _, comes = self.made[name]
        only_if(comes, lambda: describe(src).wait_recv())

    def drain(self):
        for describe, src, leaves, _ in self.made.values():
            only_if(leaves, functools.partial(lambda describe, src: describe(src).wait_send(), describe, src))


def place():
    rep, owner = lax.axis_index("rep"), lax.axis_index("fsdp")
    y, c, z, x = rep // 2, rep % 2, owner // 2, owner % 2
    where = {
        "core": (y * 2 + 1 - c, owner),
        "y": ((1 - y) * 2 + c, owner),
        "x": (rep, z * 2 + 1 - x),
    }
    for k in (1, 2, 3):
        where["z", k] = (rep, ((z + k) % 4) * 2 + x)
        where["zx", k] = (rep, ((z + k) % 4) * 2 + 1 - x)
    return rep, owner, y, c, z, x, where


def greet(where):
    barrier = pltpu.get_barrier_semaphore()
    for to in where.values():
        pl.semaphore_signal(barrier, inc=1, device_id=to, device_id_type=MESH_ID)
    pl.semaphore_wait(barrier, len(where))


def total(*refs):
    value = refs[0][...].astype(jnp.float32)
    for ref in refs[1:]:
        value = value + ref[...].astype(jnp.float32)
    return value


def inner_lines(part):
    return -(-4 * part // 128)


def pack(vectors, inner):
    owners, _, part = vectors.shape
    lines = inner_lines(part)
    first = jnp.pad(vectors, ((0, 0), (0, 0), (0, 128 - part)))
    second = jnp.pad(inner, ((0, 0), (0, lines * 128 - 4 * part)))
    second = second.reshape(owners, lines, 128)
    return jnp.pad(jnp.concatenate([first, second], axis=1), ((0, 0), (0, 8 - lines), (0, 0)))


def unpack(packed, part):
    owners = packed.shape[0]
    lines = inner_lines(part)
    first = packed[:, :8, :part].transpose(1, 0, 2).reshape(8, owners * part)
    second = packed[:, 8 : 8 + lines].reshape(owners, lines * 128)[:, : 4 * part]
    return first, second.reshape(4, owners * part)


def plain_gather(wq, wk, wv, wo, inner, outer, vectors):
    gathered = lax.all_gather(inner, "fsdp", axis=0, tiled=True)
    return (
        lax.all_gather(jnp.stack([wq, wk, wv, wo]), "fsdp", axis=1, tiled=True),
        gathered.reshape(W, 4, W).transpose(1, 0, 2),
        lax.all_gather(outer, "fsdp", axis=0, tiled=True),
        lax.all_gather(vectors, "fsdp", axis=0),
    )


def plain_reduce(*grads):
    def over_all(value):
        part = lax.psum_scatter(value, "fsdp", scatter_dimension=0, tiled=True)
        return lax.psum(part, "rep").astype(jnp.float32)

    return tuple(over_all(grad) for grad in grads[:-1]) + (over_all(grads[-1])[0],)


def product(left, right):
    return jnp.dot(left, right, preferred_element_type=jnp.float32)


def inner_rows(left, right):
    return lax.dot_general(
        left, right, (((0,), (0,)), ((), ())), preferred_element_type=jnp.float32
    )


def against(left, right):
    return lax.dot_general(
        left, right, (((1,), (1,)), ((), ())), preferred_element_type=jnp.float32
    )


def column_sum(values):
    return jnp.sum(values.astype(jnp.float32), axis=0)


TILE = 128
HEAD_DIM = 64
FACTOR = HEAD_DIM ** (-0.5)
HIDDEN = -1e30


def spans(i, count):
    last = count - 1
    if i == last:
        return [(0, count * TILE)]
    low, high = max(0, i - 2), min(last, i + 2)
    if high == last:
        return [(low * TILE, count * TILE)]
    return [(low * TILE, (high + 1) * TILE), (last * TILE, count * TILE)]


def two_heads(block):
    lanes = lax.broadcasted_iota(jnp.int32, block.shape, 1)
    zero = jnp.zeros_like(block)
    first = jnp.where(lanes < HEAD_DIM, block, zero)
    second = jnp.where(lanes < HEAD_DIM, zero, block)
    return jnp.concatenate([first, second], axis=0)


def own_head(value):
    rows = lax.broadcasted_iota(jnp.int32, (TILE, TILE), 0)
    return jnp.where(rows < HEAD_DIM, value[:, :TILE], value[:, TILE:]).T


def masked_scores(k_ref, key_ids, query_ids, stacked, i, span, count):
    low, high = span
    scores = against(k_ref[low:high, :], stacked)
    ids = key_ids[low:high, :]
    row = query_ids[i : i + 1, :]
    seen = ids == row
    if high == count * TILE:
        seen = seen | (ids < 0)
    if i == count - 1:
        seen = seen | (row < 0)
    return jnp.concatenate(
        [jnp.where(seen, scores[:, :TILE], HIDDEN), jnp.where(seen, scores[:, TILE:], HIDDEN)], axis=1
    )


def attend_kernel(key_ids, query_ids, q_ref, k_ref, v_ref, out_ref, lse_ref, v_turned):
    attend_pair(key_ids, query_ids, q_ref, k_ref, v_ref, out_ref, lse_ref.at[0], v_turned)


def attend_pair(
    key_ids, query_ids, q_ref, k_ref, v_ref, out_ref, lse_ref, v_turned, middle=lambda: None
):
    count = q_ref.shape[0] // TILE
    v_turned[...] = v_ref[:, :].T
    for i in range(count):
        rows = slice(i * TILE, (i + 1) * TILE)
        stacked = two_heads(q_ref[rows, :] * jnp.bfloat16(FACTOR))
        parts = spans(i, count)
        scores = [masked_scores(k_ref, key_ids, query_ids, stacked, i, p, count) for p in parts]
        peak = functools.reduce(
            jnp.maximum, [jnp.max(s, axis=0, keepdims=True) for s in scores]
        )
        weights = [jnp.exp(s - peak) for s in scores]
        total = sum(jnp.sum(w, axis=0, keepdims=True) for w in weights)
        mixed = sum(
            product(v_turned[:, low:high], w.astype(jnp.bfloat16)) for (low, high), w in zip(parts, weights)
        )
        out_ref[rows, :] = own_head(mixed * (1.0 / total)).astype(jnp.bfloat16)
        lse_ref[i : i + 1, :] = peak + jnp.log(total)
        if i == count // 2 - 1:
            middle()


def attend_back_kernel(
    key_ids, query_ids, q_ref, k_ref, v_ref, g_ref, lse_ref, gq_ref, gk_ref, gv_ref,
    k_turned, k_total, v_total,
):
    attend_back_pair(
        key_ids, query_ids, q_ref, k_ref, v_ref, g_ref, lse_ref.at[0], gq_ref, gk_ref, gv_ref,
        k_turned, k_total, v_total,
    )


def attend_back_pair(
    key_ids, query_ids, q_ref, k_ref, v_ref, g_ref, lse_ref, gq_ref, gk_ref, gv_ref,
    k_turned, k_total, v_total, middle=lambda: None,
):
    count = q_ref.shape[0] // TILE
    k_turned[...] = k_ref[:, :].T
    k_total[...] = jnp.zeros_like(k_total)
    v_total[...] = jnp.zeros_like(v_total)
    for i in range(count):
        rows = slice(i * TILE, (i + 1) * TILE)
        stacked = two_heads(q_ref[rows, :] * jnp.bfloat16(FACTOR))
        grads = two_heads(g_ref[rows, :])
        lse = lse_ref[i : i + 1, :]
        parts = spans(i, count)
        probs, pulls = [], []
        for low, high in parts:
            scores = masked_scores(k_ref, key_ids, query_ids, stacked, i, (low, high), count)
            p = jnp.exp(scores - lse)
            v_total[low:high, :] += product(p.astype(jnp.bfloat16), grads)
            probs.append(p)
            pulls.append(against(v_ref[low:high, :], grads))
        centre = sum(jnp.sum(p * g, axis=0, keepdims=True) for p, g in zip(probs, pulls))
        mixed = 0.0
        for (low, high), p, g in zip(parts, probs, pulls):
            turned = (p * (g - centre)).astype(jnp.bfloat16)
            k_total[low:high, :] += product(turned, stacked)
            mixed = mixed + product(k_turned[:, low:high], turned)
        gq_ref[rows, :] = (own_head(mixed) * FACTOR).astype(jnp.bfloat16)
        if i == count // 2 - 1:
            middle()
    gk_ref[:, :] = k_total[...].astype(jnp.bfloat16)
    gv_ref[:, :] = v_total[...].astype(jnp.bfloat16)


def attend(key_ids, query_ids, query, keys, values):
    rows, width = query.shape
    pair = 2 * HEAD_DIM
    count = rows // TILE
    column = pl.BlockSpec((rows, pair), lambda h: (0, h))
    whole = lambda a: pl.BlockSpec(a.shape, lambda h: (0, 0))
    return pl.pallas_call(
        attend_kernel,
        grid=(width // pair,),
        out_shape=(
            jax.ShapeDtypeStruct((rows, width), jnp.bfloat16),
            jax.ShapeDtypeStruct((width // pair, count, 2 * TILE), jnp.float32),
        ),
        in_specs=[whole(key_ids), whole(query_ids), column, column, column],
        out_specs=[column, pl.BlockSpec((1, count, 2 * TILE), lambda h: (h, 0, 0))],
        scratch_shapes=[pltpu.VMEM((pair, rows), jnp.bfloat16)],
        compiler_params=pltpu.CompilerParams(vmem_limit_bytes=48 << 20),
        name="attend",
    )(key_ids, query_ids, query, keys, values)


def picked(ref, low, high, *runs):
    rows = lax.broadcasted_iota(jnp.int32, (TILE, high - low), 0)
    source = lax.broadcasted_iota(jnp.int32, (TILE, high - low), 1)
    choice = None
    for first, last, offset in runs:
        one = (source == rows + offset) & (rows >= first) & (rows < last)
        choice = one if choice is None else choice | one
    return product(choice.astype(jnp.bfloat16), ref[low:high, :])


def to_tokens_first(ref, into, mem):
    count = ref.shape[0] // TILE
    end = TILE - 2 * mem
    for i in range(count - 1):
        value = picked(ref, i * TILE, i * TILE + TILE + 16, (0, TILE, mem))
        into[i * TILE : (i + 1) * TILE, :] = value.astype(jnp.bfloat16)
    last = (count - 1) * TILE
    value = picked(ref, last, last + TILE, (0, end, mem), (end + mem, TILE, 0))
    value = value + picked(ref, 0, 16, (end, end + mem, -end))
    into[last:, :] = value.astype(jnp.bfloat16)


def to_memory_first(ref, into, mem):
    count = ref.shape[0] // TILE
    last = (count - 1) * TILE
    value = picked(ref, 0, TILE, (mem, TILE, -mem))
    value = value + picked(ref, last, last + TILE, (0, mem, TILE - 2 * mem))
    into[:TILE, :] = value.astype(jnp.bfloat16)
    for i in range(1, count):
        runs = [(0, TILE, 16 - mem)]
        if i == count - 1:
            runs = [(0, TILE - mem, 16 - mem), (TILE - mem, TILE, 16)]
        value = picked(ref, i * TILE - 16, (i + 1) * TILE, *runs)
        into[i * TILE : (i + 1) * TILE, :] = value.astype(jnp.bfloat16)


def gather_attend_kernel(
    mem, wq, wk, wv, wo, w1, w2, vec, x_ref, key_ids, query_ids, pull_in,
    o0, o1, o2, small, inner, q_out, k_out, v_out, out_ref, lse_ref, pull_out,
    q_ref, k_ref, v_ref, w0, a1, a2, av, got, v_turned, send, recv, own_sem, load_sem,
):
    rep, owner, y, c, z, x, where = place()
    part = W // 8
    low = jnp.bfloat16
    across = (1 - y) * 2 + c
    mine0 = pl.ds(owner * part, part)
    loads = [
        pltpu.make_async_copy(source, into, load_sem.at[i])
        for i, (source, into) in enumerate(
            [(source, w0.at[i, mine0, :]) for i, source in enumerate((wq, wk, wv, wo))]
            + [(w1.at[:, i * W : (i + 1) * W], a1.at[i]) for i in range(4)]
            + [(w2, a2), (vec, av)]
        )
    ]
    for load in loads:
        load.start()

    near = (z + 3) % 4 - 2 * ((3 - z) // 3)
    far = 3 * (1 - z // 2)
    owners_z = (z, near, 6 - z - near - far, far)

    def shard(turn, other_x):
        return owners_z[turn] * 2 + (1 - x if other_x else x)

    def spot(g, kind, turn, other_x, quarter):
        at = 2 * TILE + quarter * TILE if kind else c * TILE
        lanes = pl.ds(pl.multiple_of(at, TILE), TILE)
        if g == 2:
            return o2.at[pl.ds(shard(turn, other_x) * 4 * part, 4 * part), lanes]
        return (w0, o1)[g].at[:, pl.ds(shard(turn, other_x) * part, part), lanes]

    greet(where)
    for load in loads:
        load.wait()
    own = [
        pltpu.make_async_copy(a1, o1.at[:, mine0, :], own_sem.at[0]),
        pltpu.make_async_copy(a2, o2.at[pl.ds(owner * 4 * part, 4 * part), :], own_sem.at[1]),
    ]
    kept = pltpu.make_async_copy(w0, o0, own_sem.at[2])
    note = pltpu.make_async_copy(av, got.at[owner], own_sem.at[3])
    copies = Copies(send, recv)

    for k in (1, 2, 3):
        copies.start(("v", "z", k), av, got.at[owner], where["z", k])
        copies.start(("v", "zx", k), av, got.at[owner], where["zx", k])
    copies.start(("v", "x", 0), av, got.at[owner], where["x"])
    for g in (0, 1, 2):
        for kind in (1, 0):
            at = 2 * TILE + rep * TILE if kind else c * TILE
            lanes = pl.ds(pl.multiple_of(at, TILE), TILE)
            source = (w0.at[:, mine0, lanes], a1.at[:, :, lanes], a2.at[:, lanes])[g]
            here = spot(g, kind, 0, False, rep)
            copies.plan((g, kind, "x", 0), source, here, where["x"])
            for start, end, turn in Z_ROUTES:
                through = (rep, end * 2 + x)
                relayed = turn == 3 and start in (1, 2) and end in (0, 3)
                from_here = spot(g, kind, 3, False, rep) if relayed else source
                into = spot(g, kind, 3, False, rep) if relayed else here
                copies.plan(
                    (g, kind, "z", start, end, turn), from_here, into, through, z == start, z == end
                )
    steps = [
        (0, True, "x"), (1, False, "z"), (2, False, "z"), (1, True, "x"),
        (3, False, "z"), (2, True, "x"), (3, True, "x"),
    ]
    for g in (0, 1, 2):
        for turn, other_x, stage in steps:
            for kind in (0, 1):
                here = spot(g, kind, turn, other_x, rep)
                if stage == "z":
                    copies.plan((g, kind, "x", turn), here, here, where["x"])
                if kind:
                    copies.plan((g, "y", turn, other_x), here, here, where["y"])
                    there = spot(g, kind, turn, other_x, across)
                    copies.plan((g, "diagonal", turn, other_x), there, there, where["core"])
                copies.plan((g, kind, "core", turn, other_x), here, here, where["core"])

    def begin(g, turns):
        for start, end, turn in Z_ROUTES:
            if turn in turns and not (turn == 3 and start in (1, 2)):
                for kind in (1, 0):
                    copies.go((g, kind, "z", start, end, turn))

    copies.go((0, 1, "x", 0))
    copies.go((0, 0, "x", 0))
    for g in (0, 1, 2):
        begin(g, (1, 2, 3))
    note.start()
    for copy in own:
        copy.start()
    to_tokens_first(pull_in, pull_out, mem)

    def pass_on(g, step):
        turn, other_x, stage = steps[step]
        for kind in (1, 0):
            if stage == "x":
                copies.arrived((g, kind, "x", turn))
            else:
                for start, end, at_turn in Z_ROUTES:
                    if at_turn == turn:
                        copies.arrived((g, kind, "z", start, end, turn))
                if turn == 3:
                    copies.go((g, kind, "z", 1, 0, 3))
                    copies.go((g, kind, "z", 2, 3, 3))
                copies.go((g, kind, "x", turn))
            if kind:
                copies.go((g, "y", turn, other_x))
            copies.go((g, kind, "core", turn, other_x))
        if step == 4 and g < 2:
            for kind in (1, 0):
                copies.go((g + 1, kind, "x", 0))

    def pass_core(g, step):
        turn, other_x, _ = steps[step]
        copies.arrived((g, "y", turn, other_x))
        copies.go((g, "diagonal", turn, other_x))

    def settle(g):
        for k, other_x, _ in steps:
            copies.arrived((g, 0, "core", k, other_x))
            copies.arrived((g, 1, "core", k, other_x))
            copies.arrived((g, "diagonal", k, other_x))

    def pump(events):
        for kind, g, step in events:
            (pass_core if kind == "c" else pass_on)(g, step)

    pump(EARLY)
    settle(0)
    for k in (1, 2, 3):
        copies.arrived(("v", "z", k))
        copies.arrived(("v", "zx", k))
    copies.arrived(("v", "x", 0))
    note.wait()
    kept.start()

    lanes = lax.broadcasted_iota(jnp.int32, (TILE, W), 1)
    rows = lax.broadcasted_iota(jnp.int32, (TILE, W), 0)
    joined = jnp.zeros((16, W), jnp.float32)
    for o in range(8):
        pick = ((lanes == rows + o * part) & (rows < part)).astype(low)
        joined = joined + product(got[o], pick)
        for j in range(3):
            i = o * 3 + j
            inner[i // 6 : i // 6 + 1, (i % 6) * TILE : (i % 6 + 1) * TILE] = got[
                o, 8 + j : 9 + j, :
            ].astype(jnp.float32)
    small[...] = joined[:8]

    @pl.loop(0, 4)
    def _(block):
        span = pl.ds(pl.multiple_of(block * 256, 256), 256)
        value = x_ref[span, :]
        q_ref[span, :] = (product(value, w0[0]) + small[0:1, :]).astype(low)
        k_ref[span, :] = product(value, w0[1]).astype(low)
        v_ref[span, :] = (product(value, w0[2]) + small[1:2, :]).astype(low)
        for which, events in enumerate(DURING_PROJECTIONS):

            @pl.when(block == which)
            def _():
                pump(events)

    leaving = [
        pltpu.make_async_copy(ref, into, own_sem.at[4 + i])
        for i, (ref, into) in enumerate(((q_ref, q_out), (k_ref, k_out), (v_ref, v_out)))
    ]
    for copy in leaving:
        copy.start()

    def at_half(pair, half):
        for which, events in enumerate(DURING_ATTENTION[half::2]):
            if events:
                pl.when(pair == which)(functools.partial(pump, events))

    @pl.loop(0, 6)
    def _(pair):
        columns = pl.ds(pl.multiple_of(pair * TILE, TILE), TILE)
        attend_pair(
            key_ids, query_ids, q_ref.at[:, columns], k_ref.at[:, columns], v_ref.at[:, columns],
            out_ref.at[:, columns], lse_ref.at[pair], v_turned, lambda: at_half(pair, 0),
        )
        at_half(pair, 1)

    pump(LATE)
    settle(1)
    settle(2)
    copies.drain()
    for copy in own:
        copy.wait()
    kept.wait()
    for copy in leaving:
        copy.wait()


Z_ROUTES = (
    (0, 1, 1), (1, 0, 1), (1, 2, 1), (2, 3, 1), (2, 1, 2), (3, 2, 2), (1, 3, 2), (2, 0, 2),
    (0, 2, 3), (3, 1, 3), (1, 0, 3), (2, 3, 3),
)
GATHER_COPIES = 7 + 3 * (2 * (1 + 12) + 2 * 3 + 7 * 4)


def run(g, *order):
    return [(name[0], g, int(name[1])) for name in order]


EARLY = run(0, "p0", "p1", "p2", "c0", "p3", "p4", "c1", "p5", "c2", "p6", "c3", "c4", "c5", "c6")
DURING_PROJECTIONS = [run(1, "p0"), run(1, "p1"), run(1, "p2", "c0"), run(1, "p3", "c1")]
DURING_ATTENTION = [
    run(1, "p4"),
    run(1, "c2"),
    run(1, "p5", "c3", "p6"),
    run(2, "p0") + run(1, "c4"),
    run(2, "p1"),
    run(1, "c5", "c6"),
    run(2, "p2", "c0"),
    run(2, "p3"),
    run(2, "c1"),
    run(2, "p4"),
    run(2, "c2", "p5"),
    run(2, "c3"),
]
LATE = run(2, "p6", "c4", "c5", "c6")


def gather_attend(shards, rows, key_ids, query_ids, pull, mem):
    low, full = jnp.bfloat16, jnp.float32
    count = rows.shape[0]
    vectors = shards[-1]
    anywhere, near = pl.BlockSpec(memory_space=pl.ANY), pl.BlockSpec(memory_space=pltpu.VMEM)
    thin = jax.ShapeDtypeStruct((count, W), low)
    return pl.pallas_call(
        functools.partial(gather_attend_kernel, mem),
        out_shape=(
            jax.ShapeDtypeStruct((4, W, W), low),
            jax.ShapeDtypeStruct((4, W, W), low),
            jax.ShapeDtypeStruct((4 * W, W), low),
            jax.ShapeDtypeStruct((8, W), full),
            jax.ShapeDtypeStruct((4, W), full),
            thin,
            thin,
            thin,
            thin,
            jax.ShapeDtypeStruct((W // TILE, count // TILE, 2 * TILE), full),
            thin,
        ),
        in_specs=[anywhere] * 7 + [near] * 4,
        out_specs=[anywhere] * 3 + [near] * 2 + [anywhere] * 3 + [near] * 3,
        scratch_shapes=[
            pltpu.VMEM((count, W), low),
            pltpu.VMEM((count, W), low),
            pltpu.VMEM((count, W), low),
            pltpu.VMEM((4, W, W), low),
            pltpu.VMEM((4, W // 8, W), low),
            pltpu.VMEM(shards[5].shape, low),
            pltpu.VMEM(vectors.shape, low),
            pltpu.VMEM((8,) + vectors.shape, low),
            pltpu.VMEM((TILE, count), low),
            pltpu.SemaphoreType.DMA((GATHER_COPIES,)),
            pltpu.SemaphoreType.DMA((GATHER_COPIES,)),
            pltpu.SemaphoreType.DMA((7,)),
            pltpu.SemaphoreType.DMA((10,)),
        ],
        compiler_params=pltpu.CompilerParams(
            collective_id=0, has_side_effects=True, vmem_limit_bytes=48 << 20
        ),
        name="gather_attend",
    )(*shards, rows, key_ids, query_ids, pull)


def attend_back(key_ids, query_ids, query, keys, values, grads, lse):
    rows, width = query.shape
    pair = 2 * HEAD_DIM
    count = rows // TILE
    column = pl.BlockSpec((rows, pair), lambda h: (0, h))
    whole = lambda a: pl.BlockSpec(a.shape, lambda h: (0, 0))
    return pl.pallas_call(
        attend_back_kernel,
        grid=(width // pair,),
        out_shape=(jax.ShapeDtypeStruct((rows, width), jnp.bfloat16),) * 3,
        in_specs=[whole(key_ids), whole(query_ids)]
        + [column] * 4
        + [pl.BlockSpec((1, count, 2 * TILE), lambda h: (h, 0, 0))],
        out_specs=[column] * 3,
        scratch_shapes=[
            pltpu.VMEM((pair, rows), jnp.bfloat16),
            pltpu.VMEM((rows, pair), jnp.float32),
            pltpu.VMEM((rows, pair), jnp.float32),
        ],
        compiler_params=pltpu.CompilerParams(vmem_limit_bytes=48 << 20),
        name="attend_back",
    )(key_ids, query_ids, query, keys, values, grads, lse)


ERFC_TERMS = (
    -1.26551223, 1.00002368, 0.37409196, 0.09678418, -0.18628806,
    0.27886807, -1.13520398, 1.48851587, -0.82215223, 0.17087277,
)


def gelu_and_slope(value):
    half_square = value * value * 0.5
    step = 1.0 / (1.0 + jnp.abs(value) * (0.5 * 0.5**0.5))
    power = ERFC_TERMS[-1]
    for term in ERFC_TERMS[-2::-1]:
        power = power * step + term
    tail = 0.5 * step * jnp.exp(power - half_square)
    cover = jnp.where(value < 0, tail, 1.0 - tail)
    density = jnp.exp(-half_square) * ((0.5 / math.pi) ** 0.5)
    return value * cover, cover + value * density


def reduce_attend_kernel(
    mem, q_in, k_in, v_in, g_in, x_in, gh_in, w_in, go, g1, g2, layer_in, lse_ref, key_ids,
    query_ids, sums_in, inner_in, tokens_ref, memory_ref, layer_ref, rq, rk, rw, ro, r1, r2, rv,
    gx, held, x_kept, x_turned, grads, dw, k_turned, k_total, v_total,
    keep0, keep1, keep2, core0, core1, core2, got_y, got_x, got_z, ends, vec,
    send, recv, load_sem, own_sem,
):
    rep, owner, y, c, z, x, where = place()
    part = W // 8
    low = jnp.bfloat16
    loads = [
        pltpu.make_async_copy(source, into, load_sem.at[i])
        for i, (source, into) in enumerate(
            [(source, held.at[i]) for i, source in enumerate((q_in, k_in, v_in, g_in))]
            + [(x_in, x_kept), (gh_in, gx), (go, dw.at[3])]
        )
    ]
    for load in loads:
        load.start()
    copies = Copies(send, recv)
    keep, core = (keep0, keep1, keep2), (core0, core1, core2)
    order = (1, 3, 2, 0)
    flat = [(k, o) for k in order for o in (1, 0)]

    def shard(k, o):
        return ((z + k) % 4) * 2 + (1 - x if o else x)

    def lanes(kind, this_core):
        which = 0 if this_core else 1
        own_core = c if which == 0 else 1 - c
        at = {
            0: 2 * TILE + ((1 - y) * 2 + own_core) * TILE,
            1: own_core * TILE,
            2: 2 * TILE + (y * 2 + own_core) * TILE,
        }[kind]
        return at

    def columns(kind, this_core, block=0):
        return pl.ds(pl.multiple_of(block * W + lanes(kind, this_core), TILE), TILE)

    def sources(g, kind, this_core):
        if g == 0:
            return [dw.at[j, :, columns(kind, this_core)] for j in range(4)]
        if g == 1:
            return [g1.at[:, columns(kind, this_core, j)] for j in range(4)]
        return [g2.at[:, :, columns(kind, this_core)]]

    def targets(g, kind, refs):
        return [refs[g].at[kind, j] for j in range(4)] if g < 2 else [refs[g].at[kind]]

    def cut(g, kind, refs, k, o):
        if g == 2:
            return refs[g].at[kind, pl.ds(shard(k, o) * 4, 4), :, :]
        return refs[g].at[kind, :, pl.ds(shard(k, o) * part, part), :]

    own = {}
    for g in (2, 1, 0):
        for kind in (0, 1, 2):
            pairs = zip(sources(g, kind, False), targets(g, kind, core))
            for j, (source, into) in enumerate(pairs):
                copies.plan((g, "core", kind, j), source, into, where["core"])
            pairs = zip(sources(g, kind, True), targets(g, kind, keep))
            for j, (source, into) in enumerate(pairs):
                own[g, kind, j] = pltpu.make_async_copy(source, into, own_sem.at[len(own)])
        for i, (k, o) in enumerate(flat):
            copies.plan((g, "y", k, o), cut(g, 0, keep, k, o), got_y.at[g, i], where["y"])
        for k in order:
            for s, kind in enumerate((1, 2)):
                copies.plan(
                    (g, kind, "x", k), cut(g, kind, keep, k, 1), got_x.at[g, s, k], where["x"]
                )
                if k:
                    copies.plan(
                        (g, kind, "z", k), cut(g, kind, keep, k, 0), got_z.at[g, s, k - 1],
                        where["z", k],
                    )
        copies.plan((g, 1, "ey"), ends.at[g, 0, 0], ends.at[g, 0, 1], where["y"])
        copies.plan((g, 1, "ecore"), ends.at[g, 0, 2], ends.at[g, 0, 3], where["core"])
        copies.plan((g, 2, "ey"), ends.at[g, 1, 0], ends.at[g, 1, 1], where["y"])
        copies.plan((g, 2, "ecore"), ends.at[g, 1, 0], ends.at[g, 1, 2], where["core"])
        copies.plan((g, 2, "ediagonal"), ends.at[g, 1, 1], ends.at[g, 1, 3], where["core"])
    copies.plan(("v", "core"), vec.at[0], vec.at[1], where["core"])
    copies.plan(("v", "y"), vec.at[2], vec.at[3], where["y"])
    copies.plan(("v", "x"), vec.at[4], vec.at[5], where["x"])
    for k in (1, 2, 3):
        copies.plan(("v", "z", k), vec.at[6], vec.at[6 + k], where["z", k])

    def begin(g, blocks):
        for kind in (0, 1, 2):
            for j in blocks:
                copies.go((g, "core", kind, j))
                own[g, kind, j].start()

    def ready(g, kind):
        for j in range(4 if g < 2 else 1):
            own[g, kind, j].wait()
            copies.arrived((g, "core", kind, j))

    def put(target, *refs):
        target[...] = total(*refs).astype(low)

    def cores(g):
        ready(g, 0)
        for k, o in flat:
            here = cut(g, 0, keep, k, o)
            put(here, here, cut(g, 0, core, k, o))
            copies.go((g, "y", k, o))
        ready(g, 1)
        for k in order:
            here = cut(g, 1, keep, k, 1)
            put(here, here, cut(g, 1, core, k, 1))
            copies.go((g, 1, "x", k))
        ready(g, 2)

    def over_y(g, k):
        copies.arrived((g, "y", k, 1))
        here = cut(g, 2, keep, k, 1)
        put(here, here, cut(g, 2, core, k, 1), got_y.at[g, flat.index((k, 1))])
        copies.go((g, 2, "x", k))

    def half_over_x(g, k):
        copies.arrived((g, 1, "x", k))
        here = cut(g, 1, keep, k, 0)
        put(here, here, cut(g, 1, core, k, 0), got_x.at[g, 0, k])
        copies.go((g, 1, "z", k))

    def over_x(g, k):
        copies.arrived((g, "y", k, 0))
        copies.arrived((g, 2, "x", k))
        here = cut(g, 2, keep, k, 0)
        put(
            here, here, cut(g, 2, core, k, 0), got_y.at[g, flat.index((k, 0))], got_x.at[g, 1, k]
        )
        copies.go((g, 2, "z", k))

    def half_over_z(g):
        copies.arrived((g, 1, "x", 0))
        for k in (1, 2, 3):
            copies.arrived((g, 1, "z", k))
        put(
            ends.at[g, 0, 0], cut(g, 1, keep, 0, 0), cut(g, 1, core, 0, 0), got_x.at[g, 0, 0],
            *(got_z.at[g, 0, k] for k in range(3)),
        )
        copies.go((g, 1, "ey"))

    def over_z(g):
        copies.arrived((g, 2, "x", 0))
        copies.arrived((g, "y", 0, 0))
        for k in (1, 2, 3):
            copies.arrived((g, 2, "z", k))
        put(
            ends.at[g, 1, 0], cut(g, 2, keep, 0, 0), cut(g, 2, core, 0, 0), got_x.at[g, 1, 0],
            got_y.at[g, flat.index((0, 0))], *(got_z.at[g, 1, k] for k in range(3)),
        )
        copies.go((g, 2, "ey"))
        copies.go((g, 2, "ecore"))

    def write(g, s, slot, at):
        value = ends[g, s, slot].astype(jnp.float32)
        for j in range(4):
            if g == 0:
                (rq, rk, rw, ro)[j][:, pl.ds(pl.multiple_of(at, TILE), TILE)] = value[j]
            elif g == 1:
                r1[:, pl.ds(pl.multiple_of(j * W + at, TILE), TILE)] = value[j]
            else:
                r2[j * part : (j + 1) * part, pl.ds(pl.multiple_of(at, TILE), TILE)] = value[j]

    def half_finish(g):
        copies.arrived((g, 1, "ey"))
        put(ends.at[g, 0, 2], ends.at[g, 0, 0], ends.at[g, 0, 1])
        copies.go((g, 1, "ecore"))

    def finish(g):
        copies.arrived((g, 2, "ey"))
        copies.go((g, 2, "ediagonal"))
        write(g, 0, 2, lanes(1, True))
        write(g, 1, 0, lanes(2, True))
        write(g, 1, 1, lanes(0, True))

    def close(g):
        copies.arrived((g, 2, "ecore"))
        write(g, 1, 2, lanes(2, False))
        copies.arrived((g, 1, "ecore"))
        write(g, 0, 3, lanes(1, False))
        copies.arrived((g, 2, "ediagonal"))
        write(g, 1, 3, lanes(0, False))

    acts = {
        "a": cores, "h": half_over_x, "b": over_y, "c": over_x, "s": half_over_z, "d": over_z,
        "t": half_finish, "f": finish, "g": close,
    }

    def pump(events):
        for event in events:
            act = acts[event[0]]
            if len(event) == 3:
                act(int(event[1]), int(event[2]))
            else:
                act(int(event[1]))

    greet(where)
    begin(2, (0,))
    begin(1, range(4))
    for load in loads:
        load.wait()
    begin(0, (3,))
    x_turned[...] = x_kept[...].T
    pump(BEFORE_BACK)

    def at_half(pair, half):
        for which, events in enumerate(DURING_BACK[half::2]):
            if events:
                pl.when(pair == which)(functools.partial(pump, events))

    @pl.loop(0, 6)
    def _(pair):
        at = pl.ds(pl.multiple_of(pair * TILE, TILE), TILE)
        attend_back_pair(
            key_ids, query_ids, *(held.at[i, :, at] for i in range(4)), lse_ref.at[pair],
            *(grads.at[i, :, at] for i in range(3)), k_turned, k_total, v_total,
            lambda: at_half(pair, 0),
        )
        at_half(pair, 1)

    fetch = [pltpu.make_async_copy(w_in.at[i], held.at[i, 0:W, :], load_sem.at[i]) for i in range(3)]
    fetch.append(pltpu.make_async_copy(layer_in, held.at[3], load_sem.at[3]))
    for copy in fetch:
        copy.start()
    for i in range(3):

        @pl.loop(0, 3)
        def _(block):
            span = pl.ds(pl.multiple_of(block * 256, 256), 256)
            dw[i, span, :] = product(x_turned[span, :], grads[i]).astype(low)

        begin(0, (i,))
        pump(DURING_WEIGHTS[i])
    vec[0, 0:1, :] = column_sum(grads[0])[None]
    vec[0, 1:2, :] = column_sum(grads[2])[None]
    vec[0, 2:8, :] = sums_in[2:8, :]
    vec[0, 8:12, :] = inner_in[...]
    vec[0, 12:16, :] = jnp.zeros((4, W), jnp.float32)
    copies.go(("v", "core"))
    pump(("a0",))
    copies.arrived(("v", "core"))
    vec[2] = vec[0] + vec[1]
    copies.go(("v", "y"))
    for copy in fetch:
        copy.wait()

    @pl.loop(0, 4)
    def _(block):
        span = pl.ds(pl.multiple_of(block * 256, 256), 256)
        value = gx[span, :]
        for i in range(3):
            value = value + against(grads[i, span, :], held[i, 0:W, :])
        gx[span, :] = value
        for which, events in enumerate(DURING_ROWS):

            @pl.when(block == which)
            def _():
                pump(events)

    copies.arrived(("v", "y"))
    vec[4] = vec[2] + vec[3]
    copies.go(("v", "x"))
    pump(AFTER_ROWS)
    copies.arrived(("v", "x"))
    vec[6] = vec[4] + vec[5]
    for k in (1, 2, 3):
        copies.go(("v", "z", k))
    pump(LAST)
    seg = gx.shape[0] - 2 * mem
    tokens_ref[...] = gx[...].astype(low)
    memory_ref[...] = (gx[seg : seg + mem, :] + gx[seg + mem : seg + 2 * mem, :]).astype(low)
    pump(("d0",))
    to_memory_first(held.at[3], layer_ref, mem)
    pump(("f0",))
    for k in (1, 2, 3):
        copies.arrived(("v", "z", k))
    rv[...] = (vec[6] + vec[7]) + (vec[8] + vec[9])
    pump(("g2", "g1", "g0"))
    copies.drain()


REDUCE_COPIES = 3 + 12 + 12 + 3 * (8 + 4 + 4 + 3 + 3 + 5) + 6
BEFORE_BACK = ("a2",)
DURING_BACK = (
    ("a1", "h21", "b21"),
    ("h23",),
    ("b23", "h22"),
    ("b22", "h11"),
    ("h13", "s2"),
    ("b20", "h12"),
    ("c21", "b11"),
    ("c23", "s1"),
    ("c22", "b13"),
    ("c11", "b12"),
    ("c13", "d2"),
    ("b10", "c12"),
)
DURING_WEIGHTS = (
    ("t2",),
    (),
    ("t1", "d1"),
)
DURING_ROWS = (
    ("f2", "f1"),
    (),
    ("h01", "b01"),
    ("h03",),
)
AFTER_ROWS = ("h02", "b03", "c01", "b02", "c03")
LAST = ("b00", "c02", "s0", "t0")


def reduce_attend(
    mem, query, keys, values, grad_mixed, rows, grad_hidden, weights, grad_out, grad_inner,
    grad_outer, layer, lse, key_ids, query_ids, sums, inner_sums,
):
    low, full = jnp.bfloat16, jnp.float32
    count = rows.shape[0]
    part = W // 8
    anywhere, near = pl.BlockSpec(memory_space=pl.ANY), pl.BlockSpec(memory_space=pltpu.VMEM)
    slab = jax.ShapeDtypeStruct((part, W), full)
    piece = (4, part, TILE)
    wide, tall = pltpu.VMEM((3, 4, W, TILE), low), pltpu.VMEM((3, 32, part, TILE), low)
    return pl.pallas_call(
        functools.partial(reduce_attend_kernel, mem),
        out_shape=(
            jax.ShapeDtypeStruct((count, W), low),
            jax.ShapeDtypeStruct((mem, W), low),
            jax.ShapeDtypeStruct((count, W), low),
            slab,
            slab,
            slab,
            slab,
            jax.ShapeDtypeStruct((part, 4 * W), full),
            jax.ShapeDtypeStruct((4 * part, W), full),
            jax.ShapeDtypeStruct((16, W), full),
        ),
        in_specs=[anywhere] * 11 + [near] * 5,
        out_specs=[near] * 10,
        scratch_shapes=[
            pltpu.VMEM((count, W), full),
            pltpu.VMEM((4, count, W), low),
            pltpu.VMEM((count, W), low),
            pltpu.VMEM((W, count), low),
            pltpu.VMEM((3, count, W), low),
            pltpu.VMEM((4, W, W), low),
            pltpu.VMEM((TILE, count), low),
            pltpu.VMEM((count, TILE), full),
            pltpu.VMEM((count, TILE), full),
            wide,
            wide,
            tall,
            wide,
            wide,
            tall,
            pltpu.VMEM((3, 8) + piece, low),
            pltpu.VMEM((3, 2, 4) + piece, low),
            pltpu.VMEM((3, 2, 3) + piece, low),
            pltpu.VMEM((3, 2, 4) + piece, low),
            pltpu.VMEM((10, 16, W), full),
            pltpu.SemaphoreType.DMA((REDUCE_COPIES,)),
            pltpu.SemaphoreType.DMA((REDUCE_COPIES,)),
            pltpu.SemaphoreType.DMA((7,)),
            pltpu.SemaphoreType.DMA((27,)),
        ],
        compiler_params=pltpu.CompilerParams(
            collective_id=1, has_side_effects=True, vmem_limit_bytes=62 << 20
        ),
        name="reduce_attend",
    )(
        query, keys, values, grad_mixed, rows, grad_hidden, weights, grad_out, grad_inner,
        grad_outer.reshape(32, part, W), layer, lse, key_ids, query_ids, sums, inner_sums,
    )


def normalise(value):
    mean = jnp.mean(value, axis=1, keepdims=True)
    centred = value - mean
    scale = lax.rsqrt(jnp.mean(centred * centred, axis=1, keepdims=True) + 1e-05)
    return centred * scale, scale


def normalise_back(grad, unit, scale):
    middle = jnp.mean(grad, axis=1, keepdims=True)
    along = jnp.mean(grad * unit, axis=1, keepdims=True)
    return scale * (grad - middle - unit * along)


def chain_kernel(
    mixed_ref, rows_ref, pull_ref, wo_ref, w1_ref, w2_ref, small_ref, b1_ref,
    out_ref, y1_ref, u_ref, gz_ref, gf_ref, gh_ref, ga_ref, gmix_ref, sums_ref, b1_sum_ref,
    slope_ref,
):
    low = jnp.bfloat16

    @pl.when(pl.program_id(0) == 0)
    def _():
        sums_ref[...] = jnp.zeros_like(sums_ref)
        b1_sum_ref[...] = jnp.zeros_like(b1_sum_ref)

    def small(i):
        return small_ref[i : i + 1, :]

    def gather_sum(ref, i, value):
        ref[i : i + 1, :] += jnp.sum(value, axis=0, keepdims=True)

    hidden = rows_ref[...].astype(jnp.float32) + product(mixed_ref[...], wo_ref[0]) + small(2)
    unit_one, scale_one = normalise(hidden)
    y1 = unit_one * small(3) + small(4)
    y1_low = y1.astype(low)
    y1_ref[...] = y1_low
    second = y1 + small(5)
    for r in range(4):
        inner = product(y1_low, w1_ref[r]) + b1_ref[r : r + 1, :]
        active, slope = gelu_and_slope(inner)
        active = active.astype(low)
        u_ref[:, r * W : (r + 1) * W] = active
        slope_ref[:, r * W : (r + 1) * W] = slope
        second = second + product(active, w2_ref[r * W : (r + 1) * W, :])
    unit_two, scale_two = normalise(second)
    out_ref[...] = (unit_two * small(6) + small(7)).astype(low)
    pull = pull_ref[...].astype(jnp.float32)
    gather_sum(sums_ref, 6, pull * unit_two)
    gather_sum(sums_ref, 7, pull)
    grad_second = normalise_back(pull * small(6), unit_two, scale_two)
    gz = grad_second.astype(low)
    gz_ref[...] = gz
    gather_sum(sums_ref, 5, gz.astype(jnp.float32))
    grad_y1 = grad_second
    for r in range(4):
        gf = against(gz, w2_ref[r * W : (r + 1) * W, :]) * slope_ref[:, r * W : (r + 1) * W]
        gf = gf.astype(low)
        gf_ref[:, r * W : (r + 1) * W] = gf
        gather_sum(b1_sum_ref, r, gf.astype(jnp.float32))
        grad_y1 = grad_y1 + against(gf, w1_ref[r])
    gather_sum(sums_ref, 3, grad_y1 * unit_one)
    gather_sum(sums_ref, 4, grad_y1)
    grad_hidden = normalise_back(grad_y1 * small(3), unit_one, scale_one)
    gh_ref[...] = grad_hidden
    ga = grad_hidden.astype(low)
    ga_ref[...] = ga
    gather_sum(sums_ref, 2, ga.astype(jnp.float32))
    gmix_ref[...] = against(ga, wo_ref[0]).astype(low)


def chain(mixed, rows, pull, weights, inner_blocks, outer_mat, small, inner_bias):
    count, width = rows.shape
    step = 256
    low, full = jnp.bfloat16, jnp.float32
    thin = pl.BlockSpec((step, width), lambda i: (i, 0))
    fat = pl.BlockSpec((step, 4 * width), lambda i: (i, 0))
    held = lambda shape: pl.BlockSpec(shape, lambda i: (0,) * len(shape))
    once = pl.Buffered(1)
    return pl.pallas_call(
        chain_kernel,
        grid=(count // step,),
        out_shape=(
            jax.ShapeDtypeStruct((count, width), low),
            jax.ShapeDtypeStruct((count, width), low),
            jax.ShapeDtypeStruct((count, 4 * width), low),
            jax.ShapeDtypeStruct((count, width), low),
            jax.ShapeDtypeStruct((count, 4 * width), low),
            jax.ShapeDtypeStruct((count, width), full),
            jax.ShapeDtypeStruct((count, width), low),
            jax.ShapeDtypeStruct((count, width), low),
            jax.ShapeDtypeStruct((8, width), full),
            jax.ShapeDtypeStruct((4, width), full),
        ),
        in_specs=[
            thin, thin, thin,
            pl.BlockSpec((1, width, width), lambda i: (3, 0, 0), pipeline_mode=once),
            pl.BlockSpec((4, width, width), lambda i: (0, 0, 0), pipeline_mode=once),
            pl.BlockSpec((4 * width, width), lambda i: (0, 0), pipeline_mode=once),
            held((8, width)), held((4, width)),
        ],
        out_specs=[thin, thin, fat, thin, fat, thin, thin, thin, held((8, width)), held((4, width))],
        scratch_shapes=[pltpu.VMEM((step, 4 * width), full)],
        compiler_params=pltpu.CompilerParams(vmem_limit_bytes=60 << 20),
        name="chain",
    )(mixed, rows, pull, weights, inner_blocks, outer_mat, small, inner_bias)


def on_device(
    tokens,
    read_memory,
    doc_ids,
    w_query,
    w_key,
    w_value,
    w_out,
    query_bias,
    value_bias,
    out_bias,
    norm_one_gain,
    norm_one_bias,
    w_inner,
    inner_bias,
    w_outer,
    outer_bias,
    norm_two_gain,
    norm_two_bias,
    out_grad,
):
    owners = lax.axis_size("fsdp")
    wide = owners == 8 and lax.axis_size("rep") == 4
    part = w_query.shape[0]
    low = jnp.bfloat16
    small = pack(
        jnp.stack(
            [
                query_bias, value_bias, out_bias, norm_one_gain,
                norm_one_bias, outer_bias, norm_two_gain, norm_two_bias,
            ]
        )[None],
        inner_bias[None],
    )[0]
    seqs, seg = doc_ids.shape
    width = tokens.shape[1]
    mem = read_memory.shape[0] // seqs
    length = seg + 2 * mem
    memory_rows = read_memory.reshape(seqs, mem, width)
    rows = jnp.concatenate([tokens.reshape(seqs, seg, width), memory_rows, memory_rows], axis=1)
    rows = rows.reshape(seqs * length, width)
    marks = jnp.full((seqs, 2 * mem), -1, jnp.int32)
    ids = jnp.concatenate([doc_ids, marks], axis=1)

    def each(function, *arrays):
        results = []
        for s in range(seqs):
            own = slice(s * length, (s + 1) * length)
            spread = jnp.broadcast_to(ids[s][:, None], (length, TILE))
            by_block = ids[s].reshape(length // TILE, TILE)
            results.append(function(spread, by_block, *[a[own] for a in arrays]))
        return results

    shards = (w_query, w_key, w_value, w_out, w_inner, w_outer, small)
    wide = wide and seqs == 1
    if wide:
        spread, by_block = each(lambda *a: a)[0]
        (
            weights, inner_blocks, outer_mat, vectors, inner_shift, query, keys, values, mixed,
            lse, out_rows,
        ) = gather_attend(shards, rows, spread, by_block, out_grad, mem)
    else:
        out_rows = out_grad.reshape(seqs, length, width)
        out_rows = jnp.concatenate(
            [out_rows[:, mem : mem + seg], out_rows[:, :mem], out_rows[:, mem + seg :]], axis=1
        ).reshape(seqs * length, width)
        weights, inner_blocks, outer_mat, packed = plain_gather(*shards)
        vectors, inner_shift = unpack(packed.astype(jnp.float32), part)
        query = (product(rows, weights[0]) + vectors[0]).astype(low)
        keys = product(rows, weights[1]).astype(low)
        values = (product(rows, weights[2]) + vectors[1]).astype(low)
        pairs = each(attend, query, keys, values)
        mixed = jnp.concatenate([pair[0] for pair in pairs], axis=0)
    output, normed, active, grad_outer, grad_inner, grad_residual, grad_branch, grad_mixed, sums, inner_sums = chain(
        mixed, rows, out_rows, weights, inner_blocks, outer_mat, vectors, inner_shift
    )
    grad_w_outer = inner_rows(active, grad_outer).astype(low)
    grad_w_inner = inner_rows(normed, grad_inner).astype(low)
    grad_w_out = inner_rows(mixed, grad_branch).astype(low)
    if wide:
        grad_tokens, grad_memory, layer_out, *shares, joined = reduce_attend(
            mem, query, keys, values, grad_mixed, rows, grad_residual, weights, grad_w_out,
            grad_w_inner, grad_w_outer, output, lse, spread, by_block, sums, inner_sums,
        )
        grad_tokens = grad_tokens[:seg]
        place_of = lax.axis_index("fsdp")
        last = lax.dynamic_slice(joined[:8], (0, place_of * part), (8, part))
        last_inner = lax.dynamic_slice(
            joined[8:12].reshape(-1), (place_of * 4 * part,), (4 * part,)
        )
    else:
        triples = [
            attend_back(spread, by_block, q, k, v, g, pairs[s][1])
            for s, (spread, by_block, q, k, v, g) in enumerate(
                each(lambda *a: a, query, keys, values, grad_mixed)
            )
        ]
        grad_query_low, grad_keys_low, grad_values_low = (
            jnp.concatenate([triple[i] for triple in triples], axis=0) for i in range(3)
        )
        grad_w_query = inner_rows(rows, grad_query_low).astype(low)
        grad_w_key = inner_rows(rows, grad_keys_low).astype(low)
        grad_w_value = inner_rows(rows, grad_values_low).astype(low)
        sums = jnp.concatenate(
            [column_sum(grad_query_low)[None], column_sum(grad_values_low)[None], sums[2:]], axis=0
        )
        grad_rows = (
            grad_residual
            + against(grad_query_low, weights[0])
            + against(grad_keys_low, weights[1])
            + against(grad_values_low, weights[2])
        )
        *shares, share_small = plain_reduce(
            grad_w_query,
            grad_w_key,
            grad_w_value,
            grad_w_out,
            grad_w_inner,
            grad_w_outer,
            pack(
                sums.reshape(8, owners, part).transpose(1, 0, 2),
                inner_sums.reshape(owners, 4 * part),
            ),
        )
        last, last_inner = unpack(share_small[None], part)
        grad_rows = grad_rows.reshape(seqs, length, width)
        grad_tokens = grad_rows[:, :seg].reshape(seqs * seg, width).astype(jnp.bfloat16)
        grad_memory = (
            (grad_rows[:, seg : seg + mem] + grad_rows[:, seg + mem :])
            .reshape(seqs * mem, width)
            .astype(jnp.bfloat16)
        )
        layer_out = output.reshape(seqs, length, width)
        layer_out = jnp.concatenate(
            [layer_out[:, seg : seg + mem], layer_out[:, :seg], layer_out[:, seg + mem :]], axis=1
        ).reshape(seqs * length, width)
    return (
        layer_out,
        grad_tokens,
        grad_memory,
        *shares[:4],
        *(last[i] for i in range(5)),
        shares[4],
        last_inner.reshape(-1),
        shares[5],
        *(last[i] for i in range(5, 8)),
    )


def solution(mesh):
    return jax.shard_map(
        on_device,
        mesh=mesh,
        in_specs=(
            P(("rep", "fsdp"), None),
            P(("rep", "fsdp"), None),
            P(("rep", "fsdp"), None),
            P("fsdp", None),
            P("fsdp", None),
            P("fsdp", None),
            P("fsdp", None),
            P("fsdp"),
            P("fsdp"),
            P("fsdp"),
            P("fsdp"),
            P("fsdp"),
            P("fsdp", None),
            P("fsdp"),
            P("fsdp", None),
            P("fsdp"),
            P("fsdp"),
            P("fsdp"),
            P(("rep", "fsdp"), None),
        ),
        out_specs=(
            P(("rep", "fsdp"), None),
            P(("rep", "fsdp"), None),
            P(("rep", "fsdp"), None),
            P("fsdp", None),
            P("fsdp", None),
            P("fsdp", None),
            P("fsdp", None),
            P("fsdp"),
            P("fsdp"),
            P("fsdp"),
            P("fsdp"),
            P("fsdp"),
            P("fsdp", None),
            P("fsdp"),
            P("fsdp", None),
            P("fsdp"),
            P("fsdp"),
            P("fsdp"),
        ),
        check_vma=False,
    )
```
